256 devices in a mesh: groups: 2 (over z), scan: 128 (over x, y, core).
Axes of the slice: x: 8, y: 8, z: 2, core: 2. Of those that a mesh axis runs over, the one named last changes fastest.
The devices are a block of a 8x8x16 slice.
Arguments:
- object_field: float32 [2, 6144, 1792], P(None, ('groups', 'scan')), parts along dimension 1, may hold values from -8 to 8
- probe_field: float32 [2, 2048, 256], P(None, 'groups'), parts along dimension 1, may hold values from -3 to 3
- amplitudes: float32 [1024, 256, 256], P(('groups', 'scan')), parts along dimension 0, may hold values from 0.2 to 3
- offsets: int32 [1024, 2], P(('groups', 'scan')), parts along dimension 0, may hold values from -8 to 2984, as said below
- live_counts: int32 [256], P(('groups', 'scan')), parts along dimension 0, may hold values from 1 to 4, as said below
Outputs:
- new_object: float32 [2, 6144, 1792], P(None, ('groups', 'scan')), parts along dimension 1
- new_probe: float32 [2, 2048, 256], P(None, ('groups', 'scan')), parts along dimension 1
The draws below stay inside these ranges and needn't reach their ends.
There are 2 independent parts, one for each index of `groups`. The reference program is written for one: setup_inputs(seed, part) draws one part's arguments, and reference() takes and returns one part's arrays. A program takes and returns all parts, laid end to end along the dimension named above; each array names one. Nothing has to cross between parts.
Inputs may be any that keep to these rules, and one draw needn't show every extreme that they name: Position p lies in scan row p // 16, column p % 16: offsets[p, 0] is within 8 of 96 * (p // 16) and offsets[p, 1] within 8 of 48 + 96 * (p % 16); the first position of every block of 4, except position 511, has offsets[p, 0] = 96 * (p // 16) - 8; the single position 511 has offsets[p, 0] = 96 * (p // 16) + 8. Block b of 4 consecutive positions measures its first live_counts[b]; some block measures all 4 and some only one.
All inputs are finite; a program needn't handle non-finite values.
Results may differ from the reference program's by a relative error of at most 0.0013.
Values sent between devices are 32-bit elements; how exact they have to be, the bound alone decides.
A program may use at most 128 MiB of HBM per device.

```python
import math
import jax
import jax.numpy as jnp
from jax import lax

PATCH = 256
MODES = 4
STEP = 96
JITTER = 8
SIDE = 48
POS_DEV = 4
GRID_COLS = 16
COLS = 1792
OBJ_ROWS = 3072
POSITIONS = 512


def draw_object_field(key, part):
    first_key = jax.random.fold_in(key, 11)
    row_place = jnp.arange(OBJ_ROWS, dtype=jnp.float32) / OBJ_ROWS
    rising = 0.5 * jnp.exp(row_place * math.log(3.0))
    values = jax.random.normal(first_key, (2, OBJ_ROWS, COLS), jnp.float32)
    return jnp.clip(values * rising[None, :, None], -8.0, 8.0)


def draw_offsets(key, part):
    position_ids = jnp.arange(POSITIONS, dtype=jnp.int32)
    scan_row = position_ids // GRID_COLS
    scan_col = position_ids % GRID_COLS
    shake = jax.random.randint(jax.random.fold_in(key, 21), (POSITIONS, 2), -JITTER, JITTER + 1).astype(jnp.int32)
    row_shake = jnp.where(position_ids % POS_DEV == 0, -JITTER, shake[:, 0]).astype(jnp.int32)
    row_shake = row_shake.at[POSITIONS - 1].set(JITTER)
    col_shake = shake[:, 1].at[GRID_COLS - 1].set(JITTER)
    top_row = STEP * scan_row + row_shake
    left_col = SIDE + STEP * scan_col + col_shake
    return jnp.stack([top_row, left_col], 1).astype(jnp.int32)


def draw_live_counts(key, part):
    row_count = POSITIONS // POS_DEV
    counts = jax.random.randint(jax.random.fold_in(key, 31), (row_count,), 1, POS_DEV + 1).astype(jnp.int32)
    fullest = jax.random.randint(jax.random.fold_in(key, 32), (), 0, row_count).astype(jnp.int32)
    row_ids = jnp.arange(row_count, dtype=jnp.int32)
    counts = jnp.where(row_ids == fullest, POS_DEV, counts)
    counts = jnp.where(row_ids == (fullest + row_count // 2) % row_count, 1, counts)
    return counts.astype(jnp.int32)


def level_of(key, extent, cuts, low, high):
    level, own = 1.0, jax.random.fold_in(key, 6)
    for axis_at, blocks in cuts:
        steps = jnp.exp(jax.random.uniform(jax.random.fold_in(own, axis_at), (blocks,), jnp.float32, low / len(cuts), high / len(cuts)))
        level = level * jnp.repeat(steps, extent[axis_at] // blocks).reshape([-1 if axis == axis_at else 1 for axis in range(len(extent))])
    return level


def scatter_about(own_key, extent, width, most, kind=jnp.bfloat16):
    values = width * jax.random.normal(own_key, extent, jnp.float32)
    return jnp.clip(values, min=-most, max=most).astype(kind)


def setup_inputs(seed: int = 0, part: int = 0) -> dict:
    keys = jax.random.split(jax.random.key(seed), 6)
    own_keys = jax.random.split(jax.random.fold_in(keys[5], part), 6)
    return {
        "object_field": draw_object_field(jax.random.fold_in(jax.random.fold_in(keys[5], part), 71), part),
        "probe_field": scatter_about(own_keys[1], (2, MODES * PATCH, PATCH), 0.5, 3.0, jnp.float32),
        "amplitudes": jnp.clip(jnp.exp(math.log(3.0) - 2.7080502 * jax.random.uniform(own_keys[2], (POSITIONS, PATCH, PATCH), jnp.float32) ** level_of(own_keys[2], (POSITIONS, PATCH, PATCH), ((0, 128),), -0.2, 0.2)), 0.2, 3.0),
        "offsets": draw_offsets(jax.random.fold_in(jax.random.fold_in(keys[5], part), 71), part),
        "live_counts": draw_live_counts(jax.random.fold_in(jax.random.fold_in(keys[5], part), 71), part),
    }


def dft_tables(length, sine_sign):
    numbers = jnp.arange(length, dtype=jnp.int32)
    product = numbers[:, None] * numbers[None, :] % length
    angles = product.astype(jnp.float32) * (2.0 * math.pi / length)
    scaling = 1.0 / math.sqrt(length)
    cosine = jnp.cos(angles) * scaling
    sine_part = jnp.sin(angles) * (sine_sign * scaling)
    left_table = jnp.stack([jnp.stack([cosine, sine_part], 1), jnp.stack([-sine_part, cosine], 1)], 0).astype(jnp.bfloat16)
    right_table = jnp.stack([jnp.stack([cosine, -sine_part], 1), jnp.stack([sine_part, cosine], 1)], 0).astype(jnp.bfloat16)
    return (left_table, right_table)

def transform(exit_wave, tables):
    left_table, right_table = tables
    half_done = jnp.einsum('dkcm,camn->dakn', left_table.astype(jnp.float32), exit_wave.astype(jnp.float32), precision=lax.Precision.HIGHEST).astype(jnp.bfloat16)
    return jnp.einsum('camn,cndk->damk', half_done.astype(jnp.float32), right_table.astype(jnp.float32), precision=lax.Precision.HIGHEST)

def exit_update(obj_patch, probe_modes, amplitude, forward, inverse):
    probe_re, probe_im = (probe_modes[0], probe_modes[1])
    patch_re, patch_im = (obj_patch[0], obj_patch[1])
    exit_wave = jnp.stack([probe_re * patch_re - probe_im * patch_im, probe_re * patch_im + probe_im * patch_re]).astype(jnp.bfloat16)
    far_field = transform(exit_wave, forward)
    intensity = lax.optimization_barrier(jnp.sum(far_field[0] * far_field[0] + far_field[1] * far_field[1], axis=0))
    factor = amplitude / jnp.maximum(jnp.sqrt(intensity), 0.5) - 1.0
    far_change = (far_field * factor).astype(jnp.bfloat16)
    exit_change = transform(far_change, inverse)
    grad_re = lax.optimization_barrier(jnp.sum(probe_re * exit_change[0] + probe_im * exit_change[1], axis=0))
    grad_im = lax.optimization_barrier(jnp.sum(probe_re * exit_change[1] - probe_im * exit_change[0], axis=0))
    mode_re = patch_re * exit_change[0] + patch_im * exit_change[1]
    mode_im = patch_re * exit_change[1] - patch_im * exit_change[0]
    return (grad_re, grad_im, jnp.stack([mode_re, mode_im]), patch_re * patch_re + patch_im * patch_im)

def reference(object_field, probe_field, amplitudes, offsets, live_counts):
    probe_modes = probe_field.reshape(2, MODES, PATCH, PATCH)
    illum_one = lax.optimization_barrier(jnp.sum(probe_modes[0] ** 2 + probe_modes[1] ** 2, axis=0))
    forward = dft_tables(PATCH, 1.0)
    inverse = dft_tables(PATCH, -1.0)
    padded_rows = OBJ_ROWS + JITTER + PATCH
    padded = jnp.zeros((2, padded_rows, COLS), jnp.float32).at[:, JITTER:JITTER + OBJ_ROWS].set(object_field)
    position_ids = jnp.arange(POSITIONS, dtype=jnp.int32)
    weights = (position_ids % POS_DEV < live_counts[position_ids // POS_DEV]).astype(jnp.float32)
    zero_index = jnp.zeros((), jnp.int32)

    def visit(running, record):
        grad_grid, grad_probe, obj_norm = running
        amplitude, corner, alive_weight = record
        top_row = (corner[0] + JITTER).astype(jnp.int32)
        left_col = corner[1].astype(jnp.int32)
        obj_patch = lax.dynamic_slice(padded, (zero_index, top_row, left_col), (2, PATCH, PATCH))
        grad_re, grad_im, probe_part, norm_part = exit_update(obj_patch, probe_modes, amplitude, forward, inverse)
        contrib = jnp.stack([grad_re, grad_im, illum_one]) * alive_weight
        current = lax.dynamic_slice(grad_grid, (zero_index, top_row, left_col), (3, PATCH, PATCH))
        grad_grid = lax.dynamic_update_slice(grad_grid, current + contrib, (zero_index, top_row, left_col))
        return ((grad_grid, grad_probe + probe_part * alive_weight, obj_norm + norm_part * alive_weight), None)
    start_state = (jnp.zeros((3, padded_rows, COLS), jnp.float32), jnp.zeros((2, MODES, PATCH, PATCH), jnp.float32), jnp.zeros((PATCH, PATCH), jnp.float32))
    (grad_grid, grad_probe, obj_norm), _ = lax.scan(visit, start_state, (amplitudes, offsets, weights))
    grad_grid = grad_grid[:, JITTER:JITTER + OBJ_ROWS]
    obj_step = grad_grid[:2] / (grad_grid[2] + 1.0)
    probe_step = grad_probe / (obj_norm + 1.0)
    sum_uu = jnp.sum((obj_step[0] ** 2 + obj_step[1] ** 2) * grad_grid[2])
    sum_uc = jnp.sum(obj_step[0] * grad_grid[0] + obj_step[1] * grad_grid[1])
    sum_vv = jnp.sum((probe_step[0] ** 2 + probe_step[1] ** 2) * obj_norm)
    sum_vc = jnp.sum(probe_step * grad_probe)
    step_padded = jnp.zeros((2, padded_rows, COLS), jnp.float32).at[:, JITTER:JITTER + OBJ_ROWS].set(obj_step)

    def cross_terms(summed, record):
        corner, alive_weight = record
        top_row = (corner[0] + JITTER).astype(jnp.int32)
        left_col = corner[1].astype(jnp.int32)
        obj_patch = lax.dynamic_slice(padded, (zero_index, top_row, left_col), (2, PATCH, PATCH))
        step_patch = lax.dynamic_slice(step_padded, (zero_index, top_row, left_col), (2, PATCH, PATCH))
        cross_re = step_patch[0] * obj_patch[0] + step_patch[1] * obj_patch[1]
        cross_im = step_patch[0] * obj_patch[1] - step_patch[1] * obj_patch[0]
        return (summed + jnp.stack([cross_re, cross_im]) * alive_weight, None)
    cross_sum, _ = lax.scan(cross_terms, jnp.zeros((2, PATCH, PATCH), jnp.float32), (offsets, weights))
    conj_re = probe_modes[0] * probe_step[0] + probe_modes[1] * probe_step[1]
    conj_im = probe_modes[0] * probe_step[1] - probe_modes[1] * probe_step[0]
    sum_uv = jnp.sum(conj_re * cross_sum[0] - conj_im * cross_sum[1])
    diag_obj = 1.1 * sum_uu + 1e-06
    diag_probe = 1.1 * sum_vv + 1e-06
    determinant = diag_obj * diag_probe - sum_uv * sum_uv
    rate_obj = (sum_uc * diag_probe - sum_uv * sum_vc) / determinant
    rate_probe = (diag_obj * sum_vc - sum_uv * sum_uc) / determinant
    new_object = object_field + rate_obj * obj_step
    new_probe = probe_field + rate_probe * probe_step.reshape(2, MODES * PATCH, PATCH)
    return (new_object, new_probe)
```

```python
import functools
import math

import jax
import jax.numpy as jnp
import numpy as np
from jax import lax
from jax.experimental import pallas as pl
from jax.experimental.pallas import tpu as pltpu
from jax.sharding import PartitionSpec as P

MESH = pl.DeviceIdType.MESH
SPLIT = 4
JITTER = 8
STEP = 96
PATCH = 256
MODES = 4
STRIP = 24
LANES = 128
OWN = 512
WIN = 640
ROWS = JITTER + 2 * STEP + 72
ZTOP = 104
KROWS = 408
KCOLS = 384
F32 = jnp.float32
BF16 = jnp.bfloat16


def mult(value, of):
    return pl.multiple_of(value, of)


class Messages:
    def __init__(self, send, recv):
        self.send, self.recv, self.count, self.open = send, recv, 0, []

    def make(self, src, dst, scan, when=None):
        at = self.count
        self.count += 1
        copy = pltpu.make_async_remote_copy(
            src_ref=src,
            dst_ref=dst,
            send_sem=self.send.at[at],
            recv_sem=self.recv.at[at],
            device_id={"scan": scan},
            device_id_type=MESH,
        )
        self.open.append((copy, when))
        return copy

    def drain(self):
        for copy, when in self.open:
            if when is None:
                copy.wait_send()
            else:
                pl.when(when)(copy.wait_send)


def greet(peers):
    barrier = pltpu.get_barrier_semaphore()
    for peer in peers:
        pl.semaphore_signal(barrier, inc=1, device_id={"scan": peer}, device_id_type=MESH)
    pl.semaphore_wait(barrier, len(peers))


def gather_kernel(n, obj, meta, own, sib, metas, send, recv, msend, mrecv):
    me = lax.axis_index("scan")
    q = me % SPLIT
    core = me % 2
    first = me - q
    up = (me - SPLIT + n) % n
    down = (me + SPLIT) % n
    sibling = me + 1 - 2 * core
    msg = Messages(send, recv)
    peers = [(first + SPLIT * e + k + 2 * n) % n for e in (-2, -1, 1, 2) for k in range(SPLIT)]
    peers += [first + (q + k) % SPLIT for k in range(1, SPLIT)]
    greet(peers)

    def columns(quarter):
        return pl.ds(mult(768 * (quarter // 2) + OWN * (quarter % 2), LANES), OWN)

    def rows(start, size):
        return pl.ds(mult(start, 8), size)

    own[:, rows(JITTER + STRIP * q, STRIP), :] = obj[:, :, columns(q)]
    strips = []
    for k in range(1, SPLIT):
        there = (q + k) % SPLIT
        copy = msg.make(
            obj.at[:, :, columns(there)],
            own.at[:, rows(JITTER + STRIP * q, STRIP), :],
            first + there,
        )
        copy.start()
        strips.append(copy)
    metas[2 * SPLIT + q] = meta[...]
    meta_copies = []
    for e in (-1, 0, 1, 2):
        for k in range(SPLIT):
            if e == 0 and k == 0:
                continue
            there = (first + SPLIT * e + (q + k) % SPLIT + n) % n
            at = len(meta_copies)
            copy = pltpu.make_async_remote_copy(
                src_ref=meta,
                dst_ref=metas.at[(2 - e) * SPLIT + q],
                send_sem=msend.at[at],
                recv_sem=mrecv,
                device_id={"scan": there},
                device_id_type=MESH,
            )
            copy.start()
            meta_copies.append(copy)

    ahead = []
    for k in range(SPLIT):
        if k > 0:
            strips[k - 1].wait_recv()
        strip = (q - k + SPLIT) % SPLIT
        copy = msg.make(
            own.at[:, rows(JITTER + STRIP * strip, STRIP), :] if k else obj.at[:, :, columns(q)],
            own.at[:, rows(JITTER + STEP + STRIP * strip, STRIP), :],
            up,
        )
        copy.start()
        ahead.append(copy)
    tail = msg.make(own.at[:, rows(STEP, JITTER), :], own.at[:, rows(0, JITTER), :], down)
    tail.start()
    edge = pl.ds(mult(384 * (1 - core), LANES), LANES)

    def border(start, size):
        copy = msg.make(
            own.at[:, pl.ds(start, size), edge], sib.at[:, pl.ds(start, size), :], sibling
        )
        copy.start()
        return copy

    borders = [border(JITTER, STEP)]
    relays = []
    for k in range(SPLIT):
        ahead[k].wait_recv()
        strip = (q - k + SPLIT) % SPLIT
        low = jnp.minimum(strip, SPLIT - 2)
        copy = msg.make(
            own.at[:, rows(JITTER + STEP + STRIP * low, STRIP), :],
            own.at[:, rows(JITTER + 2 * STEP + STRIP * low, STRIP), :],
            up,
            when=strip != SPLIT - 1,
        )
        pl.when(strip != SPLIT - 1)(copy.start)
        relays.append((copy, strip != SPLIT - 1))
    borders.append(border(JITTER + STEP, STEP))
    tail.wait_recv()
    for copy, when in relays:
        pl.when(when)(copy.wait_recv)
    borders.append(border(0, JITTER))
    borders.append(border(JITTER + 2 * STEP, 72))
    for copy in borders:
        copy.wait_recv()
    pltpu.make_async_copy(metas.at[pl.ds(0, 15)], metas.at[pl.ds(0, 15)], mrecv).wait()
    msg.drain()
    for copy in meta_copies:
        copy.wait_send()


def gather(n, obj, meta):
    vmem = pl.BlockSpec(memory_space=pltpu.VMEM)
    return pl.pallas_call(
        functools.partial(gather_kernel, n),
        out_shape=(
            jax.ShapeDtypeStruct((2, ROWS, OWN), F32),
            jax.ShapeDtypeStruct((2, ROWS, LANES), F32),
            jax.ShapeDtypeStruct((4 * SPLIT, 8, LANES), jnp.int32),
        ),
        in_specs=[vmem] * 2,
        out_specs=[vmem] * 3,
        scratch_shapes=[
            pltpu.SemaphoreType.DMA((16,)),
            pltpu.SemaphoreType.DMA((16,)),
            pltpu.SemaphoreType.DMA((16,)),
            pltpu.SemaphoreType.DMA,
        ],
        compiler_params=pltpu.CompilerParams(collective_id=0, has_side_effects=True),
        name="gather_window",
    )(obj, meta)


def spread(n, kernel_pad, out, metas):
    me = lax.axis_index("scan")
    row = me // SPLIT
    parts = out.shape[0]
    out[...] = jnp.zeros_like(out)

    def one(at, carry):
        line, col = at // 16, at % 16
        slot = line * SPLIT + col // SPLIT
        place = col % SPLIT
        top = metas[slot, 2 * place]
        left = metas[slot, 2 * place + 1]
        there = row - 2 + line
        inside = jnp.logical_and(there >= 0, there < n // SPLIT)
        weight = jnp.where(jnp.logical_and(inside, place < metas[slot, 8]), 1.0, 0.0).astype(F32)
        start = mult(STRIP * (me % SPLIT) + STEP * (2 - line) - JITTER + ZTOP, 8)
        ahead = jnp.clip(STEP * there - top + JITTER, 0, 2 * JITTER)
        base = mult((STEP * col + 40) // LANES * LANES, LANES)
        shift = jnp.clip(left - base, 0, LANES)
        for part in range(parts):
            value = kernel_pad[part, pl.ds(start, STRIP + 2 * JITTER), :]
            value = pltpu.roll(value, (STRIP + 2 * JITTER - ahead) % (STRIP + 2 * JITTER), 0)[0:STRIP]
            value = pltpu.roll(value, shift, 1) * weight
            out[part, :, pl.ds(base, KCOLS)] += value
        return carry

    lax.fori_loop(0, 4 * 16, one, 0)


def position_kernel(
    n, metas, own, sib, probe, amps, cos, sin, g_own, g_sib, q_out, illum,
    win, grad, patch, wave, half, far, acc, kpad, ta, tb,
):
    me = lax.axis_index("scan")
    row = me // SPLIT
    q = me % SPLIT
    core = me % 2
    total = n * STRIP
    c, s = cos[...], sin[...]
    ta[0:256, 0:256] = c
    ta[0:256, 256:512] = s
    ta[256:512, 0:256] = -s
    ta[256:512, 256:512] = c
    tb[0:256, 0:256] = c
    tb[0:256, 256:512] = -s
    tb[256:512, 0:256] = s
    tb[256:512, 256:512] = c

    def valid(width):
        at = lax.broadcasted_iota(jnp.int32, (ROWS, width), 0) + (STEP * row - JITTER)
        return jnp.logical_and(at >= 0, at < total)

    own_at = mult(LANES * core, LANES)
    sib_at = mult(OWN * (1 - core), LANES)
    for part in range(2):
        win[part, 0:ROWS, pl.ds(own_at, OWN)] = jnp.where(valid(OWN), own[part], 0.0)
        win[part, 0:ROWS, pl.ds(sib_at, LANES)] = jnp.where(valid(LANES), sib[part], 0.0)
    win[:, ROWS:, :] = jnp.zeros((2, 8, WIN), F32)
    grad[...] = jnp.zeros_like(grad)
    acc[...] = jnp.zeros_like(acc)
    kpad[...] = jnp.zeros_like(kpad)
    light = jnp.zeros((PATCH, PATCH), F32)
    for m in range(MODES):
        light = light + (probe[0, m] * probe[0, m] + probe[1, m] * probe[1, m])
    kpad[0, ZTOP : ZTOP + PATCH, 0:PATCH] = light
    spread(n, kpad, illum, metas)

    chunk = 32
    chunks = PATCH // chunk
    slot = 2 * SPLIT + q

    def transform(left, right):
        for m in range(MODES):
            cols = slice(m * PATCH, (m + 1) * PATCH)
            y = jnp.dot(left[...], wave[:, cols], preferred_element_type=F32)
            half[cols, 0:PATCH] = y[0:PATCH].astype(BF16)
            half[cols, PATCH : 2 * PATCH] = y[PATCH : 2 * PATCH].astype(BF16)
        for m in range(MODES):
            cols = slice(m * PATCH, (m + 1) * PATCH)
            far[m] = jnp.dot(half[cols, :], right[...], preferred_element_type=F32)

    def visit(p, carry):
        down = metas[slot, 2 * p] - (STEP * row - JITTER)
        off = down % 8
        base = mult((STEP * p + 40) // LANES * LANES, LANES)
        shift = metas[slot, 2 * p + 1] - STEP * SPLIT * q - base

        def exits(i, carry):
            rows = pl.ds(mult(i * chunk, chunk), chunk)
            low = pl.ds(mult(PATCH + i * chunk, chunk), chunk)
            o = []
            for part in range(2):
                v = win[part, pl.ds(mult(down - off + i * chunk, 8), chunk + 8), pl.ds(base, KCOLS)]
                v = pltpu.roll(v, (chunk + 8 - off) % (chunk + 8), 0)[0:chunk]
                v = pltpu.roll(v, KCOLS - shift, 1)[:, 0:PATCH]
                patch[part, rows, :] = v
                o.append(v)
            for m in range(MODES):
                pr, pi = probe[0, m, rows, :], probe[1, m, rows, :]
                wave[rows, m * PATCH : (m + 1) * PATCH] = (pr * o[0] - pi * o[1]).astype(BF16)
                wave[low, m * PATCH : (m + 1) * PATCH] = (pr * o[1] + pi * o[0]).astype(BF16)
            return carry

        lax.fori_loop(0, chunks, exits, 0)
        transform(ta, tb)

        def changes(i, carry):
            rows = pl.ds(mult(i * chunk, chunk), chunk)
            low = pl.ds(mult(PATCH + i * chunk, chunk), chunk)
            bright = jnp.zeros((chunk, PATCH), F32)
            for m in range(MODES):
                fr, fi = far[m, rows, 0:PATCH], far[m, rows, PATCH : 2 * PATCH]
                bright = bright + (fr * fr + fi * fi)
            factor = amps[p, rows, :] / jnp.maximum(jnp.sqrt(bright), 0.5) - 1.0
            for m in range(MODES):
                fr, fi = far[m, rows, 0:PATCH], far[m, rows, PATCH : 2 * PATCH]
                wave[rows, m * PATCH : (m + 1) * PATCH] = (fr * factor).astype(BF16)
                wave[low, m * PATCH : (m + 1) * PATCH] = (fi * factor).astype(BF16)
            return carry

        lax.fori_loop(0, chunks, changes, 0)
        transform(tb, ta)

        def grads(i, carry):
            rows = pl.ds(mult(i * chunk, chunk), chunk)
            o_re, o_im = patch[0, rows, :], patch[1, rows, :]
            g_re = jnp.zeros((chunk, PATCH), F32)
            g_im = jnp.zeros((chunk, PATCH), F32)
            for m in range(MODES):
                pr, pi = probe[0, m, rows, :], probe[1, m, rows, :]
                cr, ci = far[m, rows, 0:PATCH], far[m, rows, PATCH : 2 * PATCH]
                g_re = g_re + (pr * cr + pi * ci)
                g_im = g_im + (pr * ci - pi * cr)
                acc[m, rows, :] += o_re * cr + o_im * ci
                acc[MODES + m, rows, :] += o_re * ci - o_im * cr
            acc[2 * MODES, rows, :] += o_re * o_re + o_im * o_im
            blank = jnp.zeros((chunk, KCOLS - PATCH), F32)
            below = jnp.zeros((8, KCOLS), F32)
            for part, g in enumerate((g_re, g_im)):
                v = pltpu.roll(jnp.concatenate([g, blank], 1), shift, 1)
                v = pltpu.roll(jnp.concatenate([v, below], 0), off, 0)
                grad[part, pl.ds(mult(down - off + i * chunk, 8), chunk + 8), pl.ds(base, KCOLS)] += v
            return carry

        lax.fori_loop(0, chunks, grads, 0)
        return carry

    lax.fori_loop(0, metas[slot, 8], visit, 0)

    for part in range(2):
        g_own[part] = jnp.where(valid(OWN), grad[part, 0:ROWS, pl.ds(own_at, OWN)], 0.0)
        g_sib[part] = jnp.where(valid(LANES), grad[part, 0:ROWS, pl.ds(sib_at, LANES)], 0.0)
    for band in range(PATCH // 8):
        y = (band // 2) % 8
        for side in range(2):
            x = (band // 16) * 4 + (band % 2) * 2 + side
            rows, cols = slice(8 * band, 8 * band + 8), slice(LANES * side, LANES * side + LANES)
            for k in range(2):
                for i, m in enumerate((2 * k, 2 * k + 1, MODES + 2 * k, MODES + 2 * k + 1, 8)):
                    q_out[k, x, y, i] = acc[m, rows, cols]


def positions(n, metas, own, sib, probe, amps, cos, sin):
    vmem = pl.BlockSpec(memory_space=pltpu.VMEM)
    return pl.pallas_call(
        functools.partial(position_kernel, n),
        out_shape=(
            jax.ShapeDtypeStruct((2, ROWS, OWN), F32),
            jax.ShapeDtypeStruct((2, ROWS, LANES), F32),
            jax.ShapeDtypeStruct((2, 8, 8, 5, 8, LANES), F32),
            jax.ShapeDtypeStruct((1, STRIP, 14 * LANES), F32),
        ),
        in_specs=[pl.BlockSpec(memory_space=pltpu.SMEM)] + [vmem] * 6,
        out_specs=[vmem] * 4,
        scratch_shapes=[
            pltpu.VMEM((2, ROWS + 8, WIN), F32),
            pltpu.VMEM((2, ROWS + 8, WIN), F32),
            pltpu.VMEM((2, PATCH, PATCH), F32),
            pltpu.VMEM((2 * PATCH, MODES * PATCH), BF16),
            pltpu.VMEM((MODES * PATCH, 2 * PATCH), BF16),
            pltpu.VMEM((MODES, PATCH, 2 * PATCH), F32),
            pltpu.VMEM((2 * MODES + 1, PATCH, PATCH), F32),
            pltpu.VMEM((1, KROWS, KCOLS), F32),
            pltpu.VMEM((2 * PATCH, 2 * PATCH), BF16),
            pltpu.VMEM((2 * PATCH, 2 * PATCH), BF16),
        ],
        name="positions",
    )(metas, own, sib, probe, amps, cos, sin)


def update_kernel(
    n, metas, g_own, g_sib, q_in, illum, obj, probe, new_obj, new_probe,
    gs, sib_in, t2_in, t1_in, t8_in, piece, q_sib, acc, minus_in, plus_in, y_in,
    p_tile, p_share, tile, dp, dp_in, kmine, ksib, kk, kpad, place, dobj, vec, vec1, vec2,
    send, recv, ysem, kysem, kxsem, v1sem, v2sem, bsend, dpsem, psem, lsem,
):
    me = lax.axis_index("scan")
    q = me % SPLIT
    core = me % 2
    first = me - q
    up = (me - SPLIT + n) % n
    down = (me + SPLIT) % n
    sibling = me + 1 - 2 * core
    side = 8
    x, y = me // (2 * side), (me // 2) % side
    msg = Messages(send, recv)

    def chip(at_x, at_y, at_core):
        return ((at_x % side) * side + at_y % side) * 2 + at_core

    peers = [chip(x + k, y, cc) for k in range(1, side) for cc in range(2)]
    peers += [chip(x, y + k, cc) for k in range(1, side) for cc in range(2)]
    peers += [sibling, up, down]
    greet(peers)

    to_sib = msg.make(g_sib, sib_in, sibling)
    to_sib.start()
    q_copy = msg.make(q_in.at[1 - core], q_sib, sibling)
    q_copy.start()

    band = (x // 4) * 16 + y * 2 + (x // 2) % 2
    lane = x % 2
    out_mode = x // 2
    out_band = (x % 2) * 16 + y * 2 + core
    load_tile = pltpu.make_async_copy(
        probe.at[:, pl.ds(2 * core, 2), pl.ds(mult(8 * band, 8), 8), pl.ds(mult(LANES * lane, LANES), LANES)],
        p_tile,
        lsem.at[0],
    )
    load_tile.start()
    load_share = pltpu.make_async_copy(
        probe.at[:, out_mode, pl.ds(mult(8 * out_band, 8), 8), :], p_share, lsem.at[1]
    )
    load_share.start()

    gs[...] = g_own[...]
    to_sib.wait_recv()
    edge = pl.ds(mult(384 * (1 - core), LANES), LANES)
    gs[:, :, edge] += sib_in[...]

    t2 = []
    for j in range(3):
        lo = JITTER + 2 * STEP + STRIP * j
        copy = msg.make(gs.at[:, pl.ds(lo, STRIP), :], t2_in.at[j], down)
        copy.start()
        t2.append(copy)
    t8 = msg.make(gs.at[:, pl.ds(0, JITTER), :], t8_in, up)
    t8.start()

    def send_t1(j):
        lo = JITTER + STEP + STRIP * j
        copy = msg.make(gs.at[:, pl.ds(lo, STRIP), :], t1_in.at[j], down)
        copy.start()
        return copy

    t1 = {3: send_t1(3)}

    q_copy.wait_recv()
    acc[...] = q_in[core] + q_sib[...]

    def send_minus(step):
        dest = (x - (4 - step) + side) % side
        copy = msg.make(acc.at[dest], minus_in.at[step], chip(x - 1 + side, y, core))
        copy.start()
        return copy

    def send_plus(step):
        dest = (x + 3 - step) % side
        copy = msg.make(acc.at[dest], plus_in.at[step], chip(x + 1, y, core))
        copy.start()
        return copy

    minus = [send_minus(0)]
    plus = [send_plus(0)]

    def x_step(step):
        minus[step].wait_recv()
        acc[(x - (3 - step) + side) % side] += minus_in[step]
        if step < 3:
            minus.append(send_minus(step + 1))
            plus[step].wait_recv()
            acc[(x + 2 - step) % side] += plus_in[step]
            if step < 2:
                plus.append(send_plus(step + 1))

    def t2_step(j):
        t2[j].wait_recv()
        lo = JITTER + STEP + STRIP * j
        gs[:, lo : lo + STRIP, :] += t2_in[j]
        t1[j] = send_t1(j)

    t2_step(0)
    x_step(0)
    t2_step(1)
    x_step(1)
    t2_step(2)
    x_step(2)
    x_step(3)

    y_copies = []
    for k in range(1, side):
        copy = pltpu.make_async_remote_copy(
            src_ref=acc.at[x, (y + k) % side],
            dst_ref=y_in.at[k - 1],
            send_sem=bsend.at[k - 1],
            recv_sem=ysem,
            device_id={"scan": chip(x, y + k, core)},
            device_id_type=MESH,
        )
        copy.start()
        y_copies.append(copy)
    pltpu.make_async_copy(y_in, y_in, ysem).wait()
    tile[...] = acc[x, y] + jnp.sum(y_in[...], 0)
    load_tile.wait()
    norm = tile[4]
    inverse = norm + 1.0
    k_re = jnp.zeros((8, LANES), F32)
    k_im = jnp.zeros((8, LANES), F32)
    s_vv = jnp.zeros((8, LANES), F32)
    s_vc = jnp.zeros((8, LANES), F32)
    for m in range(2):
        g_re, g_im = tile[m], tile[2 + m]
        d_re, d_im = g_re / inverse, g_im / inverse
        dp[m, 0] = d_re
        dp[m, 1] = d_im
        p_re, p_im = p_tile[0, m], p_tile[1, m]
        k_re = k_re + (p_re * d_re + p_im * d_im)
        k_im = k_im + (p_re * d_im - p_im * d_re)
        s_vv = s_vv + (d_re * d_re + d_im * d_im) * norm
        s_vc = s_vc + (d_re * g_re + d_im * g_im)
    kmine[0] = k_re
    kmine[1] = k_im
    k_copy = msg.make(kmine.at[1 - core], ksib, sibling)
    k_copy.start()

    dp_sends = []
    for m in range(2):
        dest = chip(2 * (2 * core + m) + x // 4, y, (x // 2) % 2)
        away = dest != me
        copy = pltpu.make_async_remote_copy(
            src_ref=dp.at[m],
            dst_ref=dp_in.at[lane],
            send_sem=bsend.at[21 + m],
            recv_sem=dpsem.at[lane],
            device_id={"scan": dest},
            device_id_type=MESH,
        )
        pl.when(away)(copy.start)
        dp_sends.append((copy, away))

        @pl.when(jnp.logical_not(away))
        def _():
            dp_in[lane] = dp[m]

    k_copy.wait_recv()
    kk[core, x, y] = kmine[core] + ksib[...]
    ky_copies = []
    for k in range(1, side):
        copy = pltpu.make_async_remote_copy(
            src_ref=kk.at[core, x, y],
            dst_ref=kk.at[core, x, y],
            send_sem=bsend.at[7 + k - 1],
            recv_sem=kysem,
            device_id={"scan": chip(x, y + k, core)},
            device_id_type=MESH,
        )
        copy.start()
        ky_copies.append(copy)

    pieces = []
    for j in (3, 0, 1, 2):
        t1[j].wait_recv()
        lo = JITTER + STRIP * j
        gs[:, lo : lo + STRIP, :] += t1_in[j]
        if j == 3:
            t8.wait_recv()
            gs[:, STEP : STEP + JITTER, :] += t8_in[...]
        slot = (j - q + SPLIT) % SPLIT
        copy = pltpu.make_async_remote_copy(
            src_ref=gs.at[:, pl.ds(lo, STRIP), :],
            dst_ref=piece.at[slot],
            send_sem=bsend.at[23 + j],
            recv_sem=psem.at[slot],
            device_id={"scan": first + j},
            device_id_type=MESH,
        )
        pl.when(q != j)(copy.start)
        pieces.append((copy, q != j))

    pltpu.make_async_copy(kk.at[0, 0, pl.ds(0, 7)], kk.at[0, 0, pl.ds(0, 7)], kysem).wait()
    kx_copies = []
    for k in range(1, side):
        copy = pltpu.make_async_remote_copy(
            src_ref=kk.at[core, x],
            dst_ref=kk.at[core, x],
            send_sem=bsend.at[14 + k - 1],
            recv_sem=kxsem,
            device_id={"scan": chip(x + k, y, core)},
            device_id_type=MESH,
        )
        copy.start()
        kx_copies.append(copy)
    piece[0] = gs[:, pl.ds(mult(JITTER + STRIP * q, 8), STRIP), :]

    pltpu.make_async_copy(kk.at[0, pl.ds(0, 7)], kk.at[0, pl.ds(0, 7)], kxsem).wait()
    ks_copy = msg.make(kk.at[core], kk.at[core], sibling)
    ks_copy.start()

    dobj[...] = jnp.zeros_like(dobj)
    for k in range(SPLIT):
        if k > 0:
            pltpu.make_async_copy(piece.at[k], piece.at[k], psem.at[k]).wait()
        source = (q - k + SPLIT) % SPLIT
        at = pl.ds(mult(768 * (source // 2) + OWN * (source % 2), LANES), OWN)
        dobj[:, :, at] += piece[k]
    bright = illum[0]
    g_re, g_im = dobj[0], dobj[1]
    o_re, o_im = obj[0], obj[1]
    d_re, d_im = g_re / (bright + 1.0), g_im / (bright + 1.0)
    s_uu = jnp.sum((d_re * d_re + d_im * d_im) * bright)
    s_uc = jnp.sum(d_re * g_re + d_im * g_im)
    dobj[0] = d_re
    dobj[1] = d_im

    ks_copy.wait_recv()
    kpad[...] = jnp.zeros_like(kpad)
    for at_band in range(PATCH // 8):
        for at_lane in range(2):
            xx = (at_band // 16) * 4 + (at_band % 2) * 2 + at_lane
            yy = (at_band // 2) % 8
            rows = slice(ZTOP + 8 * at_band, ZTOP + 8 * at_band + 8)
            cols = slice(LANES * at_lane, LANES * at_lane + LANES)
            kpad[0, rows, cols] = kk[0, xx, yy]
            kpad[1, rows, cols] = kk[1, xx, yy]
    spread(n, kpad, place, metas)
    d_re, d_im = dobj[0], dobj[1]
    s_uv = jnp.sum(
        place[0] * (d_re * o_re + d_im * o_im) - place[1] * (d_re * o_im - d_im * o_re)
    )

    at = lax.broadcasted_iota(jnp.int32, (8, LANES), 1)
    own_sums = jnp.zeros((8, LANES), F32)
    for i, value in enumerate((s_uu, s_uv, jnp.sum(s_vv), s_uc, jnp.sum(s_vc))):
        own_sums = jnp.where(at == i, value, own_sums)
    vec[...] = own_sums
    v1_copies = []
    for k in range(1, 2 * side):
        copy = pltpu.make_async_remote_copy(
            src_ref=vec,
            dst_ref=vec1.at[k - 1],
            send_sem=bsend.at[27 + k - 1],
            recv_sem=v1sem,
            device_id={"scan": chip(x, y + k // 2, (core + k) % 2)},
            device_id_type=MESH,
        )
        copy.start()
        v1_copies.append(copy)
    pltpu.make_async_copy(vec1, vec1, v1sem).wait()
    for copy in v1_copies:
        copy.wait_send()
    vec[...] = own_sums + jnp.sum(vec1[...], 0)
    v2_copies = []
    for k in range(1, side):
        copy = pltpu.make_async_remote_copy(
            src_ref=vec,
            dst_ref=vec2.at[k - 1],
            send_sem=bsend.at[42 + k - 1],
            recv_sem=v2sem,
            device_id={"scan": chip(x + k, y, core)},
            device_id_type=MESH,
        )
        copy.start()
        v2_copies.append(copy)
    load_share.wait()
    for at_lane in range(2):
        source = chip((x % 2) * 4 + core * 2 + at_lane, y, x // 4)
        arrived = pltpu.make_async_copy(dp_in.at[at_lane], dp_in.at[at_lane], dpsem.at[at_lane])
        pl.when(source != me)(arrived.wait)
    pltpu.make_async_copy(vec2, vec2, v2sem).wait()
    totals = vec[...] + jnp.sum(vec2[...], 0)
    uu, uv, vv, uc, vc = (totals[0:1, i : i + 1] for i in range(5))
    a = 1.1 * uu + 1e-06
    d = 1.1 * vv + 1e-06
    det = a * d - uv * uv
    rate_obj = (uc * d - uv * vc) / det
    rate_probe = (a * vc - uv * uc) / det
    for part in range(2):
        new_obj[part] = obj[part] + rate_obj * dobj[part]
        for at_lane in range(2):
            cols = slice(LANES * at_lane, LANES * at_lane + LANES)
            new_probe[part, :, cols] = p_share[part, :, cols] + rate_probe * dp_in[at_lane, part]

    msg.drain()
    for copy in y_copies + ky_copies + kx_copies + v2_copies:
        copy.wait_send()
    for copy, when in dp_sends + pieces:
        pl.when(when)(copy.wait_send)


def update(n, metas, g_own, g_sib, q_in, illum, obj, probe):
    vmem = pl.BlockSpec(memory_space=pltpu.VMEM)
    dma = pltpu.SemaphoreType.DMA
    columns = obj.shape[2]
    return pl.pallas_call(
        functools.partial(update_kernel, n),
        out_shape=(
            jax.ShapeDtypeStruct((2, STRIP, columns), F32),
            jax.ShapeDtypeStruct((2, 8, PATCH), F32),
        ),
        in_specs=[pl.BlockSpec(memory_space=pltpu.SMEM)] + [vmem] * 5 + [pl.BlockSpec(memory_space=pl.ANY)],
        out_specs=[vmem] * 2,
        scratch_shapes=[
            pltpu.VMEM((2, ROWS, OWN), F32),
            pltpu.VMEM((2, ROWS, LANES), F32),
            pltpu.VMEM((3, 2, STRIP, OWN), F32),
            pltpu.VMEM((4, 2, STRIP, OWN), F32),
            pltpu.VMEM((2, JITTER, OWN), F32),
            pltpu.VMEM((4, 2, STRIP, OWN), F32),
            pltpu.VMEM((8, 8, 5, 8, LANES), F32),
            pltpu.VMEM((8, 8, 5, 8, LANES), F32),
            pltpu.VMEM((4, 8, 5, 8, LANES), F32),
            pltpu.VMEM((3, 8, 5, 8, LANES), F32),
            pltpu.VMEM((7, 5, 8, LANES), F32),
            pltpu.VMEM((2, 2, 8, LANES), F32),
            pltpu.VMEM((2, 8, PATCH), F32),
            pltpu.VMEM((5, 8, LANES), F32),
            pltpu.VMEM((2, 2, 8, LANES), F32),
            pltpu.VMEM((2, 2, 8, LANES), F32),
            pltpu.VMEM((2, 8, LANES), F32),
            pltpu.VMEM((8, LANES), F32),
            pltpu.VMEM((2, 8, 8, 8, LANES), F32),
            pltpu.VMEM((2, KROWS, KCOLS), F32),
            pltpu.VMEM((2, STRIP, columns), F32),
            pltpu.VMEM((2, STRIP, columns), F32),
            pltpu.VMEM((8, LANES), F32),
            pltpu.VMEM((15, 8, LANES), F32),
            pltpu.VMEM((7, 8, LANES), F32),
            dma((24,)),
            dma((24,)),
            dma,
            dma,
            dma,
            dma,
            dma,
            dma((50,)),
            dma((2,)),
            dma((4,)),
            dma((2,)),
        ],
        compiler_params=pltpu.CompilerParams(collective_id=1, has_side_effects=True),
        name="update",
    )(metas, g_own, g_sib, q_in, illum, obj, probe)


def tables(length):
    numbers = np.arange(length, dtype=np.int64)
    angles = (numbers[:, None] * numbers[None, :] % length).astype(np.float32)
    angles = angles * np.float32(2.0 * math.pi / length)
    scaling = np.float32(1.0 / math.sqrt(length))
    return tuple(jnp.asarray(f(angles) * scaling).astype(BF16) for f in (np.cos, np.sin))


def on_device(n, object_field, probe_field, amplitudes, offsets, live_counts):
    probe = probe_field.reshape(2, MODES, PATCH, PATCH)
    meta = jnp.concatenate([offsets.reshape(-1), live_counts])
    meta = jnp.broadcast_to(jnp.pad(meta, (0, LANES - meta.shape[0]))[None], (8, LANES))
    cos, sin = tables(PATCH)
    own, sib, metas = gather(n, object_field, meta)
    metas = metas[:, 0, 0:16]
    g_own, g_sib, q_out, illum = positions(n, metas, own, sib, probe, amplitudes, cos, sin)
    return update(n, metas, g_own, g_sib, q_out, illum, object_field, probe)


def solution(mesh):
    groups_scan = ("groups", "scan")
    placed = (
        P(None, groups_scan, None),
        P(None, "groups", None),
        P(groups_scan, None, None),
        P(groups_scan, None),
        P(groups_scan),
    )
    return jax.shard_map(
        functools.partial(on_device, mesh.shape["scan"]),
        mesh=mesh,
        in_specs=placed,
        out_specs=(P(None, groups_scan, None), P(None, groups_scan, None)),
        check_vma=False,
    )
```

```python
import functools
import math

import jax
import jax.numpy as jnp
import numpy as np
from jax import lax
from jax.experimental import pallas as pl
from jax.experimental.pallas import tpu as pltpu
from jax.sharding import PartitionSpec as P

MESH = pl.DeviceIdType.MESH
SPLIT = 4
JITTER = 8
STEP = 96
PATCH = 256
MODES = 4
STRIP = 24
LANES = 128
OWN = 512
WIN = 640
ROWS = JITTER + 2 * STEP + 72
ZTOP = 104
KROWS = 408
KCOLS = 384
F32 = jnp.float32
BF16 = jnp.bfloat16


def mult(value, of):
    return pl.multiple_of(value, of)


class Messages:
    def __init__(self, send, recv):
        self.send, self.recv, self.count, self.open = send, recv, 0, []

    def make(self, src, dst, scan, when=None):
        at = self.count
        self.count += 1
        copy = pltpu.make_async_remote_copy(
            src_ref=src,
            dst_ref=dst,
            send_sem=self.send.at[at],
            recv_sem=self.recv.at[at],
            device_id={"scan": scan},
            device_id_type=MESH,
        )
        self.open.append((copy, when))
        return copy

    def drain(self):
        for copy, when in self.open:
            if when is None:
                copy.wait_send()
            else:
                pl.when(when)(copy.wait_send)


def greet(peers):
    barrier = pltpu.get_barrier_semaphore()
    for peer in peers:
        pl.semaphore_signal(barrier, inc=1, device_id={"scan": peer}, device_id_type=MESH)
    pl.semaphore_wait(barrier, len(peers))


def long_way(me, step):
    line, at, q = me // 16, (me // SPLIT) % 4, me % SPLIT
    scale = 16

    def device(at_line, at_row):
        return (at_line + 8) % 8 * scale + (at_row + 8) % 4 * SPLIT + q

    def turn(row):
        row = (row + 8) % 4
        return jnp.where(jnp.logical_or(row == 0, row == 3), 0, 1)

    relay = device(line, at - step)
    origin = device(line, at + step)
    target = device(line + step * turn(at), at - step)
    source = device(line - step * turn(at + step), at + step)
    return relay, origin, target, source


def gather_kernel(n, obj, meta, own, sib, metas, relay_in, send, recv, msend, mrecv):
    me = lax.axis_index("scan")
    q = me % SPLIT
    core = me % 2
    first = me - q
    up = (me - SPLIT + n) % n
    down = (me + SPLIT) % n
    sibling = me + 1 - 2 * core
    relay, origin, target, source = long_way(me, -1)
    msg = Messages(send, recv)
    peers = [(first + SPLIT * e + k + 2 * n) % n for e in (-2, -1, 1, 2) for k in range(SPLIT)]
    peers += [first + (q + k) % SPLIT for k in range(1, SPLIT)]
    peers += [relay, origin, target, source]
    greet(peers)

    def columns(quarter):
        return pl.ds(mult(768 * (quarter // 2) + OWN * (quarter % 2), LANES), OWN)

    def rows(start, size):
        return pl.ds(mult(start, 8), size)

    strips = []
    for k in range(1, SPLIT):
        there = (q + k) % SPLIT
        copy = msg.make(
            obj.at[:, :, columns(there)],
            own.at[:, rows(JITTER + STRIP * q, STRIP), :],
            first + there,
        )
        copy.start()
        strips.append(copy)

    ahead, relays = [], []
    for k in range(SPLIT):
        if k > 0:
            strips[k - 1].wait_recv()
        strip = (q - k + SPLIT) % SPLIT
        block = own.at[:, rows(JITTER + STRIP * strip, STRIP), :] if k else obj.at[:, :, columns(q)]
        copy = msg.make(block, own.at[:, rows(JITTER + STEP + STRIP * strip, STRIP), :], up)
        copy.start()
        ahead.append(copy)
        far = jnp.logical_or(strip == 1, strip == 2)
        copy = msg.make(block, relay_in.at[k], relay, when=far)
        pl.when(far)(copy.start)
        relays.append((copy, far))
        if k == 0:
            own[:, rows(JITTER + STRIP * q, STRIP), :] = obj[:, :, columns(q)]
            metas[2 * SPLIT + q] = meta[...]
            meta_copies = []
            for e in (-1, 0, 1, 2):
                for kk in range(SPLIT):
                    if e == 0 and kk == 0:
                        continue
                    there = (first + SPLIT * e + (q + kk) % SPLIT + n) % n
                    at = len(meta_copies)
                    copy = pltpu.make_async_remote_copy(
                        src_ref=meta,
                        dst_ref=metas.at[(2 - e) * SPLIT + q],
                        send_sem=msend.at[at],
                        recv_sem=mrecv,
                        device_id={"scan": there},
                        device_id_type=MESH,
                    )
                    copy.start()
                    meta_copies.append(copy)
    tail = msg.make(own.at[:, rows(STEP, JITTER), :], own.at[:, rows(0, JITTER), :], down)
    tail.start()
    edge = pl.ds(mult(384 * (1 - core), LANES), LANES)

    def border(start, size):
        copy = msg.make(
            own.at[:, pl.ds(start, size), edge], sib.at[:, pl.ds(start, size), :], sibling
        )
        copy.start()
        return copy

    borders = [border(JITTER, STEP)]
    finals = []
    for k in range(SPLIT):
        strip = (q - k + SPLIT) % SPLIT
        far = jnp.logical_or(strip == 1, strip == 2)
        near = strip == 0
        place = own.at[:, rows(JITTER + 2 * STEP + STRIP * jnp.minimum(strip, 2), STRIP), :]
        pl.when(far)(relays[k][0].wait_recv)
        copy = msg.make(relay_in.at[k], place, target, when=far)
        pl.when(far)(copy.start)
        finals.append((copy, far))
        ahead[k].wait_recv()
        block = own.at[:, rows(JITTER + STEP + STRIP * strip, STRIP), :]
        copy = msg.make(block, place, up, when=near)
        pl.when(near)(copy.start)
        finals.append((copy, near))
    borders.append(border(JITTER + STEP, STEP))
    tail.wait_recv()
    borders.append(border(0, JITTER))
    for copy, when in finals:
        pl.when(when)(copy.wait_recv)
    borders.append(border(JITTER + 2 * STEP, 72))
    for copy in borders:
        copy.wait_recv()
    pltpu.make_async_copy(metas.at[pl.ds(0, 15)], metas.at[pl.ds(0, 15)], mrecv).wait()
    msg.drain()
    for copy in meta_copies:
        copy.wait_send()


def gather(n, obj, meta):
    vmem = pl.BlockSpec(memory_space=pltpu.VMEM)
    return pl.pallas_call(
        functools.partial(gather_kernel, n),
        out_shape=(
            jax.ShapeDtypeStruct((2, ROWS, OWN), F32),
            jax.ShapeDtypeStruct((2, ROWS, LANES), F32),
            jax.ShapeDtypeStruct((4 * SPLIT, 8, LANES), jnp.int32),
        ),
        in_specs=[vmem] * 2,
        out_specs=[vmem] * 3,
        scratch_shapes=[
            pltpu.VMEM((SPLIT, 2, STRIP, OWN), F32),
            pltpu.SemaphoreType.DMA((24,)),
            pltpu.SemaphoreType.DMA((24,)),
            pltpu.SemaphoreType.DMA((16,)),
            pltpu.SemaphoreType.DMA,
        ],
        compiler_params=pltpu.CompilerParams(collective_id=0, has_side_effects=True),
        name="gather_window",
    )(obj, meta)


def spread(n, kernel_pad, out, metas, line):
    me = lax.axis_index("scan")
    q = me % SPLIT
    line = line + jnp.where(q == SPLIT - 1, 1, 0)
    there = me // SPLIT - 2 + line
    inside = jnp.logical_and(there >= 0, there < n // SPLIT)
    start = mult(STRIP * q + STEP * (2 - line) - JITTER + ZTOP, 8)
    parts = out.shape[0]
    tall = STRIP + 2 * JITTER

    def one(col, carry):
        slot = line * SPLIT + col // SPLIT
        place = col % SPLIT
        top = metas[slot, 2 * place]
        left = metas[slot, 2 * place + 1]
        weight = jnp.where(jnp.logical_and(inside, place < metas[slot, 8]), 1.0, 0.0).astype(F32)
        ahead = jnp.clip(STEP * there - top + JITTER, 0, 2 * JITTER)
        base = mult((STEP * col + 40) // LANES * LANES, LANES)
        shift = jnp.clip(left - base, 0, LANES)
        for part in range(parts):
            value = kernel_pad[part, pl.ds(start, tall), :]
            value = pltpu.roll(value, (tall - ahead) % tall, 0)[0:STRIP]
            value = pltpu.roll(value, shift, 1) * weight
            out[part, :, pl.ds(base, KCOLS)] += value
        return carry

    lax.fori_loop(0, 16, one, 0, unroll=4)


def position_kernel(
    n, metas, own, sib, probe, amps, cos, sin, g_own, g_sib, q_out, light_out,
    win, grad, patch, wave, half, far, acc, ta, tb,
):
    me = lax.axis_index("scan")
    row = me // SPLIT
    q = me % SPLIT
    core = me % 2
    total = n * STRIP
    c, s = cos[...], sin[...]
    ta[0:256, 0:256] = c
    ta[0:256, 256:512] = s
    ta[256:512, 0:256] = -s
    ta[256:512, 256:512] = c
    tb[0:256, 0:256] = c
    tb[0:256, 256:512] = -s
    tb[256:512, 0:256] = s
    tb[256:512, 256:512] = c

    def valid(width):
        at = lax.broadcasted_iota(jnp.int32, (ROWS, width), 0) + (STEP * row - JITTER)
        return jnp.logical_and(at >= 0, at < total)

    own_at = mult(LANES * core, LANES)
    sib_at = mult(OWN * (1 - core), LANES)
    for part in range(2):
        win[part, 0:ROWS, pl.ds(own_at, OWN)] = jnp.where(valid(OWN), own[part], 0.0)
        win[part, 0:ROWS, pl.ds(sib_at, LANES)] = jnp.where(valid(LANES), sib[part], 0.0)
    win[:, ROWS:, :] = jnp.zeros((2, 8, WIN), F32)
    grad[...] = jnp.zeros_like(grad)
    acc[...] = jnp.zeros_like(acc)
    light = jnp.zeros((PATCH, PATCH), F32)
    for m in range(MODES):
        light = light + (probe[0, m] * probe[0, m] + probe[1, m] * probe[1, m])
    light_out[...] = light

    chunk = 32
    chunks = PATCH // chunk
    slot = 2 * SPLIT + q

    def transform(left, right):
        for m in range(MODES):
            cols = slice(m * PATCH, (m + 1) * PATCH)
            y = jnp.dot(left[...], wave[:, cols], preferred_element_type=F32)
            half[cols, 0:PATCH] = y[0:PATCH].astype(BF16)
            half[cols, PATCH : 2 * PATCH] = y[PATCH : 2 * PATCH].astype(BF16)
        for m in range(MODES):
            cols = slice(m * PATCH, (m + 1) * PATCH)
            far[m] = jnp.dot(half[cols, :], right[...], preferred_element_type=F32)

    def visit(p, carry):
        down = metas[slot, 2 * p] - (STEP * row - JITTER)
        off = down % 8
        base = mult((STEP * p + 40) // LANES * LANES, LANES)
        shift = metas[slot, 2 * p + 1] - STEP * SPLIT * q - base

        def exits(i, carry):
            rows = pl.ds(mult(i * chunk, chunk), chunk)
            low = pl.ds(mult(PATCH + i * chunk, chunk), chunk)
            o = []
            for part in range(2):
                v = win[part, pl.ds(mult(down - off + i * chunk, 8), chunk + 8), pl.ds(base, KCOLS)]
                v = pltpu.roll(v, (chunk + 8 - off) % (chunk + 8), 0)[0:chunk]
                v = pltpu.roll(v, KCOLS - shift, 1)[:, 0:PATCH]
                patch[part, rows, :] = v
                o.append(v)
            for m in range(MODES):
                pr, pi = probe[0, m, rows, :], probe[1, m, rows, :]
                wave[rows, m * PATCH : (m + 1) * PATCH] = (pr * o[0] - pi * o[1]).astype(BF16)
                wave[low, m * PATCH : (m + 1) * PATCH] = (pr * o[1] + pi * o[0]).astype(BF16)
            return carry

        lax.fori_loop(0, chunks, exits, 0)
        transform(ta, tb)

        def changes(i, carry):
            rows = pl.ds(mult(i * chunk, chunk), chunk)
            low = pl.ds(mult(PATCH + i * chunk, chunk), chunk)
            bright = jnp.zeros((chunk, PATCH), F32)
            for m in range(MODES):
                fr, fi = far[m, rows, 0:PATCH], far[m, rows, PATCH : 2 * PATCH]
                bright = bright + (fr * fr + fi * fi)
            factor = amps[p, rows, :] / jnp.maximum(jnp.sqrt(bright), 0.5) - 1.0
            for m in range(MODES):
                fr, fi = far[m, rows, 0:PATCH], far[m, rows, PATCH : 2 * PATCH]
                wave[rows, m * PATCH : (m + 1) * PATCH] = (fr * factor).astype(BF16)
                wave[low, m * PATCH : (m + 1) * PATCH] = (fi * factor).astype(BF16)
            return carry

        lax.fori_loop(0, chunks, changes, 0)
        transform(tb, ta)

        def grads(i, carry):
            rows = pl.ds(mult(i * chunk, chunk), chunk)
            o_re, o_im = patch[0, rows, :], patch[1, rows, :]
            g_re = jnp.zeros((chunk, PATCH), F32)
            g_im = jnp.zeros((chunk, PATCH), F32)
            for m in range(MODES):
                pr, pi = probe[0, m, rows, :], probe[1, m, rows, :]
                cr, ci = far[m, rows, 0:PATCH], far[m, rows, PATCH : 2 * PATCH]
                g_re = g_re + (pr * cr + pi * ci)
                g_im = g_im + (pr * ci - pi * cr)
                acc[m, rows, :] += o_re * cr + o_im * ci
                acc[MODES + m, rows, :] += o_re * ci - o_im * cr
            acc[2 * MODES, rows, :] += o_re * o_re + o_im * o_im
            blank = jnp.zeros((chunk, KCOLS - PATCH), F32)
            below = jnp.zeros((8, KCOLS), F32)
            for part, g in enumerate((g_re, g_im)):
                v = pltpu.roll(jnp.concatenate([g, blank], 1), shift, 1)
                v = pltpu.roll(jnp.concatenate([v, below], 0), off, 0)
                grad[part, pl.ds(mult(down - off + i * chunk, 8), chunk + 8), pl.ds(base, KCOLS)] += v
            return carry

        lax.fori_loop(0, chunks, grads, 0)
        return carry

    lax.fori_loop(0, metas[slot, 8], visit, 0)

    for part in range(2):
        g_own[part] = jnp.where(valid(OWN), grad[part, 0:ROWS, pl.ds(own_at, OWN)], 0.0)
        g_sib[part] = jnp.where(valid(LANES), grad[part, 0:ROWS, pl.ds(sib_at, LANES)], 0.0)
    for band in range(PATCH // 8):
        y = (band // 2) % 8
        for side in range(2):
            x = (band // 16) * 4 + (band % 2) * 2 + side
            rows, cols = slice(8 * band, 8 * band + 8), slice(LANES * side, LANES * side + LANES)
            for k in range(2):
                for i, m in enumerate((2 * k, 2 * k + 1, MODES + 2 * k, MODES + 2 * k + 1, 8)):
                    q_out[k, x, y, i] = acc[m, rows, cols]


def positions(n, metas, own, sib, probe, amps, cos, sin):
    vmem = pl.BlockSpec(memory_space=pltpu.VMEM)
    return pl.pallas_call(
        functools.partial(position_kernel, n),
        out_shape=(
            jax.ShapeDtypeStruct((2, ROWS, OWN), F32),
            jax.ShapeDtypeStruct((2, ROWS, LANES), F32),
            jax.ShapeDtypeStruct((2, 8, 8, 5, 8, LANES), F32),
            jax.ShapeDtypeStruct((PATCH, PATCH), F32),
        ),
        in_specs=[pl.BlockSpec(memory_space=pltpu.SMEM)] + [vmem] * 6,
        out_specs=[vmem] * 4,
        scratch_shapes=[
            pltpu.VMEM((2, ROWS + 8, WIN), F32),
            pltpu.VMEM((2, ROWS + 8, WIN), F32),
            pltpu.VMEM((2, PATCH, PATCH), F32),
            pltpu.VMEM((2 * PATCH, MODES * PATCH), BF16),
            pltpu.VMEM((MODES * PATCH, 2 * PATCH), BF16),
            pltpu.VMEM((MODES, PATCH, 2 * PATCH), F32),
            pltpu.VMEM((2 * MODES + 1, PATCH, PATCH), F32),
            pltpu.VMEM((2 * PATCH, 2 * PATCH), BF16),
            pltpu.VMEM((2 * PATCH, 2 * PATCH), BF16),
        ],
        name="positions",
    )(metas, own, sib, probe, amps, cos, sin)


def update_kernel(
    n, metas, g_own, g_sib, q_in, light, obj, probe, new_obj, new_probe,
    gs, sib_in, t2_in, t1_in, t8_in, relay_in, far_in, piece, q_sib, acc, minus_in, plus_in, y_in,
    p_tile, p_share, tile, dp, dp_in, kmine, ksib, kk, kpad, illum, place, dobj, vec, vec1, vec2,
    send, recv, ysem, kysem, kxsem, v1sem, v2sem, bsend, dpsem, psem, lsem,
):
    me = lax.axis_index("scan")
    q = me % SPLIT
    core = me % 2
    first = me - q
    up = (me - SPLIT + n) % n
    down = (me + SPLIT) % n
    sibling = me + 1 - 2 * core
    side = 8
    x, y = me // (2 * side), (me // 2) % side
    msg = Messages(send, recv)

    def chip(at_x, at_y, at_core):
        return ((at_x % side) * side + at_y % side) * 2 + at_core

    peers = [chip(x + k, y, cc) for k in range(1, side) for cc in range(2)]
    peers += [chip(x, y + k, cc) for k in range(1, side) for cc in range(2)]
    relay, origin, target, source = long_way(me, 1)
    peers += [sibling, up, down, relay, origin, target, source]
    greet(peers)

    to_sib = msg.make(g_sib, sib_in, sibling)
    to_sib.start()
    chunks = [(x + k) % side for k in (4, 5, 3, 6, 2, 7, 1, 0)]
    q_copies = []
    for at in chunks:
        copy = msg.make(q_in.at[1 - core, at], q_sib.at[at], sibling)
        copy.start()
        q_copies.append(copy)

    band = (x // 4) * 16 + y * 2 + (x // 2) % 2
    lane = x % 2
    out_mode = x // 2
    out_band = (x % 2) * 16 + y * 2 + core
    load_tile = pltpu.make_async_copy(
        probe.at[:, pl.ds(2 * core, 2), pl.ds(mult(8 * band, 8), 8), pl.ds(mult(LANES * lane, LANES), LANES)],
        p_tile,
        lsem.at[0],
    )
    load_tile.start()
    load_share = pltpu.make_async_copy(
        probe.at[:, out_mode, pl.ds(mult(8 * out_band, 8), 8), :], p_share, lsem.at[1]
    )
    load_share.start()

    gs[...] = g_own[...]
    to_sib.wait_recv()
    edge = pl.ds(mult(384 * (1 - core), LANES), LANES)
    gs[:, :, edge] += sib_in[...]

    def sums(start):
        return gs.at[:, pl.ds(start, STRIP), :]

    far_out = []
    for j in (1, 2):
        copy = msg.make(sums(JITTER + 2 * STEP + STRIP * j), relay_in.at[j - 1], relay)
        copy.start()
        far_out.append(copy)
    t2 = msg.make(sums(JITTER + 2 * STEP), t2_in, down)
    t2.start()
    t8 = msg.make(gs.at[:, pl.ds(0, JITTER), :], t8_in, up)
    t8.start()

    def send_t1(j):
        copy = msg.make(sums(JITTER + STEP + STRIP * j), t1_in.at[j], down)
        copy.start()
        return copy

    t1 = {j: send_t1(j) for j in (1, 2, 3)}

    def add_sibling(i):
        q_copies[i].wait_recv()
        acc[chunks[i]] = q_in[core, chunks[i]] + q_sib[chunks[i]]

    half = side // 2

    def send_chain(way, i):
        which = (i % 2 if way < 0 else 1 - i % 2) * half
        reach = (4 if i % 2 == 0 else 3) - i // 2
        dest = (x + way * reach + side) % side
        copy = msg.make(
            acc.at[dest, pl.ds(which, half)],
            (minus_in if way < 0 else plus_in).at[i],
            chip(x + way + side, y, core),
        )
        copy.start()
        return copy

    chains = {}
    add_sibling(0)
    chains[-1, 0], chains[1, 0] = send_chain(-1, 0), send_chain(1, 0)
    add_sibling(1)
    chains[-1, 1] = send_chain(-1, 1)
    add_sibling(2)
    chains[1, 1] = send_chain(1, 1)
    for i in range(3, 8):
        add_sibling(i)

    def x_step(i):
        for way, arrived in ((-1, minus_in), (1, plus_in)):
            which = (i % 2 if way < 0 else 1 - i % 2) * half
            reach = (4 if i % 2 == 0 else 3) - 1 - i // 2
            dest = (x + way * reach + side) % side
            chains[way, i].wait_recv()
            acc[dest, which : which + half] += arrived[i]
            if reach > 0:
                chains[way, i + 2] = send_chain(way, i + 2)

    kpad[...] = jnp.zeros_like(kpad)
    illum[...] = jnp.zeros_like(illum)
    kpad[0, ZTOP : ZTOP + PATCH, 0:PATCH] = light[...]
    dim = kpad.at[pl.ds(0, 1)]
    x_step(0)
    t2.wait_recv()
    gs[:, JITTER + STEP : JITTER + STEP + STRIP, :] += t2_in[...]
    t1[0] = send_t1(0)
    far_final = []
    for j in range(2):
        far_out[j].wait_recv()
        copy = msg.make(relay_in.at[j], far_in.at[j], target)
        copy.start()
        far_final.append(copy)
    x_step(1)
    spread(n, dim, illum, metas, 0)
    x_step(2)
    spread(n, dim, illum, metas, 1)
    x_step(3)
    spread(n, dim, illum, metas, 2)
    x_step(4)
    x_step(5)
    x_step(6)

    y_copies = []
    for k in range(1, side):
        copy = pltpu.make_async_remote_copy(
            src_ref=acc.at[x, (y + k) % side],
            dst_ref=y_in.at[k - 1],
            send_sem=bsend.at[k - 1],
            recv_sem=ysem,
            device_id={"scan": chip(x, y + k, core)},
            device_id_type=MESH,
        )
        copy.start()
        y_copies.append(copy)
    pltpu.make_async_copy(y_in, y_in, ysem).wait()
    tile[...] = acc[x, y] + jnp.sum(y_in[...], 0)
    load_tile.wait()
    norm = tile[4]
    inverse = norm + 1.0
    k_re = jnp.zeros((8, LANES), F32)
    k_im = jnp.zeros((8, LANES), F32)
    s_vv = jnp.zeros((8, LANES), F32)
    s_vc = jnp.zeros((8, LANES), F32)
    for m in range(2):
        g_re, g_im = tile[m], tile[2 + m]
        d_re, d_im = g_re / inverse, g_im / inverse
        dp[m, 0] = d_re
        dp[m, 1] = d_im
        p_re, p_im = p_tile[0, m], p_tile[1, m]
        k_re = k_re + (p_re * d_re + p_im * d_im)
        k_im = k_im + (p_re * d_im - p_im * d_re)
        s_vv = s_vv + (d_re * d_re + d_im * d_im) * norm
        s_vc = s_vc + (d_re * g_re + d_im * g_im)
    kmine[0] = k_re
    kmine[1] = k_im
    k_copy = msg.make(kmine.at[1 - core], ksib, sibling)
    k_copy.start()

    dp_sends = []
    for m in range(2):
        dest = chip(2 * (2 * core + m) + x // 4, y, (x // 2) % 2)
        away = dest != me
        copy = pltpu.make_async_remote_copy(
            src_ref=dp.at[m],
            dst_ref=dp_in.at[lane],
            send_sem=bsend.at[21 + m],
            recv_sem=dpsem.at[lane],
            device_id={"scan": dest},
            device_id_type=MESH,
        )
        pl.when(away)(copy.start)
        dp_sends.append((copy, away))

        @pl.when(jnp.logical_not(away))
        def _():
            dp_in[lane] = dp[m]

    k_copy.wait_recv()
    kk[core, x, y] = kmine[core] + ksib[...]
    ky_copies = []
    for k in range(1, side):
        copy = pltpu.make_async_remote_copy(
            src_ref=kk.at[core, x, y],
            dst_ref=kk.at[core, x, y],
            send_sem=bsend.at[7 + k - 1],
            recv_sem=kysem,
            device_id={"scan": chip(x, y + k, core)},
            device_id_type=MESH,
        )
        copy.start()
        ky_copies.append(copy)

    pieces = []
    for j in (3, 1, 2, 0):
        t1[j].wait_recv()
        lo = JITTER + STRIP * j
        gs[:, lo : lo + STRIP, :] += t1_in[j]
        if j == 3:
            t8.wait_recv()
            gs[:, STEP : STEP + JITTER, :] += t8_in[...]
        if j in (1, 2):
            far_final[j - 1].wait_recv()
            gs[:, lo : lo + STRIP, :] += far_in[j - 1]
        slot = (j - q + SPLIT) % SPLIT
        copy = pltpu.make_async_remote_copy(
            src_ref=gs.at[:, pl.ds(lo, STRIP), :],
            dst_ref=piece.at[slot],
            send_sem=bsend.at[23 + j],
            recv_sem=psem.at[slot],
            device_id={"scan": first + j},
            device_id_type=MESH,
        )
        pl.when(q != j)(copy.start)
        pieces.append((copy, q != j))

    pltpu.make_async_copy(kk.at[0, 0, pl.ds(0, 7)], kk.at[0, 0, pl.ds(0, 7)], kysem).wait()
    kx_copies = []
    for k in range(1, side):
        copy = pltpu.make_async_remote_copy(
            src_ref=kk.at[core, x],
            dst_ref=kk.at[core, x],
            send_sem=bsend.at[14 + k - 1],
            recv_sem=kxsem,
            device_id={"scan": chip(x + k, y, core)},
            device_id_type=MESH,
        )
        copy.start()
        kx_copies.append(copy)
    piece[0] = gs[:, pl.ds(mult(JITTER + STRIP * q, 8), STRIP), :]

    pltpu.make_async_copy(kk.at[0, pl.ds(0, 7)], kk.at[0, pl.ds(0, 7)], kxsem).wait()
    ks_copy = msg.make(kk.at[core], kk.at[core], sibling)
    ks_copy.start()

    dobj[...] = jnp.zeros_like(dobj)
    for k in range(SPLIT):
        if k > 0:
            pltpu.make_async_copy(piece.at[k], piece.at[k], psem.at[k]).wait()
        source = (q - k + SPLIT) % SPLIT
        at = pl.ds(mult(768 * (source // 2) + OWN * (source % 2), LANES), OWN)
        dobj[:, :, at] += piece[k]
    bright = illum[0]
    g_re, g_im = dobj[0], dobj[1]
    o_re, o_im = obj[0], obj[1]
    d_re, d_im = g_re / (bright + 1.0), g_im / (bright + 1.0)
    s_uu = jnp.sum((d_re * d_re + d_im * d_im) * bright)
    s_uc = jnp.sum(d_re * g_re + d_im * g_im)
    dobj[0] = d_re
    dobj[1] = d_im

    place[...] = jnp.zeros_like(place)
    ks_copy.wait_recv()
    for at_band in range(PATCH // 8):
        for at_lane in range(2):
            xx = (at_band // 16) * 4 + (at_band % 2) * 2 + at_lane
            yy = (at_band // 2) % 8
            rows = slice(ZTOP + 8 * at_band, ZTOP + 8 * at_band + 8)
            cols = slice(LANES * at_lane, LANES * at_lane + LANES)
            kpad[0, rows, cols] = kk[0, xx, yy]
            kpad[1, rows, cols] = kk[1, xx, yy]
    for line in range(3):
        spread(n, kpad, place, metas, line)
    d_re, d_im = dobj[0], dobj[1]
    s_uv = jnp.sum(
        place[0] * (d_re * o_re + d_im * o_im) - place[1] * (d_re * o_im - d_im * o_re)
    )

    at = lax.broadcasted_iota(jnp.int32, (8, LANES), 1)
    own_sums = jnp.zeros((8, LANES), F32)
    for i, value in enumerate((s_uu, s_uv, jnp.sum(s_vv), s_uc, jnp.sum(s_vc))):
        own_sums = jnp.where(at == i, value, own_sums)
    vec[...] = own_sums
    v1_copies = []
    for k in range(1, 2 * side):
        copy = pltpu.make_async_remote_copy(
            src_ref=vec,
            dst_ref=vec1.at[k - 1],
            send_sem=bsend.at[27 + k - 1],
            recv_sem=v1sem,
            device_id={"scan": chip(x, y + k // 2, (core + k) % 2)},
            device_id_type=MESH,
        )
        copy.start()
        v1_copies.append(copy)
    pltpu.make_async_copy(vec1, vec1, v1sem).wait()
    for copy in v1_copies:
        copy.wait_send()
    vec[...] = own_sums + jnp.sum(vec1[...], 0)
    v2_copies = []
    for k in range(1, side):
        copy = pltpu.make_async_remote_copy(
            src_ref=vec,
            dst_ref=vec2.at[k - 1],
            send_sem=bsend.at[42 + k - 1],
            recv_sem=v2sem,
            device_id={"scan": chip(x + k, y, core)},
            device_id_type=MESH,
        )
        copy.start()
        v2_copies.append(copy)
    load_share.wait()
    for at_lane in range(2):
        source = chip((x % 2) * 4 + core * 2 + at_lane, y, x // 4)
        arrived = pltpu.make_async_copy(dp_in.at[at_lane], dp_in.at[at_lane], dpsem.at[at_lane])
        pl.when(source != me)(arrived.wait)
    pltpu.make_async_copy(vec2, vec2, v2sem).wait()
    totals = vec[...] + jnp.sum(vec2[...], 0)
    uu, uv, vv, uc, vc = (totals[0:1, i : i + 1] for i in range(5))
    a = 1.1 * uu + 1e-06
    d = 1.1 * vv + 1e-06
    det = a * d - uv * uv
    rate_obj = (uc * d - uv * vc) / det
    rate_probe = (a * vc - uv * uc) / det
    for part in range(2):
        new_obj[part] = obj[part] + rate_obj * dobj[part]
        for at_lane in range(2):
            cols = slice(LANES * at_lane, LANES * at_lane + LANES)
            new_probe[part, :, cols] = p_share[part, :, cols] + rate_probe * dp_in[at_lane, part]

    msg.drain()
    for copy in y_copies + ky_copies + kx_copies + v2_copies:
        copy.wait_send()
    for copy, when in dp_sends + pieces:
        pl.when(when)(copy.wait_send)


def update(n, metas, g_own, g_sib, q_in, light, obj, probe):
    vmem = pl.BlockSpec(memory_space=pltpu.VMEM)
    dma = pltpu.SemaphoreType.DMA
    columns = obj.shape[2]
    return pl.pallas_call(
        functools.partial(update_kernel, n),
        out_shape=(
            jax.ShapeDtypeStruct((2, STRIP, columns), F32),
            jax.ShapeDtypeStruct((2, 8, PATCH), F32),
        ),
        in_specs=[pl.BlockSpec(memory_space=pltpu.SMEM)] + [vmem] * 5 + [pl.BlockSpec(memory_space=pl.ANY)],
        out_specs=[vmem] * 2,
        scratch_shapes=[
            pltpu.VMEM((2, ROWS, OWN), F32),
            pltpu.VMEM((2, ROWS, LANES), F32),
            pltpu.VMEM((2, STRIP, OWN), F32),
            pltpu.VMEM((4, 2, STRIP, OWN), F32),
            pltpu.VMEM((2, JITTER, OWN), F32),
            pltpu.VMEM((2, 2, STRIP, OWN), F32),
            pltpu.VMEM((2, 2, STRIP, OWN), F32),
            pltpu.VMEM((4, 2, STRIP, OWN), F32),
            pltpu.VMEM((8, 8, 5, 8, LANES), F32),
            pltpu.VMEM((8, 8, 5, 8, LANES), F32),
            pltpu.VMEM((7, 4, 5, 8, LANES), F32),
            pltpu.VMEM((7, 4, 5, 8, LANES), F32),
            pltpu.VMEM((7, 5, 8, LANES), F32),
            pltpu.VMEM((2, 2, 8, LANES), F32),
            pltpu.VMEM((2, 8, PATCH), F32),
            pltpu.VMEM((5, 8, LANES), F32),
            pltpu.VMEM((2, 2, 8, LANES), F32),
            pltpu.VMEM((2, 2, 8, LANES), F32),
            pltpu.VMEM((2, 8, LANES), F32),
            pltpu.VMEM((8, LANES), F32),
            pltpu.VMEM((2, 8, 8, 8, LANES), F32),
            pltpu.VMEM((2, KROWS, KCOLS), F32),
            pltpu.VMEM((1, STRIP, columns), F32),
            pltpu.VMEM((2, STRIP, columns), F32),
            pltpu.VMEM((2, STRIP, columns), F32),
            pltpu.VMEM((8, LANES), F32),
            pltpu.VMEM((15, 8, LANES), F32),
            pltpu.VMEM((7, 8, LANES), F32),
            dma((48,)),
            dma((48,)),
            dma,
            dma,
            dma,
            dma,
            dma,
            dma((50,)),
            dma((2,)),
            dma((4,)),
            dma((2,)),
        ],
        compiler_params=pltpu.CompilerParams(collective_id=1, has_side_effects=True),
        name="update",
    )(metas, g_own, g_sib, q_in, light, obj, probe)


def tables(length):
    numbers = np.arange(length, dtype=np.int64)
    angles = (numbers[:, None] * numbers[None, :] % length).astype(np.float32)
    angles = angles * np.float32(2.0 * math.pi / length)
    scaling = np.float32(1.0 / math.sqrt(length))
    return tuple(jnp.asarray(f(angles) * scaling).astype(BF16) for f in (np.cos, np.sin))


def on_device(n, object_field, probe_field, amplitudes, offsets, live_counts):
    probe = probe_field.reshape(2, MODES, PATCH, PATCH)
    meta = jnp.concatenate([offsets.reshape(-1), live_counts])
    meta = jnp.broadcast_to(jnp.pad(meta, (0, LANES - meta.shape[0]))[None], (8, LANES))
    cos, sin = tables(PATCH)
    own, sib, metas = gather(n, object_field, meta)
    metas = metas[:, 0, 0:16]
    g_own, g_sib, q_out, light = positions(n, metas, own, sib, probe, amplitudes, cos, sin)
    return update(n, metas, g_own, g_sib, q_out, light, object_field, probe)


def solution(mesh):
    groups_scan = ("groups", "scan")
    placed = (
        P(None, groups_scan, None),
        P(None, "groups", None),
        P(groups_scan, None, None),
        P(groups_scan, None),
        P(groups_scan),
    )
    return jax.shard_map(
        functools.partial(on_device, mesh.shape["scan"]),
        mesh=mesh,
        in_specs=placed,
        out_specs=(P(None, groups_scan, None), P(None, groups_scan, None)),
        check_vma=False,
    )
```

```python
import functools
import math

import jax
import jax.numpy as jnp
import numpy as np
from jax import lax
from jax.experimental import pallas as pl
from jax.experimental.pallas import tpu as pltpu
from jax.sharding import PartitionSpec as P

MESH = pl.DeviceIdType.MESH
SPLIT = 4
JITTER = 8
STEP = 96
PATCH = 256
MODES = 4
STRIP = 24
LANES = 128
OWN = 512
WIN = 640
ROWS = JITTER + 2 * STEP + 72
ZTOP = 104
KROWS = 408
KCOLS = 384
F32 = jnp.float32
BF16 = jnp.bfloat16


def mult(value, of):
    return pl.multiple_of(value, of)


class Messages:
    def __init__(self, send, recv):
        self.send, self.recv, self.count, self.open = send, recv, 0, []

    def make(self, src, dst, scan, when=None):
        at = self.count
        self.count += 1
        copy = pltpu.make_async_remote_copy(
            src_ref=src,
            dst_ref=dst,
            send_sem=self.send.at[at],
            recv_sem=self.recv.at[at],
            device_id={"scan": scan},
            device_id_type=MESH,
        )
        self.open.append((copy, when))
        return copy

    def drain(self):
        for copy, when in self.open:
            if when is None:
                copy.wait_send()
            else:
                pl.when(when)(copy.wait_send)
        self.open = []


def greet(peers):
    barrier = pltpu.get_barrier_semaphore()
    for peer in peers:
        pl.semaphore_signal(barrier, inc=1, device_id={"scan": peer}, device_id_type=MESH)
    pl.semaphore_wait(barrier, len(peers))


def long_way(me, step):
    line, at, q = me // 16, (me // SPLIT) % 4, me % SPLIT
    scale = 16

    def device(at_line, at_row):
        return (at_line + 8) % 8 * scale + (at_row + 8) % 4 * SPLIT + q

    def turn(row):
        row = (row + 8) % 4
        return jnp.where(jnp.logical_or(row == 0, row == 3), 0, 1)

    relay = device(line, at - step)
    origin = device(line, at + step)
    target = device(line + step * turn(at), at - step)
    source = device(line - step * turn(at + step), at + step)
    return relay, origin, target, source


def spread(n, kernel_pad, out, metas, line):
    me = lax.axis_index("scan")
    q = me % SPLIT
    line = line + jnp.where(q == SPLIT - 1, 1, 0)
    there = me // SPLIT - 2 + line
    inside = jnp.logical_and(there >= 0, there < n // SPLIT)
    start = mult(STRIP * q + STEP * (2 - line) - JITTER + ZTOP, 8)
    parts = out.shape[0]
    tall = STRIP + 2 * JITTER

    def one(col, carry):
        slot = line * SPLIT + col // SPLIT
        place = col % SPLIT
        top = metas[slot, 0, 2 * place]
        left = metas[slot, 0, 2 * place + 1]
        weight = jnp.where(jnp.logical_and(inside, place < metas[slot, 0, 8]), 1.0, 0.0).astype(F32)
        ahead = jnp.clip(STEP * there - top + JITTER, 0, 2 * JITTER)
        base = mult((STEP * col + 40) // LANES * LANES, LANES)
        shift = jnp.clip(left - base, 0, LANES)
        for part in range(parts):
            value = kernel_pad[part, pl.ds(start, tall), :]
            value = pltpu.roll(value, (tall - ahead) % tall, 0)[0:STRIP]
            value = pltpu.roll(value, shift, 1) * weight
            out[part, :, pl.ds(base, KCOLS)] += value
        return carry

    lax.fori_loop(0, 16, one, 0, unroll=4)


def step_kernel(
    n, offsets, live, meta, obj, probe_hbm, amps_hbm, cos, sin, new_obj, new_probe,
    metas_in, metas, probe, amps, win, relay_in, grad, patch, wave, half_done, far, sums9, ta, tb,
    q_in, sib_in, t2_in, t1_in, t8_in, back_in, far_in, piece, q_sib, acc, minus_in, plus_in, y_in,
    tile, dp, dp_in, kmine, ksib, kk, kpad, illum, place, dobj, vec, vec1, vec2,
    send, recv, ysem, kysem, kxsem, v1sem, v2sem, bsend, dpsem, psem, lsem,
    gsend, ownsem, aheadsem, relaysem, finalsem, tailsem, mrecv, msem,
):
    me = lax.axis_index("scan")
    q = me % SPLIT
    core = me % 2
    first = me - q
    row = me // SPLIT
    rows_all = n // SPLIT
    up = (me - SPLIT + n) % n
    down = (me + SPLIT) % n
    sibling = me + 1 - 2 * core
    side = 8
    x, y = me // (2 * side), (me // 2) % side
    msg = Messages(send, recv)

    def chip(at_x, at_y, at_core):
        return ((at_x % side) * side + at_y % side) * 2 + at_core

    def columns(quarter):
        return pl.ds(mult(768 * (quarter // 2) + OWN * (quarter % 2), LANES), OWN)

    def rows(start, size):
        return pl.ds(mult(start, 8), size)

    load_probe = pltpu.make_async_copy(probe_hbm, probe, lsem.at[0])
    load_probe.start()
    load_amps = pltpu.make_async_copy(amps_hbm, amps, lsem.at[1])
    load_amps.start()
    peers = [(first + SPLIT * e + k + 2 * n) % n for e in (-2, -1, 1, 2) for k in range(SPLIT)]
    peers += [chip(x + k, y, cc) for k in range(1, side) for cc in range(2)]
    peers += [chip(x, y + k, cc) for k in range(1, side) for cc in range(2)]
    peers += [sibling]
    greet(peers)

    sends = []

    def put(src, dst, recv_sem, there, when=None):
        copy = pltpu.make_async_remote_copy(
            src_ref=src,
            dst_ref=dst,
            send_sem=gsend.at[len(sends)],
            recv_sem=recv_sem,
            device_id={"scan": there},
            device_id_type=MESH,
        )
        sends.append((copy, when))
        if when is None:
            copy.start()
        else:
            pl.when(when)(copy.start)

    def landing(quarter, start, size=STRIP):
        return win.at[:, rows(start, size), pl.ds(mult(LANES * (quarter % 2), LANES), OWN)]

    relay, origin, target, source = long_way(me, -1)
    middle = jnp.logical_or(q == 1, q == 2)
    middle_at = jnp.clip(q - 1, 0, 1)
    around = [(q + k) % SPLIT for k in range(SPLIT)]
    for there in around:
        block = obj.at[:, :, columns(there)]
        put(block, relay_in.at[middle_at], relaysem.at[middle_at], relay - q + there, when=middle)
        put(block, landing(there, JITTER + STEP + STRIP * q), aheadsem.at[q], (first - SPLIT + there + n) % n)
    for there in around[1:]:
        block = obj.at[:, :, columns(there)]
        put(block, landing(there, JITTER + STRIP * q), ownsem.at[q], first + there)
    for there in around:
        block = obj.at[:, pl.ds(STRIP - JITTER, JITTER), columns(there)]
        put(block, landing(there, 0, JITTER), tailsem, (first + SPLIT + there) % n, when=q == SPLIT - 1)
    for e in (-1, 0, 1, 2):
        for k in range(SPLIT):
            if e or k:
                there = (first + SPLIT * e + (q + k) % SPLIT + n) % n
                put(meta, metas_in.at[(2 - e) * SPLIT + q], mrecv, there)
    own_at = mult(LANES * core, LANES)
    own_cols = pl.ds(own_at, OWN)
    sib_cols = pl.ds(mult(OWN * (1 - core), LANES), LANES)
    win[:, rows(JITTER + STRIP * q, STRIP), own_cols] = obj[:, :, columns(q)]
    metas_in[2 * SPLIT + q] = meta[...]

    c, s = cos[...], sin[...]
    ta[0:256, 0:256] = c
    ta[0:256, 256:512] = s
    ta[256:512, 0:256] = -s
    ta[256:512, 256:512] = c
    tb[0:256, 0:256] = c
    tb[0:256, 256:512] = -s
    tb[256:512, 0:256] = s
    tb[256:512, 256:512] = c
    grad[...] = jnp.zeros_like(grad)
    sums9[...] = jnp.zeros_like(sums9)
    kpad[...] = jnp.zeros_like(kpad)
    illum[...] = jnp.zeros_like(illum)
    place[...] = jnp.zeros_like(place)
    dobj[...] = jnp.zeros_like(dobj)
    win[:, ROWS:, :] = jnp.zeros((2, 16, WIN), F32)
    load_probe.wait()
    light = jnp.zeros((PATCH, PATCH), F32)
    for m in range(MODES):
        light = light + (probe[0, m] * probe[0, m] + probe[1, m] * probe[1, m])
    kpad[0, ZTOP : ZTOP + PATCH, 0:PATCH] = light

    def arrived(ref, sem):
        return pltpu.make_async_copy(ref, ref, sem)

    def border(start, size):
        mine = pl.ds(mult(LANES * core + 384 * (1 - core), LANES), LANES)
        src = win.at[:, pl.ds(start, size), mine]
        dst = win.at[:, pl.ds(start, size), pl.ds(mult(OWN * core, LANES), LANES)]
        copy = msg.make(src, dst, sibling)
        copy.start()
        return copy

    def far_on(j):
        arrived(relay_in.at[j - 1], relaysem.at[j - 1]).wait()
        put(relay_in.at[j - 1], landing(q, JITTER + 2 * STEP + STRIP * j), finalsem.at[j], target)

    for j in range(SPLIT):
        pl.when(q != j)(arrived(landing(q, JITTER + STRIP * j), ownsem.at[j]).wait)
        if j == 0:
            arrived(landing(q, JITTER + STEP), aheadsem.at[0]).wait()
            put(landing(q, JITTER + STEP), landing(q, JITTER + 2 * STEP), finalsem.at[0], up)
            far_on(1)
        if j == 1:
            far_on(2)
    borders = [border(JITTER, STEP)]
    arrived(metas_in.at[pl.ds(0, 15)], mrecv).wait()
    to_smem = pltpu.make_async_copy(metas_in, metas, msem)
    to_smem.start()
    to_smem.wait()
    for line in range(3):
        spread(n, kpad.at[pl.ds(0, 1)], illum, metas, line)
    arrived(landing(q, 0, JITTER), tailsem).wait()
    borders.append(border(0, JITTER))
    for j in range(1, SPLIT):
        arrived(landing(q, JITTER + STEP + STRIP * j), aheadsem.at[j]).wait()
    borders.append(border(JITTER + STEP, STEP))
    for j in range(3):
        arrived(landing(q, JITTER + 2 * STEP + STRIP * j), finalsem.at[j]).wait()
    borders.append(border(JITTER + 2 * STEP, 72))
    load_amps.wait()
    for copy in borders:
        copy.wait_recv()

    def clear_outside(ref):
        @pl.when(row == 0)
        def _():
            ref[:, 0:JITTER, :] = jnp.zeros((2, JITTER, WIN), F32)

        @pl.when(row == rows_all - 1)
        def _():
            ref[:, JITTER + STEP : JITTER + 2 * STEP, :] = jnp.zeros((2, STEP, WIN), F32)

        @pl.when(row >= rows_all - 2)
        def _():
            ref[:, JITTER + 2 * STEP : ROWS, :] = jnp.zeros((2, 72, WIN), F32)

    msg.drain()
    for copy, when in sends:
        if when is None:
            copy.wait_send()
        else:
            pl.when(when)(copy.wait_send)
    clear_outside(win)

    chunk = 32
    chunks = PATCH // chunk
    slab = chunk + 2 * JITTER

    def transform(left, right):
        for m in range(MODES):
            cols = slice(m * PATCH, (m + 1) * PATCH)
            z = jnp.dot(left[...], wave[:, cols], preferred_element_type=F32)
            half_done[cols, 0:PATCH] = z[0:PATCH].astype(BF16)
            half_done[cols, PATCH : 2 * PATCH] = z[PATCH : 2 * PATCH].astype(BF16)
        for m in range(MODES):
            cols = slice(m * PATCH, (m + 1) * PATCH)
            far[m] = jnp.dot(half_done[cols, :], right[...], preferred_element_type=F32)

    def visit(p, carry):
        ahead = jnp.clip(offsets[p, 0] - (STEP * row - JITTER), 0, 2 * JITTER)
        base = mult((STEP * p + 40) // LANES * LANES, LANES)
        shift = jnp.clip(offsets[p, 1] - STEP * SPLIT * q - base, 0, LANES)
        weight = jnp.where(p < live[0], 1.0, 0.0).astype(F32)

        def exits(i, carry):
            at = pl.ds(mult(i * chunk, chunk), chunk)
            low = pl.ds(mult(PATCH + i * chunk, chunk), chunk)
            o = []
            for part in range(2):
                v = win[part, pl.ds(mult(i * chunk, chunk), slab), pl.ds(base, KCOLS)]
                v = pltpu.roll(v, (slab - ahead) % slab, 0)[0:chunk]
                v = pltpu.roll(v, KCOLS - shift, 1)[:, 0:PATCH]
                patch[part, at, :] = v
                o.append(v)
            for m in range(MODES):
                pr, pi = probe[0, m, at, :], probe[1, m, at, :]
                wave[at, m * PATCH : (m + 1) * PATCH] = (pr * o[0] - pi * o[1]).astype(BF16)
                wave[low, m * PATCH : (m + 1) * PATCH] = (pr * o[1] + pi * o[0]).astype(BF16)
            return carry

        lax.fori_loop(0, chunks, exits, 0)
        transform(ta, tb)

        def changes(i, carry):
            at = pl.ds(mult(i * chunk, chunk), chunk)
            low = pl.ds(mult(PATCH + i * chunk, chunk), chunk)
            bright = jnp.zeros((chunk, PATCH), F32)
            for m in range(MODES):
                fr, fi = far[m, at, 0:PATCH], far[m, at, PATCH : 2 * PATCH]
                bright = bright + (fr * fr + fi * fi)
            factor = (amps[p, at, :] / jnp.maximum(jnp.sqrt(bright), 0.5) - 1.0) * weight
            for m in range(MODES):
                fr, fi = far[m, at, 0:PATCH], far[m, at, PATCH : 2 * PATCH]
                wave[at, m * PATCH : (m + 1) * PATCH] = (fr * factor).astype(BF16)
                wave[low, m * PATCH : (m + 1) * PATCH] = (fi * factor).astype(BF16)
            return carry

        lax.fori_loop(0, chunks, changes, 0)
        transform(tb, ta)

        def grads(i, carry):
            at = pl.ds(mult(i * chunk, chunk), chunk)
            o_re, o_im = patch[0, at, :], patch[1, at, :]
            g_re = jnp.zeros((chunk, PATCH), F32)
            g_im = jnp.zeros((chunk, PATCH), F32)
            for m in range(MODES):
                pr, pi = probe[0, m, at, :], probe[1, m, at, :]
                cr, ci = far[m, at, 0:PATCH], far[m, at, PATCH : 2 * PATCH]
                g_re = g_re + (pr * cr + pi * ci)
                g_im = g_im + (pr * ci - pi * cr)
                sums9[m, at, :] += o_re * cr + o_im * ci
                sums9[MODES + m, at, :] += o_re * ci - o_im * cr
            sums9[2 * MODES, at, :] += (o_re * o_re + o_im * o_im) * weight
            blank = jnp.zeros((chunk, KCOLS - PATCH), F32)
            below = jnp.zeros((2 * JITTER, KCOLS), F32)
            for part, g in enumerate((g_re, g_im)):
                v = pltpu.roll(jnp.concatenate([g, blank], 1), shift, 1)
                v = pltpu.roll(jnp.concatenate([v, below], 0), ahead, 0)
                grad[part, pl.ds(mult(i * chunk, chunk), slab), pl.ds(base, KCOLS)] += v
            return carry

        lax.fori_loop(0, chunks, grads, 0)
        return carry

    lax.fori_loop(0, SPLIT, visit, 0)
    clear_outside(grad)

    to_sib = msg.make(grad.at[:, pl.ds(0, ROWS), sib_cols], sib_in, sibling)
    to_sib.start()
    for at_band in range(PATCH // 8):
        yy = (at_band // 2) % 8
        for at_lane in range(2):
            xx = (at_band // 16) * 4 + (at_band % 2) * 2 + at_lane
            at_rows = slice(8 * at_band, 8 * at_band + 8)
            at_cols = slice(LANES * at_lane, LANES * at_lane + LANES)
            for k in range(2):
                for i, m in enumerate((2 * k, 2 * k + 1, MODES + 2 * k, MODES + 2 * k + 1, 8)):
                    q_in[k, xx, yy, i] = sums9[m, at_rows, at_cols]
    chunks = [(x + k) % side for k in (4, 5, 3, 6, 2, 7, 1, 0)]
    q_copies = []
    for at in chunks:
        copy = msg.make(q_in.at[1 - core, at], q_sib.at[at], sibling)
        copy.start()
        q_copies.append(copy)
    relay, origin, target, source = long_way(me, 1)

    band = (x // 4) * 16 + y * 2 + (x // 2) % 2
    lane = x % 2
    out_mode = x // 2
    out_band = (x % 2) * 16 + y * 2 + core
    p_tile = probe[:, pl.ds(2 * core, 2), pl.ds(mult(8 * band, 8), 8), pl.ds(mult(LANES * lane, LANES), LANES)]

    to_sib.wait_recv()
    edge = pl.ds(mult(LANES * core + 384 * (1 - core), LANES), LANES)
    grad[:, 0:ROWS, edge] += sib_in[...]

    def sums(start):
        return grad.at[:, pl.ds(start, STRIP), own_cols]

    def add_sibling(i):
        q_copies[i].wait_recv()
        acc[chunks[i]] = q_in[core, chunks[i]] + q_sib[chunks[i]]

    halves = side // 2

    def send_chain(way, i):
        which = (i % 2 if way < 0 else 1 - i % 2) * halves
        reach = (4 if i % 2 == 0 else 3) - i // 2
        dest = (x + way * reach + side) % side
        copy = msg.make(
            acc.at[dest, pl.ds(which, halves)],
            (minus_in if way < 0 else plus_in).at[i],
            chip(x + way + side, y, core),
        )
        copy.start()
        return copy

    chains = {}
    add_sibling(0)
    chains[-1, 0], chains[1, 0] = send_chain(-1, 0), send_chain(1, 0)
    add_sibling(1)
    chains[-1, 1] = send_chain(-1, 1)
    add_sibling(2)
    chains[1, 1] = send_chain(1, 1)
    far_out = []
    for j in (1, 2):
        copy = msg.make(sums(JITTER + 2 * STEP + STRIP * j), back_in.at[j - 1], relay)
        copy.start()
        far_out.append(copy)
    t2 = msg.make(sums(JITTER + 2 * STEP), t2_in, down)
    t2.start()
    t8 = msg.make(grad.at[:, pl.ds(0, JITTER), own_cols], t8_in, up)
    t8.start()

    def send_t1(j):
        copy = msg.make(sums(JITTER + STEP + STRIP * j), t1_in.at[j], down)
        copy.start()
        return copy

    t1 = {3: send_t1(3)}

    for i in range(3, 8):
        add_sibling(i)

    def x_step(i):
        for way, arrived in ((-1, minus_in), (1, plus_in)):
            which = (i % 2 if way < 0 else 1 - i % 2) * halves
            reach = (4 if i % 2 == 0 else 3) - 1 - i // 2
            dest = (x + way * reach + side) % side
            chains[way, i].wait_recv()
            acc[dest, which : which + halves] += arrived[i]
            if reach > 0:
                chains[way, i + 2] = send_chain(way, i + 2)

    x_step(0)
    t1[1] = send_t1(1)
    x_step(1)
    t1[2] = send_t1(2)
    x_step(2)
    t2.wait_recv()
    grad[:, JITTER + STEP : JITTER + STEP + STRIP, own_cols] += t2_in[...]
    t1[0] = send_t1(0)
    x_step(3)
    far_final = []
    for j in range(2):
        far_out[j].wait_recv()
        copy = msg.make(back_in.at[j], far_in.at[j], target)
        copy.start()
        far_final.append(copy)
    x_step(4)
    x_step(5)
    x_step(6)

    y_copies = []
    for k in range(1, side):
        copy = pltpu.make_async_remote_copy(
            src_ref=acc.at[x, (y + k) % side],
            dst_ref=y_in.at[k - 1],
            send_sem=bsend.at[k - 1],
            recv_sem=ysem,
            device_id={"scan": chip(x, y + k, core)},
            device_id_type=MESH,
        )
        copy.start()
        y_copies.append(copy)
    pltpu.make_async_copy(y_in, y_in, ysem).wait()
    tile[...] = acc[x, y] + jnp.sum(y_in[...], 0)
    norm = tile[4]
    inverse = norm + 1.0
    k_re = jnp.zeros((8, LANES), F32)
    k_im = jnp.zeros((8, LANES), F32)
    s_vv = jnp.zeros((8, LANES), F32)
    s_vc = jnp.zeros((8, LANES), F32)
    for m in range(2):
        g_re, g_im = tile[m], tile[2 + m]
        d_re, d_im = g_re / inverse, g_im / inverse
        dp[m, 0] = d_re
        dp[m, 1] = d_im
        p_re, p_im = p_tile[0, m], p_tile[1, m]
        k_re = k_re + (p_re * d_re + p_im * d_im)
        k_im = k_im + (p_re * d_im - p_im * d_re)
        s_vv = s_vv + (d_re * d_re + d_im * d_im) * norm
        s_vc = s_vc + (d_re * g_re + d_im * g_im)
    kmine[0] = k_re
    kmine[1] = k_im
    k_copy = msg.make(kmine.at[1 - core], ksib, sibling)
    k_copy.start()

    dp_sends = []
    for m in range(2):
        dest = chip(2 * (2 * core + m) + x // 4, y, (x // 2) % 2)
        away = dest != me
        copy = pltpu.make_async_remote_copy(
            src_ref=dp.at[m],
            dst_ref=dp_in.at[lane],
            send_sem=bsend.at[21 + m],
            recv_sem=dpsem.at[lane],
            device_id={"scan": dest},
            device_id_type=MESH,
        )
        pl.when(away)(copy.start)
        dp_sends.append((copy, away))

        @pl.when(jnp.logical_not(away))
        def _():
            dp_in[lane] = dp[m]

    k_copy.wait_recv()
    kk[core, x, y] = kmine[core] + ksib[...]
    ky_copies = []
    for k in range(1, side):
        copy = pltpu.make_async_remote_copy(
            src_ref=kk.at[core, x, y],
            dst_ref=kk.at[core, x, y],
            send_sem=bsend.at[7 + k - 1],
            recv_sem=kysem,
            device_id={"scan": chip(x, y + k, core)},
            device_id_type=MESH,
        )
        copy.start()
        ky_copies.append(copy)

    pieces = []
    for j in (3, 1, 2, 0):
        t1[j].wait_recv()
        lo = JITTER + STRIP * j
        grad[:, lo : lo + STRIP, own_cols] += t1_in[j]
        if j == 3:
            t8.wait_recv()
            grad[:, STEP : STEP + JITTER, own_cols] += t8_in[...]
        if j in (1, 2):
            far_final[j - 1].wait_recv()
            grad[:, lo : lo + STRIP, own_cols] += far_in[j - 1]
        slot = (j - q + SPLIT) % SPLIT
        copy = pltpu.make_async_remote_copy(
            src_ref=grad.at[:, pl.ds(lo, STRIP), own_cols],
            dst_ref=piece.at[slot],
            send_sem=bsend.at[23 + j],
            recv_sem=psem.at[slot],
            device_id={"scan": first + j},
            device_id_type=MESH,
        )
        pl.when(q != j)(copy.start)
        pieces.append((copy, q != j))

    pltpu.make_async_copy(kk.at[0, 0, pl.ds(0, 7)], kk.at[0, 0, pl.ds(0, 7)], kysem).wait()
    kx_copies = []
    for k in range(1, side):
        copy = pltpu.make_async_remote_copy(
            src_ref=kk.at[core, x],
            dst_ref=kk.at[core, x],
            send_sem=bsend.at[14 + k - 1],
            recv_sem=kxsem,
            device_id={"scan": chip(x + k, y, core)},
            device_id_type=MESH,
        )
        copy.start()
        kx_copies.append(copy)
    piece[0] = grad[:, pl.ds(mult(JITTER + STRIP * q, 8), STRIP), own_cols]

    pltpu.make_async_copy(kk.at[0, pl.ds(0, 7)], kk.at[0, pl.ds(0, 7)], kxsem).wait()
    ks_copy = msg.make(kk.at[core], kk.at[core], sibling)
    ks_copy.start()

    for k in range(SPLIT):
        if k > 0:
            pltpu.make_async_copy(piece.at[k], piece.at[k], psem.at[k]).wait()
        source = (q - k + SPLIT) % SPLIT
        at = pl.ds(mult(768 * (source // 2) + OWN * (source % 2), LANES), OWN)
        dobj[:, :, at] += piece[k]
    bright = illum[0]
    g_re, g_im = dobj[0], dobj[1]
    o_re, o_im = obj[0], obj[1]
    d_re, d_im = g_re / (bright + 1.0), g_im / (bright + 1.0)
    s_uu = jnp.sum((d_re * d_re + d_im * d_im) * bright)
    s_uc = jnp.sum(d_re * g_re + d_im * g_im)
    dobj[0] = d_re
    dobj[1] = d_im

    ks_copy.wait_recv()
    for at_band in range(PATCH // 8):
        for at_lane in range(2):
            xx = (at_band // 16) * 4 + (at_band % 2) * 2 + at_lane
            yy = (at_band // 2) % 8
            rows = slice(ZTOP + 8 * at_band, ZTOP + 8 * at_band + 8)
            cols = slice(LANES * at_lane, LANES * at_lane + LANES)
            kpad[0, rows, cols] = kk[0, xx, yy]
            kpad[1, rows, cols] = kk[1, xx, yy]
    for line in range(3):
        spread(n, kpad, place, metas, line)
    d_re, d_im = dobj[0], dobj[1]
    s_uv = jnp.sum(
        place[0] * (d_re * o_re + d_im * o_im) - place[1] * (d_re * o_im - d_im * o_re)
    )

    at = lax.broadcasted_iota(jnp.int32, (8, LANES), 1)
    own_sums = jnp.zeros((8, LANES), F32)
    for i, value in enumerate((s_uu, s_uv, jnp.sum(s_vv), s_uc, jnp.sum(s_vc))):
        own_sums = jnp.where(at == i, value, own_sums)
    vec[...] = own_sums
    v1_copies = []
    for k in range(1, 2 * side):
        copy = pltpu.make_async_remote_copy(
            src_ref=vec,
            dst_ref=vec1.at[k - 1],
            send_sem=bsend.at[27 + k - 1],
            recv_sem=v1sem,
            device_id={"scan": chip(x, y + k // 2, (core + k) % 2)},
            device_id_type=MESH,
        )
        copy.start()
        v1_copies.append(copy)
    pltpu.make_async_copy(vec1, vec1, v1sem).wait()
    for copy in v1_copies:
        copy.wait_send()
    vec[...] = own_sums + jnp.sum(vec1[...], 0)
    v2_copies = []
    for k in range(1, side):
        copy = pltpu.make_async_remote_copy(
            src_ref=vec,
            dst_ref=vec2.at[k - 1],
            send_sem=bsend.at[42 + k - 1],
            recv_sem=v2sem,
            device_id={"scan": chip(x + k, y, core)},
            device_id_type=MESH,
        )
        copy.start()
        v2_copies.append(copy)
    for at_lane in range(2):
        source = chip((x % 2) * 4 + core * 2 + at_lane, y, x // 4)
        arrived = pltpu.make_async_copy(dp_in.at[at_lane], dp_in.at[at_lane], dpsem.at[at_lane])
        pl.when(source != me)(arrived.wait)
    pltpu.make_async_copy(vec2, vec2, v2sem).wait()
    totals = vec[...] + jnp.sum(vec2[...], 0)
    uu, uv, vv, uc, vc = (totals[0:1, i : i + 1] for i in range(5))
    a = 1.1 * uu + 1e-06
    d = 1.1 * vv + 1e-06
    det = a * d - uv * uv
    rate_obj = (uc * d - uv * vc) / det
    rate_probe = (a * vc - uv * uc) / det
    for part in range(2):
        new_obj[part] = obj[part] + rate_obj * dobj[part]
        for at_lane in range(2):
            cols = slice(LANES * at_lane, LANES * at_lane + LANES)
            new_probe[part, :, cols] = probe[part, out_mode, pl.ds(mult(8 * out_band, 8), 8), cols] + rate_probe * dp_in[at_lane, part]

    msg.drain()
    for copy in y_copies + ky_copies + kx_copies + v2_copies:
        copy.wait_send()
    for copy, when in dp_sends + pieces:
        pl.when(when)(copy.wait_send)


def step(n, offsets, live, meta, obj, probe, amps, cos, sin):
    vmem = pl.BlockSpec(memory_space=pltpu.VMEM)
    smem = pl.BlockSpec(memory_space=pltpu.SMEM)
    hbm = pl.BlockSpec(memory_space=pl.ANY)
    dma = pltpu.SemaphoreType.DMA
    columns = obj.shape[2]

    def f32(*shape):
        return pltpu.VMEM(shape, F32)

    return pl.pallas_call(
        functools.partial(step_kernel, n),
        out_shape=(
            jax.ShapeDtypeStruct((2, STRIP, columns), F32),
            jax.ShapeDtypeStruct((2, 8, PATCH), F32),
        ),
        in_specs=[smem, smem, vmem, vmem, hbm, hbm, vmem, vmem],
        out_specs=[vmem] * 2,
        scratch_shapes=[
            pltpu.VMEM((4 * SPLIT, 8, LANES), jnp.int32),
            pltpu.SMEM((4 * SPLIT, 8, LANES), jnp.int32),
            f32(2, MODES, PATCH, PATCH),
            f32(SPLIT, PATCH, PATCH),
            f32(2, ROWS + 16, WIN),
            f32(2, 2, STRIP, OWN),
            f32(2, ROWS + 16, WIN),
            f32(2, PATCH, PATCH),
            pltpu.VMEM((2 * PATCH, MODES * PATCH), BF16),
            pltpu.VMEM((MODES * PATCH, 2 * PATCH), BF16),
            f32(MODES, PATCH, 2 * PATCH),
            f32(2 * MODES + 1, PATCH, PATCH),
            pltpu.VMEM((2 * PATCH, 2 * PATCH), BF16),
            pltpu.VMEM((2 * PATCH, 2 * PATCH), BF16),
            f32(2, 8, 8, 5, 8, LANES),
            f32(2, ROWS, LANES),
            f32(2, STRIP, OWN),
            f32(4, 2, STRIP, OWN),
            f32(2, JITTER, OWN),
            f32(2, 2, STRIP, OWN),
            f32(2, 2, STRIP, OWN),
            f32(4, 2, STRIP, OWN),
            f32(8, 8, 5, 8, LANES),
            f32(8, 8, 5, 8, LANES),
            f32(7, 4, 5, 8, LANES),
            f32(7, 4, 5, 8, LANES),
            f32(7, 5, 8, LANES),
            f32(5, 8, LANES),
            f32(2, 2, 8, LANES),
            f32(2, 2, 8, LANES),
            f32(2, 8, LANES),
            f32(8, LANES),
            f32(2, 8, 8, 8, LANES),
            f32(2, KROWS, KCOLS),
            f32(1, STRIP, columns),
            f32(2, STRIP, columns),
            f32(2, STRIP, columns),
            f32(8, LANES),
            f32(15, 8, LANES),
            f32(7, 8, LANES),
            dma((48,)),
            dma((48,)),
            dma,
            dma,
            dma,
            dma,
            dma,
            dma((50,)),
            dma((2,)),
            dma((4,)),
            dma((2,)),
            dma((40,)),
            dma((4,)),
            dma((4,)),
            dma((2,)),
            dma((3,)),
            dma,
            dma,
            dma,
        ],
        compiler_params=pltpu.CompilerParams(collective_id=0, has_side_effects=True),
        name="step",
    )(offsets, live, meta, obj, probe, amps, cos, sin)


def tables(length):
    numbers = np.arange(length, dtype=np.int64)
    angles = (numbers[:, None] * numbers[None, :] % length).astype(np.float32)
    angles = angles * np.float32(2.0 * math.pi / length)
    scaling = np.float32(1.0 / math.sqrt(length))
    return tuple(jnp.asarray(f(angles) * scaling).astype(BF16) for f in (np.cos, np.sin))


def on_device(n, object_field, probe_field, amplitudes, offsets, live_counts):
    probe = probe_field.reshape(2, MODES, PATCH, PATCH)
    meta = jnp.concatenate([offsets.reshape(-1), live_counts])
    meta = jnp.broadcast_to(jnp.pad(meta, (0, LANES - meta.shape[0]))[None], (8, LANES))
    cos, sin = tables(PATCH)
    return step(n, offsets, live_counts, meta, object_field, probe, amplitudes, cos, sin)


def solution(mesh):
    groups_scan = ("groups", "scan")
    placed = (
        P(None, groups_scan, None),
        P(None, "groups", None),
        P(groups_scan, None, None),
        P(groups_scan, None),
        P(groups_scan),
    )
    return jax.shard_map(
        functools.partial(on_device, mesh.shape["scan"]),
        mesh=mesh,
        in_specs=placed,
        out_specs=(P(None, groups_scan, None), P(None, groups_scan, None)),
        check_vma=False,
    )
```

```python
import functools
import math

import jax
import jax.numpy as jnp
import numpy as np
from jax import lax
from jax.experimental import pallas as pl
from jax.experimental.pallas import tpu as pltpu
from jax.sharding import PartitionSpec as P

MESH = pl.DeviceIdType.MESH
SPLIT = 4
JITTER = 8
STEP = 96
PATCH = 256
MODES = 4
STRIP = 24
LANES = 128
OWN = 512
WIN = 640
ROWS = JITTER + 2 * STEP + 72
ZTOP = 104
KROWS = 408
KCOLS = 384
F32 = jnp.float32
BF16 = jnp.bfloat16


def mult(value, of):
    return pl.multiple_of(value, of)


class Messages:
    def __init__(self, send, recv):
        self.send, self.recv, self.count, self.open = send, recv, 0, []

    def make(self, src, dst, scan, when=None):
        at = self.count
        self.count += 1
        self.last = self.recv.at[at]
        copy = pltpu.make_async_remote_copy(
            src_ref=src,
            dst_ref=dst,
            send_sem=self.send.at[at],
            recv_sem=self.recv.at[at],
            device_id={"scan": scan},
            device_id_type=MESH,
        )
        self.open.append((copy, when))
        return copy

    def drain(self):
        for copy, when in self.open:
            if when is None:
                copy.wait_send()
            else:
                pl.when(when)(copy.wait_send)
        self.open = []


def greet(peers):
    barrier = pltpu.get_barrier_semaphore()
    for peer in peers:
        pl.semaphore_signal(barrier, inc=1, device_id={"scan": peer}, device_id_type=MESH)
    pl.semaphore_wait(barrier, len(peers))


def long_way(me, step):
    line, at, q = me // 16, (me // SPLIT) % 4, me % SPLIT
    scale = 16

    def device(at_line, at_row):
        return (at_line + 8) % 8 * scale + (at_row + 8) % 4 * SPLIT + q

    def turn(row):
        row = (row + 8) % 4
        return jnp.where(jnp.logical_or(row == 0, row == 3), 0, 1)

    relay = device(line, at - step)
    origin = device(line, at + step)
    target = device(line + step * turn(at), at - step)
    source = device(line - step * turn(at + step), at + step)
    return relay, origin, target, source


def spread(n, kernel_pad, out, metas, line):
    me = lax.axis_index("scan")
    q = me % SPLIT
    line = line + jnp.where(q == SPLIT - 1, 1, 0)
    there = me // SPLIT - 2 + line
    inside = jnp.logical_and(there >= 0, there < n // SPLIT)
    start = mult(STRIP * q + STEP * (2 - line) - JITTER + ZTOP, 8)
    parts = out.shape[0]
    tall = STRIP + 2 * JITTER

    def one(col, carry):
        slot = line * SPLIT + col // SPLIT
        place = col % SPLIT
        top = metas[slot, 0, 2 * place]
        left = metas[slot, 0, 2 * place + 1]
        weight = jnp.where(jnp.logical_and(inside, place < metas[slot, 0, 8]), 1.0, 0.0).astype(F32)
        ahead = jnp.clip(STEP * there - top + JITTER, 0, 2 * JITTER)
        base = mult((STEP * col + 40) // LANES * LANES, LANES)
        shift = jnp.clip(left - base, 0, LANES)
        for part in range(parts):
            value = kernel_pad[part, pl.ds(start, tall), :]
            value = pltpu.roll(value, (tall - ahead) % tall, 0)[0:STRIP]
            value = pltpu.roll(value, shift, 1) * weight
            out[part, :, pl.ds(base, KCOLS)] += value
        return carry

    lax.fori_loop(0, 16, one, 0, unroll=4)


def step_kernel(
    n, offsets, live, meta, obj, probe_hbm, amps_hbm, cos, sin, new_obj, new_probe,
    metas_in, metas, probe, amps, win, relay_in, grad, patch, wave, half_done, far, sums9, ta, tb,
    q_in, sib_in, t2_in, t1_in, t8_in, back_in, far_in, piece, q_sib, acc, minus_in, plus_in, y_in, hold_t1, hold_far,
    tile, dp, dp_in, kmine, ksib, kk, kpad, illum, place, dobj, vec, vec1, vec2,
    send, recv, ysem, kysem, kxsem, v1sem, v2sem, bsend, dpsem, psem, lsem,
    gsend, ownsem, aheadsem, relaysem, finalsem, tailsem, mrecv, msem, holdsem,
):
    me = lax.axis_index("scan")
    q = me % SPLIT
    core = me % 2
    first = me - q
    row = me // SPLIT
    rows_all = n // SPLIT
    up = (me - SPLIT + n) % n
    down = (me + SPLIT) % n
    sibling = me + 1 - 2 * core
    side = 8
    x, y = me // (2 * side), (me // 2) % side
    msg = Messages(send, recv)

    def chip(at_x, at_y, at_core):
        return ((at_x % side) * side + at_y % side) * 2 + at_core

    def columns(quarter):
        return pl.ds(mult(768 * (quarter // 2) + OWN * (quarter % 2), LANES), OWN)

    def rows(start, size):
        return pl.ds(mult(start, 8), size)

    load_probe = pltpu.make_async_copy(probe_hbm, probe, lsem.at[0])
    load_probe.start()
    load_amps = pltpu.make_async_copy(amps_hbm, amps, lsem.at[1])
    load_amps.start()
    peers = [(first + SPLIT * e + k + 2 * n) % n for e in (-2, -1, 1, 2) for k in range(SPLIT)]
    peers += [chip(x + k, y, cc) for k in range(1, side) for cc in range(2)]
    peers += [chip(x, y + k, cc) for k in range(1, side) for cc in range(2)]
    peers += [sibling]
    greet(peers)

    sends = []

    def put(src, dst, recv_sem, there, when=None):
        copy = pltpu.make_async_remote_copy(
            src_ref=src,
            dst_ref=dst,
            send_sem=gsend.at[len(sends)],
            recv_sem=recv_sem,
            device_id={"scan": there},
            device_id_type=MESH,
        )
        sends.append((copy, when))
        if when is None:
            copy.start()
        else:
            pl.when(when)(copy.start)

    def landing(quarter, start, size=STRIP):
        return win.at[:, rows(start, size), pl.ds(mult(LANES * (quarter % 2), LANES), OWN)]

    for e in (-1, 0, 1, 2):
        for k in range(SPLIT):
            if e or k:
                there = (first + SPLIT * e + (q + k) % SPLIT + n) % n
                put(meta, metas_in.at[(2 - e) * SPLIT + q], mrecv, there)
    relay, origin, target, source = long_way(me, -1)
    middle = jnp.logical_or(q == 1, q == 2)
    middle_at = jnp.clip(q - 1, 0, 1)
    around = [(q + k) % SPLIT for k in range(SPLIT)]
    for there in around:
        block = obj.at[:, :, columns(there)]
        put(block, relay_in.at[middle_at], relaysem.at[middle_at], relay - q + there, when=middle)
        put(block, landing(there, JITTER + STEP + STRIP * q), aheadsem.at[q], (first - SPLIT + there + n) % n)
    for there in around[1:]:
        block = obj.at[:, :, columns(there)]
        put(block, landing(there, JITTER + STRIP * q), ownsem.at[q], first + there)
    for there in around:
        block = obj.at[:, pl.ds(STRIP - JITTER, JITTER), columns(there)]
        put(block, landing(there, 0, JITTER), tailsem, (first + SPLIT + there) % n, when=q == SPLIT - 1)
    own_at = mult(LANES * core, LANES)
    own_cols = pl.ds(own_at, OWN)
    sib_cols = pl.ds(mult(OWN * (1 - core), LANES), LANES)
    win[:, rows(JITTER + STRIP * q, STRIP), own_cols] = obj[:, :, columns(q)]
    metas_in[2 * SPLIT + q] = meta[...]

    c, s = cos[...], sin[...]
    ta[0:256, 0:256] = c
    ta[0:256, 256:512] = s
    ta[256:512, 0:256] = -s
    ta[256:512, 256:512] = c
    tb[0:256, 0:256] = c
    tb[0:256, 256:512] = -s
    tb[256:512, 0:256] = s
    tb[256:512, 256:512] = c
    grad[...] = jnp.zeros_like(grad)
    sums9[...] = jnp.zeros_like(sums9)
    kpad[...] = jnp.zeros_like(kpad)
    illum[...] = jnp.zeros_like(illum)
    place[...] = jnp.zeros_like(place)
    dobj[...] = jnp.zeros_like(dobj)
    win[:, ROWS:, :] = jnp.zeros((2, 16, WIN), F32)
    load_probe.wait()
    light = jnp.zeros((PATCH, PATCH), F32)
    for m in range(MODES):
        light = light + (probe[0, m] * probe[0, m] + probe[1, m] * probe[1, m])
    kpad[0, ZTOP : ZTOP + PATCH, 0:PATCH] = light

    def arrived(ref, sem):
        return pltpu.make_async_copy(ref, ref, sem)

    def border(start, size):
        mine = pl.ds(mult(LANES * core + 384 * (1 - core), LANES), LANES)
        src = win.at[:, pl.ds(start, size), mine]
        dst = win.at[:, pl.ds(start, size), pl.ds(mult(OWN * core, LANES), LANES)]
        copy = msg.make(src, dst, sibling)
        copy.start()
        return copy

    def far_on(j):
        arrived(relay_in.at[j - 1], relaysem.at[j - 1]).wait()
        put(relay_in.at[j - 1], landing(q, JITTER + 2 * STEP + STRIP * j), finalsem.at[j], target)

    for j in range(SPLIT):
        pl.when(q != j)(arrived(landing(q, JITTER + STRIP * j), ownsem.at[j]).wait)
        if j == 0:
            arrived(landing(q, JITTER + STEP), aheadsem.at[0]).wait()
            put(landing(q, JITTER + STEP), landing(q, JITTER + 2 * STEP), finalsem.at[0], up)
            far_on(1)
        if j == 1:
            far_on(2)
    borders = [border(JITTER, STEP)]
    arrived(landing(q, 0, JITTER), tailsem).wait()
    borders.append(border(0, JITTER))
    for j in range(1, SPLIT):
        arrived(landing(q, JITTER + STEP + STRIP * j), aheadsem.at[j]).wait()
    borders.append(border(JITTER + STEP, STEP))
    for j in range(3):
        arrived(landing(q, JITTER + 2 * STEP + STRIP * j), finalsem.at[j]).wait()
    borders.append(border(JITTER + 2 * STEP, 72))
    arrived(metas_in.at[pl.ds(0, 15)], mrecv).wait()
    to_smem = pltpu.make_async_copy(metas_in, metas, msem)
    to_smem.start()
    load_amps.wait()
    for copy in borders:
        copy.wait_recv()

    def clear_outside(ref):
        @pl.when(row == 0)
        def _():
            ref[:, 0:JITTER, :] = jnp.zeros((2, JITTER, WIN), F32)

        @pl.when(row == rows_all - 1)
        def _():
            ref[:, JITTER + STEP : JITTER + 2 * STEP, :] = jnp.zeros((2, STEP, WIN), F32)

        @pl.when(row >= rows_all - 2)
        def _():
            ref[:, JITTER + 2 * STEP : ROWS, :] = jnp.zeros((2, 72, WIN), F32)

    msg.drain()
    for copy, when in sends:
        if when is None:
            copy.wait_send()
        else:
            pl.when(when)(copy.wait_send)
    clear_outside(win)

    chunk = 32
    chunks = PATCH // chunk
    slab = chunk + 2 * JITTER

    def transform(left, right):
        for m in range(MODES):
            cols = slice(m * PATCH, (m + 1) * PATCH)
            z = jnp.dot(left[...], wave[:, cols], preferred_element_type=F32)
            half_done[cols, 0:PATCH] = z[0:PATCH].astype(BF16)
            half_done[cols, PATCH : 2 * PATCH] = z[PATCH : 2 * PATCH].astype(BF16)
        for m in range(MODES):
            cols = slice(m * PATCH, (m + 1) * PATCH)
            far[m] = jnp.dot(half_done[cols, :], right[...], preferred_element_type=F32)

    def visit(p, carry):
        ahead = jnp.clip(offsets[p, 0] - (STEP * row - JITTER), 0, 2 * JITTER)
        base = mult((STEP * p + 40) // LANES * LANES, LANES)
        shift = jnp.clip(offsets[p, 1] - STEP * SPLIT * q - base, 0, LANES)
        weight = jnp.where(p < live[0], 1.0, 0.0).astype(F32)

        def exits(i, carry):
            at = pl.ds(mult(i * chunk, chunk), chunk)
            low = pl.ds(mult(PATCH + i * chunk, chunk), chunk)
            o = []
            for part in range(2):
                v = win[part, pl.ds(mult(i * chunk, chunk), slab), pl.ds(base, KCOLS)]
                v = pltpu.roll(v, (slab - ahead) % slab, 0)[0:chunk]
                v = pltpu.roll(v, KCOLS - shift, 1)[:, 0:PATCH]
                patch[part, at, :] = v
                o.append(v)
            for m in range(MODES):
                pr, pi = probe[0, m, at, :], probe[1, m, at, :]
                wave[at, m * PATCH : (m + 1) * PATCH] = (pr * o[0] - pi * o[1]).astype(BF16)
                wave[low, m * PATCH : (m + 1) * PATCH] = (pr * o[1] + pi * o[0]).astype(BF16)
            return carry

        lax.fori_loop(0, chunks, exits, 0)
        transform(ta, tb)

        def changes(i, carry):
            at = pl.ds(mult(i * chunk, chunk), chunk)
            low = pl.ds(mult(PATCH + i * chunk, chunk), chunk)
            bright = jnp.zeros((chunk, PATCH), F32)
            for m in range(MODES):
                fr, fi = far[m, at, 0:PATCH], far[m, at, PATCH : 2 * PATCH]
                bright = bright + (fr * fr + fi * fi)
            factor = (amps[p, at, :] / jnp.maximum(jnp.sqrt(bright), 0.5) - 1.0) * weight
            for m in range(MODES):
                fr, fi = far[m, at, 0:PATCH], far[m, at, PATCH : 2 * PATCH]
                wave[at, m * PATCH : (m + 1) * PATCH] = (fr * factor).astype(BF16)
                wave[low, m * PATCH : (m + 1) * PATCH] = (fi * factor).astype(BF16)
            return carry

        lax.fori_loop(0, chunks, changes, 0)
        transform(tb, ta)

        def grads(i, carry):
            at = pl.ds(mult(i * chunk, chunk), chunk)
            o_re, o_im = patch[0, at, :], patch[1, at, :]
            g_re = jnp.zeros((chunk, PATCH), F32)
            g_im = jnp.zeros((chunk, PATCH), F32)
            for m in range(MODES):
                pr, pi = probe[0, m, at, :], probe[1, m, at, :]
                cr, ci = far[m, at, 0:PATCH], far[m, at, PATCH : 2 * PATCH]
                g_re = g_re + (pr * cr + pi * ci)
                g_im = g_im + (pr * ci - pi * cr)
                sums9[m, at, :] += o_re * cr + o_im * ci
                sums9[MODES + m, at, :] += o_re * ci - o_im * cr
            sums9[2 * MODES, at, :] += (o_re * o_re + o_im * o_im) * weight
            blank = jnp.zeros((chunk, KCOLS - PATCH), F32)
            below = jnp.zeros((2 * JITTER, KCOLS), F32)
            for part, g in enumerate((g_re, g_im)):
                v = pltpu.roll(jnp.concatenate([g, blank], 1), shift, 1)
                v = pltpu.roll(jnp.concatenate([v, below], 0), ahead, 0)
                grad[part, pl.ds(mult(i * chunk, chunk), slab), pl.ds(base, KCOLS)] += v
            return carry

        lax.fori_loop(0, chunks, grads, 0)
        return carry

    lax.fori_loop(0, SPLIT, visit, 0)
    clear_outside(grad)

    to_sib = msg.make(grad.at[:, pl.ds(0, ROWS), sib_cols], sib_in, sibling)
    to_sib.start()
    for at_band in range(PATCH // 8):
        yy = (at_band // 2) % 8
        for at_lane in range(2):
            xx = (at_band // 16) * 4 + (at_band % 2) * 2 + at_lane
            at_rows = slice(8 * at_band, 8 * at_band + 8)
            at_cols = slice(LANES * at_lane, LANES * at_lane + LANES)
            for k in range(2):
                for i, m in enumerate((2 * k, 2 * k + 1, MODES + 2 * k, MODES + 2 * k + 1, 8)):
                    q_in[k, xx, yy, i] = sums9[m, at_rows, at_cols]
    chunks = [(x + k) % side for k in (4, 5, 3, 6, 2, 7, 1, 0)]
    q_copies = []
    for at in chunks:
        copy = msg.make(q_in.at[1 - core, at], q_sib.at[at], sibling)
        copy.start()
        q_copies.append(copy)
    relay, origin, target, source = long_way(me, 1)

    band = (x // 4) * 16 + y * 2 + (x // 2) % 2
    lane = x % 2
    out_mode = x // 2
    out_band = (x % 2) * 16 + y * 2 + core
    p_tile = probe[:, pl.ds(2 * core, 2), pl.ds(mult(8 * band, 8), 8), pl.ds(mult(LANES * lane, LANES), LANES)]

    to_sib.wait_recv()
    edge = pl.ds(mult(LANES * core + 384 * (1 - core), LANES), LANES)
    grad[:, 0:ROWS, edge] += sib_in[...]

    def sums(start):
        return grad.at[:, pl.ds(start, STRIP), own_cols]

    def add_sibling(i):
        q_copies[i].wait_recv()
        acc[chunks[i]] = q_in[core, chunks[i]] + q_sib[chunks[i]]

    halves = side // 2

    def send_chain(way, i):
        which = (i % 2 if way < 0 else 1 - i % 2) * halves
        reach = (4 if i % 2 == 0 else 3) - i // 2
        dest = (x + way * reach + side) % side
        copy = msg.make(
            acc.at[dest, pl.ds(which, halves)],
            (minus_in if way < 0 else plus_in).at[i],
            chip(x + way + side, y, core),
        )
        copy.start()
        return copy

    chains = {}
    add_sibling(0)
    chains[-1, 0], chains[1, 0] = send_chain(-1, 0), send_chain(1, 0)
    add_sibling(1)
    chains[-1, 1] = send_chain(-1, 1)
    add_sibling(2)
    chains[1, 1] = send_chain(1, 1)
    far_out = []
    for j in (1, 2):
        copy = msg.make(sums(JITTER + 2 * STEP + STRIP * j), back_in.at[j - 1], relay)
        copy.start()
        far_out.append(copy)
    t2 = msg.make(sums(JITTER + 2 * STEP), t2_in, down)
    t2.start()
    t8 = msg.make(grad.at[:, pl.ds(0, JITTER), own_cols], t8_in, up)
    t8.start()

    at_row = (me // SPLIT) % 4
    crossing = at_row == 3
    holder = at_row == 0
    turning = jnp.logical_or(at_row == 1, at_row == 2)
    far_holder = at_row <= 1
    below = x * 2 * side + (at_row + 1) % 4 * SPLIT + q
    beside = chip(x + 1, y, core)

    def start_t1(j):
        src = sums(JITTER + STEP + STRIP * j)
        t1[j] = msg.make(src, t1_in.at[j], below, when=jnp.logical_not(crossing))
        final_sem = msg.last
        pl.when(jnp.logical_not(crossing))(t1[j].start)
        copy = msg.make(src, hold_t1.at[j], below, when=crossing)
        pl.when(crossing)(copy.start)
        held.append((copy, holder, hold_t1.at[j], t1_in.at[j], final_sem))

    def pass_far(j):
        there = x * 2 * side + (at_row + 3) % 4 * SPLIT + q
        final = msg.make(back_in.at[j], far_in.at[j], there, when=jnp.logical_not(turning))
        final_sem = msg.last
        pl.when(jnp.logical_not(turning))(final.start)
        copy = msg.make(back_in.at[j], hold_far.at[j], there, when=turning)
        pl.when(turning)(copy.start)
        held.append((copy, far_holder, hold_far.at[j], far_in.at[j], final_sem))
        return final

    def release(i):
        copy, here, src, dst, final_sem = held[i]
        pl.when(here)(copy.wait_recv)
        onward = pltpu.make_async_remote_copy(
            src_ref=src,
            dst_ref=dst,
            send_sem=holdsem.at[i],
            recv_sem=final_sem,
            device_id={"scan": beside},
            device_id_type=MESH,
        )
        pl.when(here)(onward.start)
        msg.open.append((onward, here))

    t1, held = {}, []
    start_t1(3)
    for i in range(3, 8):
        add_sibling(i)

    def x_step(i):
        for way, arrived in ((-1, minus_in), (1, plus_in)):
            which = (i % 2 if way < 0 else 1 - i % 2) * halves
            reach = (4 if i % 2 == 0 else 3) - 1 - i // 2
            dest = (x + way * reach + side) % side
            chains[way, i].wait_recv()
            acc[dest, which : which + halves] += arrived[i]
            if reach > 0:
                chains[way, i + 2] = send_chain(way, i + 2)

    to_smem.wait()
    x_step(0)
    start_t1(1)
    spread(n, kpad.at[pl.ds(0, 1)], illum, metas, 0)
    x_step(1)
    start_t1(2)
    spread(n, kpad.at[pl.ds(0, 1)], illum, metas, 1)
    x_step(2)
    t2.wait_recv()
    grad[:, JITTER + STEP : JITTER + STEP + STRIP, own_cols] += t2_in[...]
    start_t1(0)
    x_step(3)
    far_final = []
    for j in range(2):
        far_out[j].wait_recv()
        far_final.append(pass_far(j))
    x_step(4)
    spread(n, kpad.at[pl.ds(0, 1)], illum, metas, 2)
    x_step(5)
    x_step(6)

    y_copies = []
    for k in range(1, side):
        copy = pltpu.make_async_remote_copy(
            src_ref=acc.at[x, (y + k) % side],
            dst_ref=y_in.at[k - 1],
            send_sem=bsend.at[k - 1],
            recv_sem=ysem,
            device_id={"scan": chip(x, y + k, core)},
            device_id_type=MESH,
        )
        copy.start()
        y_copies.append(copy)
    for i in range(len(held)):
        release(i)
    pltpu.make_async_copy(y_in, y_in, ysem).wait()
    tile[...] = acc[x, y] + jnp.sum(y_in[...], 0)
    norm = tile[4]
    inverse = norm + 1.0
    k_re = jnp.zeros((8, LANES), F32)
    k_im = jnp.zeros((8, LANES), F32)
    s_vv = jnp.zeros((8, LANES), F32)
    s_vc = jnp.zeros((8, LANES), F32)
    for m in range(2):
        g_re, g_im = tile[m], tile[2 + m]
        d_re, d_im = g_re / inverse, g_im / inverse
        dp[m, 0] = d_re
        dp[m, 1] = d_im
        p_re, p_im = p_tile[0, m], p_tile[1, m]
        k_re = k_re + (p_re * d_re + p_im * d_im)
        k_im = k_im + (p_re * d_im - p_im * d_re)
        s_vv = s_vv + (d_re * d_re + d_im * d_im) * norm
        s_vc = s_vc + (d_re * g_re + d_im * g_im)
    kmine[0] = k_re
    kmine[1] = k_im
    k_copy = msg.make(kmine.at[1 - core], ksib, sibling)
    k_copy.start()

    dp_sends = []
    for m in range(2):
        dest = chip(2 * (2 * core + m) + x // 4, y, (x // 2) % 2)
        away = dest != me
        copy = pltpu.make_async_remote_copy(
            src_ref=dp.at[m],
            dst_ref=dp_in.at[lane],
            send_sem=bsend.at[21 + m],
            recv_sem=dpsem.at[lane],
            device_id={"scan": dest},
            device_id_type=MESH,
        )
        pl.when(away)(copy.start)
        dp_sends.append((copy, away))

        @pl.when(jnp.logical_not(away))
        def _():
            dp_in[lane] = dp[m]

    k_copy.wait_recv()
    kk[core, x, y] = kmine[core] + ksib[...]
    ky_copies = []
    for k in range(1, side):
        copy = pltpu.make_async_remote_copy(
            src_ref=kk.at[core, x, y],
            dst_ref=kk.at[core, x, y],
            send_sem=bsend.at[7 + k - 1],
            recv_sem=kysem,
            device_id={"scan": chip(x, y + k, core)},
            device_id_type=MESH,
        )
        copy.start()
        ky_copies.append(copy)

    pltpu.make_async_copy(kk.at[0, 0, pl.ds(0, 7)], kk.at[0, 0, pl.ds(0, 7)], kysem).wait()
    kx_copies = []
    for k in range(1, side):
        copy = pltpu.make_async_remote_copy(
            src_ref=kk.at[core, x],
            dst_ref=kk.at[core, x],
            send_sem=bsend.at[14 + k - 1],
            recv_sem=kxsem,
            device_id={"scan": chip(x + k, y, core)},
            device_id_type=MESH,
        )
        copy.start()
        kx_copies.append(copy)
    pieces = []
    for j in (3, 1, 2, 0):
        t1[j].wait_recv()
        lo = JITTER + STRIP * j
        grad[:, lo : lo + STRIP, own_cols] += t1_in[j]
        if j == 3:
            t8.wait_recv()
            grad[:, STEP : STEP + JITTER, own_cols] += t8_in[...]
        if j in (1, 2):
            far_final[j - 1].wait_recv()
            grad[:, lo : lo + STRIP, own_cols] += far_in[j - 1]
        slot = (j - q + SPLIT) % SPLIT
        copy = pltpu.make_async_remote_copy(
            src_ref=grad.at[:, pl.ds(lo, STRIP), own_cols],
            dst_ref=piece.at[slot],
            send_sem=bsend.at[23 + j],
            recv_sem=psem.at[slot],
            device_id={"scan": first + j},
            device_id_type=MESH,
        )
        pl.when(q != j)(copy.start)
        pieces.append((copy, q != j))

    piece[0] = grad[:, pl.ds(mult(JITTER + STRIP * q, 8), STRIP), own_cols]

    pltpu.make_async_copy(kk.at[0, pl.ds(0, 7)], kk.at[0, pl.ds(0, 7)], kxsem).wait()
    ks_copy = msg.make(kk.at[core], kk.at[core], sibling)
    ks_copy.start()

    for k in range(SPLIT):
        if k > 0:
            pltpu.make_async_copy(piece.at[k], piece.at[k], psem.at[k]).wait()
        source = (q - k + SPLIT) % SPLIT
        at = pl.ds(mult(768 * (source // 2) + OWN * (source % 2), LANES), OWN)
        dobj[:, :, at] += piece[k]
    bright = illum[0]
    g_re, g_im = dobj[0], dobj[1]
    o_re, o_im = obj[0], obj[1]
    d_re, d_im = g_re / (bright + 1.0), g_im / (bright + 1.0)
    s_uu = jnp.sum((d_re * d_re + d_im * d_im) * bright)
    s_uc = jnp.sum(d_re * g_re + d_im * g_im)
    dobj[0] = d_re
    dobj[1] = d_im

    ks_copy.wait_recv()
    for at_band in range(PATCH // 8):
        for at_lane in range(2):
            xx = (at_band // 16) * 4 + (at_band % 2) * 2 + at_lane
            yy = (at_band // 2) % 8
            rows = slice(ZTOP + 8 * at_band, ZTOP + 8 * at_band + 8)
            cols = slice(LANES * at_lane, LANES * at_lane + LANES)
            kpad[0, rows, cols] = kk[0, xx, yy]
            kpad[1, rows, cols] = kk[1, xx, yy]
    for line in range(3):
        spread(n, kpad, place, metas, line)
    d_re, d_im = dobj[0], dobj[1]
    s_uv = jnp.sum(
        place[0] * (d_re * o_re + d_im * o_im) - place[1] * (d_re * o_im - d_im * o_re)
    )

    at = lax.broadcasted_iota(jnp.int32, (8, LANES), 1)
    own_sums = jnp.zeros((8, LANES), F32)
    for i, value in enumerate((s_uu, s_uv, jnp.sum(s_vv), s_uc, jnp.sum(s_vc))):
        own_sums = jnp.where(at == i, value, own_sums)
    vec[...] = own_sums
    v1_copies = []
    for k in range(1, 2 * side):
        copy = pltpu.make_async_remote_copy(
            src_ref=vec.at[pl.ds(0, 1)],
            dst_ref=vec1.at[pl.ds(k - 1, 1)],
            send_sem=bsend.at[27 + k - 1],
            recv_sem=v1sem,
            device_id={"scan": chip(x, y + k // 2, (core + k) % 2)},
            device_id_type=MESH,
        )
        copy.start()
        v1_copies.append(copy)
    pltpu.make_async_copy(vec1.at[pl.ds(0, 15)], vec1.at[pl.ds(0, 15)], v1sem).wait()
    for copy in v1_copies:
        copy.wait_send()
    vec[...] = own_sums + jnp.sum(vec1[0:15, :], 0, keepdims=True)
    v2_copies = []
    for k in range(1, side):
        copy = pltpu.make_async_remote_copy(
            src_ref=vec.at[pl.ds(0, 1)],
            dst_ref=vec2.at[pl.ds(k - 1, 1)],
            send_sem=bsend.at[42 + k - 1],
            recv_sem=v2sem,
            device_id={"scan": chip(x + k, y, core)},
            device_id_type=MESH,
        )
        copy.start()
        v2_copies.append(copy)
    for at_lane in range(2):
        source = chip((x % 2) * 4 + core * 2 + at_lane, y, x // 4)
        arrived = pltpu.make_async_copy(dp_in.at[at_lane], dp_in.at[at_lane], dpsem.at[at_lane])
        pl.when(source != me)(arrived.wait)
    pltpu.make_async_copy(vec2.at[pl.ds(0, 7)], vec2.at[pl.ds(0, 7)], v2sem).wait()
    totals = vec[...] + jnp.sum(vec2[0:7, :], 0, keepdims=True)
    uu, uv, vv, uc, vc = (totals[0:1, i : i + 1] for i in range(5))
    a = 1.1 * uu + 1e-06
    d = 1.1 * vv + 1e-06
    det = a * d - uv * uv
    rate_obj = (uc * d - uv * vc) / det
    rate_probe = (a * vc - uv * uc) / det
    for part in range(2):
        new_obj[part] = obj[part] + rate_obj * dobj[part]
        for at_lane in range(2):
            cols = slice(LANES * at_lane, LANES * at_lane + LANES)
            new_probe[part, :, cols] = probe[part, out_mode, pl.ds(mult(8 * out_band, 8), 8), cols] + rate_probe * dp_in[at_lane, part]

    msg.drain()
    for copy in y_copies + ky_copies + kx_copies + v2_copies:
        copy.wait_send()
    for copy, when in dp_sends + pieces:
        pl.when(when)(copy.wait_send)


def step(n, offsets, live, meta, obj, probe, amps, cos, sin):
    vmem = pl.BlockSpec(memory_space=pltpu.VMEM)
    smem = pl.BlockSpec(memory_space=pltpu.SMEM)
    hbm = pl.BlockSpec(memory_space=pl.ANY)
    dma = pltpu.SemaphoreType.DMA
    columns = obj.shape[2]

    def f32(*shape):
        return pltpu.VMEM(shape, F32)

    return pl.pallas_call(
        functools.partial(step_kernel, n),
        out_shape=(
            jax.ShapeDtypeStruct((2, STRIP, columns), F32),
            jax.ShapeDtypeStruct((2, 8, PATCH), F32),
        ),
        in_specs=[smem, smem, vmem, vmem, hbm, hbm, vmem, vmem],
        out_specs=[vmem] * 2,
        scratch_shapes=[
            pltpu.VMEM((4 * SPLIT, 8, LANES), jnp.int32),
            pltpu.SMEM((4 * SPLIT, 8, LANES), jnp.int32),
            f32(2, MODES, PATCH, PATCH),
            f32(SPLIT, PATCH, PATCH),
            f32(2, ROWS + 16, WIN),
            f32(2, 2, STRIP, OWN),
            f32(2, ROWS + 16, WIN),
            f32(2, PATCH, PATCH),
            pltpu.VMEM((2 * PATCH, MODES * PATCH), BF16),
            pltpu.VMEM((MODES * PATCH, 2 * PATCH), BF16),
            f32(MODES, PATCH, 2 * PATCH),
            f32(2 * MODES + 1, PATCH, PATCH),
            pltpu.VMEM((2 * PATCH, 2 * PATCH), BF16),
            pltpu.VMEM((2 * PATCH, 2 * PATCH), BF16),
            f32(2, 8, 8, 5, 8, LANES),
            f32(2, ROWS, LANES),
            f32(2, STRIP, OWN),
            f32(4, 2, STRIP, OWN),
            f32(2, JITTER, OWN),
            f32(2, 2, STRIP, OWN),
            f32(2, 2, STRIP, OWN),
            f32(4, 2, STRIP, OWN),
            f32(8, 8, 5, 8, LANES),
            f32(8, 8, 5, 8, LANES),
            f32(7, 4, 5, 8, LANES),
            f32(7, 4, 5, 8, LANES),
            f32(7, 5, 8, LANES),
            f32(4, 2, STRIP, OWN),
            f32(2, 2, STRIP, OWN),
            f32(5, 8, LANES),
            f32(2, 2, 8, LANES),
            f32(2, 2, 8, LANES),
            f32(2, 8, LANES),
            f32(8, LANES),
            f32(2, 8, 8, 8, LANES),
            f32(2, KROWS, KCOLS),
            f32(1, STRIP, columns),
            f32(2, STRIP, columns),
            f32(2, STRIP, columns),
            f32(8, LANES),
            f32(16, LANES),
            f32(8, LANES),
            dma((48,)),
            dma((48,)),
            dma,
            dma,
            dma,
            dma,
            dma,
            dma((50,)),
            dma((2,)),
            dma((4,)),
            dma((2,)),
            dma((40,)),
            dma((4,)),
            dma((4,)),
            dma((2,)),
            dma((3,)),
            dma,
            dma,
            dma,
            dma((6,)),
        ],
        compiler_params=pltpu.CompilerParams(collective_id=0, has_side_effects=True),
        name="step",
    )(offsets, live, meta, obj, probe, amps, cos, sin)


def tables(length):
    numbers = np.arange(length, dtype=np.int64)
    angles = (numbers[:, None] * numbers[None, :] % length).astype(np.float32)
    angles = angles * np.float32(2.0 * math.pi / length)
    scaling = np.float32(1.0 / math.sqrt(length))
    return tuple(jnp.asarray(f(angles) * scaling).astype(BF16) for f in (np.cos, np.sin))


def on_device(n, object_field, probe_field, amplitudes, offsets, live_counts):
    probe = probe_field.reshape(2, MODES, PATCH, PATCH)
    meta = jnp.concatenate([offsets.reshape(-1), live_counts])
    meta = jnp.broadcast_to(jnp.pad(meta, (0, LANES - meta.shape[0]))[None], (8, LANES))
    cos, sin = tables(PATCH)
    return step(n, offsets, live_counts, meta, object_field, probe, amplitudes, cos, sin)


def solution(mesh):
    groups_scan = ("groups", "scan")
    placed = (
        P(None, groups_scan, None),
        P(None, "groups", None),
        P(groups_scan, None, None),
        P(groups_scan, None),
        P(groups_scan),
    )
    return jax.shard_map(
        functools.partial(on_device, mesh.shape["scan"]),
        mesh=mesh,
        in_specs=placed,
        out_specs=(P(None, groups_scan, None), P(None, groups_scan, None)),
        check_vma=False,
    )
```

```python
import functools
import math

import jax
import jax.numpy as jnp
import numpy as np
from jax import lax
from jax.experimental import pallas as pl
from jax.experimental.pallas import tpu as pltpu
from jax.sharding import PartitionSpec as P

MESH = pl.DeviceIdType.MESH
SPLIT = 4
JITTER = 8
STEP = 96
PATCH = 256
MODES = 4
STRIP = 24
LANES = 128
OWN = 512
WIN = 640
ROWS = JITTER + 2 * STEP + 72
ZTOP = 104
KROWS = 408
KCOLS = 384
F32 = jnp.float32
BF16 = jnp.bfloat16


def mult(value, of):
    return pl.multiple_of(value, of)


class Messages:
    def __init__(self, send, recv):
        self.send, self.recv, self.count, self.open = send, recv, 0, []

    def make(self, src, dst, scan, when=None):
        at = self.count
        self.count += 1
        self.last = self.recv.at[at]
        copy = pltpu.make_async_remote_copy(
            src_ref=src,
            dst_ref=dst,
            send_sem=self.send.at[at],
            recv_sem=self.recv.at[at],
            device_id={"scan": scan},
            device_id_type=MESH,
        )
        self.open.append((copy, when))
        return copy

    def drain(self):
        for copy, when in self.open:
            if when is None:
                copy.wait_send()
            else:
                pl.when(when)(copy.wait_send)
        self.open = []


def greet(peers):
    barrier = pltpu.get_barrier_semaphore()
    for peer in peers:
        pl.semaphore_signal(barrier, inc=1, device_id={"scan": peer}, device_id_type=MESH)
    pl.semaphore_wait(barrier, len(peers))


def long_way(me, step):
    line, at, q = me // 16, (me // SPLIT) % 4, me % SPLIT
    scale = 16

    def device(at_line, at_row):
        return (at_line + 8) % 8 * scale + (at_row + 8) % 4 * SPLIT + q

    def turn(row):
        row = (row + 8) % 4
        return jnp.where(jnp.logical_or(row == 0, row == 3), 0, 1)

    relay = device(line, at - step)
    origin = device(line, at + step)
    target = device(line + step * turn(at), at - step)
    source = device(line - step * turn(at + step), at + step)
    return relay, origin, target, source


def spread(n, kernel_pad, out, metas, line):
    me = lax.axis_index("scan")
    q = me % SPLIT
    line = line + jnp.where(q == SPLIT - 1, 1, 0)
    there = me // SPLIT - 2 + line
    inside = jnp.logical_and(there >= 0, there < n // SPLIT)
    start = mult(STRIP * q + STEP * (2 - line) - JITTER + ZTOP, 8)
    parts = out.shape[0]
    tall = STRIP + 2 * JITTER

    def one(col, carry):
        slot = line * SPLIT + col // SPLIT
        place = col % SPLIT
        top = metas[slot, 0, 2 * place]
        left = metas[slot, 0, 2 * place + 1]
        weight = jnp.where(jnp.logical_and(inside, place < metas[slot, 0, 8]), 1.0, 0.0).astype(F32)
        ahead = jnp.clip(STEP * there - top + JITTER, 0, 2 * JITTER)
        base = mult((STEP * col + 40) // LANES * LANES, LANES)
        shift = jnp.clip(left - base, 0, LANES)
        for part in range(parts):
            value = kernel_pad[part, pl.ds(start, tall), :]
            value = pltpu.roll(value, (tall - ahead) % tall, 0)[0:STRIP]
            value = pltpu.roll(value, shift, 1) * weight
            out[part, :, pl.ds(base, KCOLS)] += value
        return carry

    lax.fori_loop(0, 16, one, 0, unroll=4)


def step_kernel(
    n, offsets, live, meta, obj, probe_hbm, amps_hbm, cos, sin, new_obj, new_probe,
    metas_in, metas, probe, amps, win, relay_in, grad, patch, share, bright, sums9, ta, tb,
    w0, w1, w2, w3, h0, h1, h2, h3, f0, f1, f2, f3,
    q_in, sib_in, t2_in, t1_in, t8_in, back_in, far_in, piece, q_sib, acc, minus_in, plus_in, y_in, hold_t1, hold_far,
    tile, dp, dp_in, kmine, ksib, kk, kpad, illum, place, dobj, vec, vec1, vec2,
    send, recv, ysem, kysem, kxsem, v1sem, v2sem, bsend, dpsem, psem, lsem,
    gsend, ownsem, aheadsem, relaysem, finalsem, tailsem, mrecv, msem, holdsem,
):
    me = lax.axis_index("scan")
    q = me % SPLIT
    core = me % 2
    first = me - q
    row = me // SPLIT
    rows_all = n // SPLIT
    up = (me - SPLIT + n) % n
    down = (me + SPLIT) % n
    sibling = me + 1 - 2 * core
    side = 8
    x, y = me // (2 * side), (me // 2) % side
    msg = Messages(send, recv)

    def chip(at_x, at_y, at_core):
        return ((at_x % side) * side + at_y % side) * 2 + at_core

    def columns(quarter):
        return pl.ds(mult(768 * (quarter // 2) + OWN * (quarter % 2), LANES), OWN)

    def rows(start, size):
        return pl.ds(mult(start, 8), size)

    load_probe = pltpu.make_async_copy(probe_hbm, probe, lsem.at[0])
    load_probe.start()
    load_amps = pltpu.make_async_copy(amps_hbm, amps, lsem.at[1])
    load_amps.start()
    peers = [(first + SPLIT * e + k + 2 * n) % n for e in (-2, -1, 1, 2) for k in range(SPLIT)]
    peers += [chip(x + k, y, cc) for k in range(1, side) for cc in range(2)]
    peers += [chip(x, y + k, cc) for k in range(1, side) for cc in range(2)]
    peers += [sibling]
    greet(peers)

    sends = []

    def put(src, dst, recv_sem, there, when=None):
        copy = pltpu.make_async_remote_copy(
            src_ref=src,
            dst_ref=dst,
            send_sem=gsend.at[len(sends)],
            recv_sem=recv_sem,
            device_id={"scan": there},
            device_id_type=MESH,
        )
        sends.append((copy, when))
        if when is None:
            copy.start()
        else:
            pl.when(when)(copy.start)

    def landing(quarter, start, size=STRIP):
        return win.at[:, rows(start, size), pl.ds(mult(LANES * (quarter % 2), LANES), OWN)]

    for e in (-1, 0, 1, 2):
        for k in range(SPLIT):
            if e or k:
                there = (first + SPLIT * e + (q + k) % SPLIT + n) % n
                put(meta, metas_in.at[(2 - e) * SPLIT + q], mrecv, there)
    relay, origin, target, source = long_way(me, -1)
    middle = jnp.logical_or(q == 1, q == 2)
    middle_at = jnp.clip(q - 1, 0, 1)
    around = [(q + k) % SPLIT for k in range(SPLIT)]
    for there in around:
        block = obj.at[:, :, columns(there)]
        put(block, relay_in.at[middle_at], relaysem.at[middle_at], relay - q + there, when=middle)
        put(block, landing(there, JITTER + STEP + STRIP * q), aheadsem.at[q], (first - SPLIT + there + n) % n)
    for there in around[1:]:
        block = obj.at[:, :, columns(there)]
        put(block, landing(there, JITTER + STRIP * q), ownsem.at[q], first + there)
    for there in around:
        block = obj.at[:, pl.ds(STRIP - JITTER, JITTER), columns(there)]
        put(block, landing(there, 0, JITTER), tailsem, (first + SPLIT + there) % n, when=q == SPLIT - 1)
    own_at = mult(LANES * core, LANES)
    own_cols = pl.ds(own_at, OWN)
    sib_cols = pl.ds(mult(OWN * (1 - core), LANES), LANES)
    win[:, rows(JITTER + STRIP * q, STRIP), own_cols] = obj[:, :, columns(q)]
    metas_in[2 * SPLIT + q] = meta[...]

    c, s = cos[...], sin[...]
    ta[0:256, 0:256] = c
    ta[0:256, 256:512] = s
    ta[256:512, 0:256] = -s
    ta[256:512, 256:512] = c
    tb[0:256, 0:256] = c
    tb[0:256, 256:512] = -s
    tb[256:512, 0:256] = s
    tb[256:512, 256:512] = c
    grad[...] = jnp.zeros_like(grad)
    sums9[...] = jnp.zeros_like(sums9)
    kpad[...] = jnp.zeros_like(kpad)
    illum[...] = jnp.zeros_like(illum)
    place[...] = jnp.zeros_like(place)
    dobj[...] = jnp.zeros_like(dobj)
    win[:, ROWS:, :] = jnp.zeros((2, 16, WIN), F32)
    load_probe.wait()
    light = jnp.zeros((PATCH, PATCH), F32)
    for m in range(MODES):
        light = light + (probe[0, m] * probe[0, m] + probe[1, m] * probe[1, m])
    kpad[0, ZTOP : ZTOP + PATCH, 0:PATCH] = light

    def arrived(ref, sem):
        return pltpu.make_async_copy(ref, ref, sem)

    def border(start, size):
        mine = pl.ds(mult(LANES * core + 384 * (1 - core), LANES), LANES)
        src = win.at[:, pl.ds(start, size), mine]
        dst = win.at[:, pl.ds(start, size), pl.ds(mult(OWN * core, LANES), LANES)]
        copy = msg.make(src, dst, sibling)
        copy.start()
        return copy

    def far_on(j):
        arrived(relay_in.at[j - 1], relaysem.at[j - 1]).wait()
        put(relay_in.at[j - 1], landing(q, JITTER + 2 * STEP + STRIP * j), finalsem.at[j], target)

    for j in range(SPLIT):
        pl.when(q != j)(arrived(landing(q, JITTER + STRIP * j), ownsem.at[j]).wait)
        if j == 0:
            arrived(landing(q, JITTER + STEP), aheadsem.at[0]).wait()
            put(landing(q, JITTER + STEP), landing(q, JITTER + 2 * STEP), finalsem.at[0], up)
            far_on(1)
        if j == 1:
            far_on(2)
    borders = [border(JITTER, STEP)]
    arrived(landing(q, 0, JITTER), tailsem).wait()
    borders.append(border(0, JITTER))
    for j in range(1, SPLIT):
        arrived(landing(q, JITTER + STEP + STRIP * j), aheadsem.at[j]).wait()
    borders.append(border(JITTER + STEP, STEP))
    for j in range(3):
        arrived(landing(q, JITTER + 2 * STEP + STRIP * j), finalsem.at[j]).wait()
    borders.append(border(JITTER + 2 * STEP, 72))
    arrived(metas_in.at[pl.ds(0, 15)], mrecv).wait()
    to_smem = pltpu.make_async_copy(metas_in, metas, msem)
    to_smem.start()
    load_amps.wait()
    for copy in borders:
        copy.wait_recv()

    def clear_outside(ref):
        @pl.when(row == 0)
        def _():
            ref[:, 0:JITTER, :] = jnp.zeros((2, JITTER, WIN), F32)

        @pl.when(row == rows_all - 1)
        def _():
            ref[:, JITTER + STEP : JITTER + 2 * STEP, :] = jnp.zeros((2, STEP, WIN), F32)

        @pl.when(row >= rows_all - 2)
        def _():
            ref[:, JITTER + 2 * STEP : ROWS, :] = jnp.zeros((2, 72, WIN), F32)

    msg.drain()
    for copy, when in sends:
        if when is None:
            copy.wait_send()
        else:
            pl.when(when)(copy.wait_send)
    clear_outside(win)

    wave, half_done, far = (w0, w1, w2, w3), (h0, h1, h2, h3), (f0, f1, f2, f3)
    chunk = 32
    chunks = PATCH // chunk
    slab = chunk + 2 * JITTER

    def visit(p, carry):
        ahead = jnp.clip(offsets[p, 0] - (STEP * row - JITTER), 0, 2 * JITTER)
        base = mult((STEP * p + 40) // LANES * LANES, LANES)
        shift = jnp.clip(offsets[p, 1] - STEP * SPLIT * q - base, 0, LANES)
        weight = jnp.where(p < live[0], 1.0, 0.0).astype(F32)
        steps = [slice(i * chunk, (i + 1) * chunk) for i in range(chunks)]
        lows = [slice(PATCH + i * chunk, PATCH + (i + 1) * chunk) for i in range(chunks)]
        left_half, right_half = slice(0, PATCH), slice(PATCH, 2 * PATCH)

        def across(table, m):
            z = jnp.dot(table[...], wave[m][...], preferred_element_type=F32)
            half_done[m][:, left_half] = z[left_half].astype(BF16)
            half_done[m][:, right_half] = z[right_half].astype(BF16)

        def along(table, m):
            far[m][...] = jnp.dot(half_done[m][...], table[...], preferred_element_type=F32)

        for i, at in enumerate(steps):
            for part in range(2):
                v = win[part, i * chunk : i * chunk + slab, pl.ds(base, KCOLS)]
                v = pltpu.roll(v, (slab - ahead) % slab, 0)[0:chunk]
                patch[part, at, :] = pltpu.roll(v, KCOLS - shift, 1)[:, 0:PATCH]
        for m in range(MODES):
            for at, low in zip(steps, lows):
                pr, pi = probe[0, m, at, :], probe[1, m, at, :]
                o_re, o_im = patch[0, at, :], patch[1, at, :]
                wave[m][at, :] = (pr * o_re - pi * o_im).astype(BF16)
                wave[m][low, :] = (pr * o_im + pi * o_re).astype(BF16)
            across(ta, m)
        for m in range(MODES):
            along(tb, m)
            for at in steps:
                fr, fi = far[m][at, left_half], far[m][at, right_half]
                power = fr * fr + fi * fi
                bright[at, :] = power if m == 0 else bright[at, :] + power
        for m in range(MODES):
            for at, low in zip(steps, lows):
                if m == 0:
                    root = jnp.maximum(jnp.sqrt(bright[at, :]), 0.5)
                    factor = (amps[p, at, :] / root - 1.0) * weight
                    bright[at, :] = factor
                else:
                    factor = bright[at, :]
                wave[m][at, :] = (far[m][at, left_half] * factor).astype(BF16)
                wave[m][low, :] = (far[m][at, right_half] * factor).astype(BF16)
            across(tb, m)
        for m in range(MODES):
            along(ta, m)
            for at in steps:
                pr, pi = probe[0, m, at, :], probe[1, m, at, :]
                o_re, o_im = patch[0, at, :], patch[1, at, :]
                cr, ci = far[m][at, left_half], far[m][at, right_half]
                g_re = pr * cr + pi * ci
                g_im = pr * ci - pi * cr
                if m > 0:
                    g_re = g_re + share[0, at, :]
                    g_im = g_im + share[1, at, :]
                share[0, at, :] = g_re
                share[1, at, :] = g_im
                sums9[m, at, :] += o_re * cr + o_im * ci
                sums9[MODES + m, at, :] += o_re * ci - o_im * cr
        blank = jnp.zeros((chunk, KCOLS - PATCH), F32)
        below = jnp.zeros((2 * JITTER, KCOLS), F32)
        for i, at in enumerate(steps):
            o_re, o_im = patch[0, at, :], patch[1, at, :]
            sums9[2 * MODES, at, :] += (o_re * o_re + o_im * o_im) * weight
            for part in range(2):
                v = pltpu.roll(jnp.concatenate([share[part, at, :], blank], 1), shift, 1)
                v = pltpu.roll(jnp.concatenate([v, below], 0), ahead, 0)
                grad[part, i * chunk : i * chunk + slab, pl.ds(base, KCOLS)] += v
        return carry

    lax.fori_loop(0, SPLIT, visit, 0)
    clear_outside(grad)

    to_sib = msg.make(grad.at[:, pl.ds(0, ROWS), sib_cols], sib_in, sibling)
    to_sib.start()
    for at_band in range(PATCH // 8):
        yy = (at_band // 2) % 8
        for at_lane in range(2):
            xx = (at_band // 16) * 4 + (at_band % 2) * 2 + at_lane
            at_rows = slice(8 * at_band, 8 * at_band + 8)
            at_cols = slice(LANES * at_lane, LANES * at_lane + LANES)
            for k in range(2):
                for i, m in enumerate((2 * k, 2 * k + 1, MODES + 2 * k, MODES + 2 * k + 1, 8)):
                    q_in[k, xx, yy, i] = sums9[m, at_rows, at_cols]
    chunks = [(x + k) % side for k in (4, 5, 3, 6, 2, 7, 1, 0)]
    q_copies = []
    for at in chunks:
        copy = msg.make(q_in.at[1 - core, at], q_sib.at[at], sibling)
        copy.start()
        q_copies.append(copy)
    relay, origin, target, source = long_way(me, 1)

    band = (x // 4) * 16 + y * 2 + (x // 2) % 2
    lane = x % 2
    out_mode = x // 2
    out_band = (x % 2) * 16 + y * 2 + core
    p_tile = probe[:, pl.ds(2 * core, 2), pl.ds(mult(8 * band, 8), 8), pl.ds(mult(LANES * lane, LANES), LANES)]

    to_sib.wait_recv()
    edge = pl.ds(mult(LANES * core + 384 * (1 - core), LANES), LANES)
    grad[:, 0:ROWS, edge] += sib_in[...]

    def sums(start):
        return grad.at[:, pl.ds(start, STRIP), own_cols]

    def add_sibling(i):
        q_copies[i].wait_recv()
        acc[chunks[i]] = q_in[core, chunks[i]] + q_sib[chunks[i]]

    halves = side // 2

    def send_chain(way, i):
        which = (i % 2 if way < 0 else 1 - i % 2) * halves
        reach = (4 if i % 2 == 0 else 3) - i // 2
        dest = (x + way * reach + side) % side
        copy = msg.make(
            acc.at[dest, pl.ds(which, halves)],
            (minus_in if way < 0 else plus_in).at[i],
            chip(x + way + side, y, core),
        )
        copy.start()
        return copy

    chains = {}
    add_sibling(0)
    chains[-1, 0], chains[1, 0] = send_chain(-1, 0), send_chain(1, 0)
    add_sibling(1)
    chains[-1, 1] = send_chain(-1, 1)
    add_sibling(2)
    chains[1, 1] = send_chain(1, 1)
    far_out = []
    for j in (1, 2):
        copy = msg.make(sums(JITTER + 2 * STEP + STRIP * j), back_in.at[j - 1], relay)
        copy.start()
        far_out.append(copy)
    t2 = msg.make(sums(JITTER + 2 * STEP), t2_in, down)
    t2.start()
    t8 = msg.make(grad.at[:, pl.ds(0, JITTER), own_cols], t8_in, up)
    t8.start()

    at_row = (me // SPLIT) % 4
    crossing = at_row == 3
    holder = at_row == 0
    turning = jnp.logical_or(at_row == 1, at_row == 2)
    far_holder = at_row <= 1
    below = x * 2 * side + (at_row + 1) % 4 * SPLIT + q
    beside = chip(x + 1, y, core)

    def start_t1(j):
        src = sums(JITTER + STEP + STRIP * j)
        t1[j] = msg.make(src, t1_in.at[j], below, when=jnp.logical_not(crossing))
        final_sem = msg.last
        pl.when(jnp.logical_not(crossing))(t1[j].start)
        copy = msg.make(src, hold_t1.at[j], below, when=crossing)
        pl.when(crossing)(copy.start)
        held.append((copy, holder, hold_t1.at[j], t1_in.at[j], final_sem))

    def pass_far(j):
        there = x * 2 * side + (at_row + 3) % 4 * SPLIT + q
        final = msg.make(back_in.at[j], far_in.at[j], there, when=jnp.logical_not(turning))
        final_sem = msg.last
        pl.when(jnp.logical_not(turning))(final.start)
        copy = msg.make(back_in.at[j], hold_far.at[j], there, when=turning)
        pl.when(turning)(copy.start)
        held.append((copy, far_holder, hold_far.at[j], far_in.at[j], final_sem))
        return final

    def release(i):
        copy, here, src, dst, final_sem = held[i]
        pl.when(here)(copy.wait_recv)
        onward = pltpu.make_async_remote_copy(
            src_ref=src,
            dst_ref=dst,
            send_sem=holdsem.at[i],
            recv_sem=final_sem,
            device_id={"scan": beside},
            device_id_type=MESH,
        )
        pl.when(here)(onward.start)
        msg.open.append((onward, here))

    t1, held = {}, []
    start_t1(3)
    for i in range(3, 8):
        add_sibling(i)

    def x_step(i):
        for way, arrived in ((-1, minus_in), (1, plus_in)):
            which = (i % 2 if way < 0 else 1 - i % 2) * halves
            reach = (4 if i % 2 == 0 else 3) - 1 - i // 2
            dest = (x + way * reach + side) % side
            chains[way, i].wait_recv()
            acc[dest, which : which + halves] += arrived[i]
            if reach > 0:
                chains[way, i + 2] = send_chain(way, i + 2)

    to_smem.wait()
    x_step(0)
    start_t1(1)
    spread(n, kpad.at[pl.ds(0, 1)], illum, metas, 0)
    x_step(1)
    start_t1(2)
    spread(n, kpad.at[pl.ds(0, 1)], illum, metas, 1)
    x_step(2)
    t2.wait_recv()
    grad[:, JITTER + STEP : JITTER + STEP + STRIP, own_cols] += t2_in[...]
    start_t1(0)
    x_step(3)
    far_final = []
    for j in range(2):
        far_out[j].wait_recv()
        far_final.append(pass_far(j))
    x_step(4)
    spread(n, kpad.at[pl.ds(0, 1)], illum, metas, 2)
    x_step(5)
    x_step(6)

    y_copies = []
    for k in range(1, side):
        copy = pltpu.make_async_remote_copy(
            src_ref=acc.at[x, (y + k) % side],
            dst_ref=y_in.at[k - 1],
            send_sem=bsend.at[k - 1],
            recv_sem=ysem,
            device_id={"scan": chip(x, y + k, core)},
            device_id_type=MESH,
        )
        copy.start()
        y_copies.append(copy)
    for i in range(len(held)):
        release(i)
    pltpu.make_async_copy(y_in, y_in, ysem).wait()
    tile[...] = acc[x, y] + jnp.sum(y_in[...], 0)
    norm = tile[4]
    inverse = norm + 1.0
    k_re = jnp.zeros((8, LANES), F32)
    k_im = jnp.zeros((8, LANES), F32)
    s_vv = jnp.zeros((8, LANES), F32)
    s_vc = jnp.zeros((8, LANES), F32)
    for m in range(2):
        g_re, g_im = tile[m], tile[2 + m]
        d_re, d_im = g_re / inverse, g_im / inverse
        dp[m, 0] = d_re
        dp[m, 1] = d_im
        p_re, p_im = p_tile[0, m], p_tile[1, m]
        k_re = k_re + (p_re * d_re + p_im * d_im)
        k_im = k_im + (p_re * d_im - p_im * d_re)
        s_vv = s_vv + (d_re * d_re + d_im * d_im) * norm
        s_vc = s_vc + (d_re * g_re + d_im * g_im)
    kmine[0] = k_re
    kmine[1] = k_im
    k_copy = msg.make(kmine.at[1 - core], ksib, sibling)
    k_copy.start()

    dp_sends = []
    for m in range(2):
        dest = chip(2 * (2 * core + m) + x // 4, y, (x // 2) % 2)
        away = dest != me
        copy = pltpu.make_async_remote_copy(
            src_ref=dp.at[m],
            dst_ref=dp_in.at[lane],
            send_sem=bsend.at[21 + m],
            recv_sem=dpsem.at[lane],
            device_id={"scan": dest},
            device_id_type=MESH,
        )
        pl.when(away)(copy.start)
        dp_sends.append((copy, away))

        @pl.when(jnp.logical_not(away))
        def _():
            dp_in[lane] = dp[m]

    k_copy.wait_recv()
    kk[core, x, y] = kmine[core] + ksib[...]
    ky_copies = []
    for k in range(1, side):
        copy = pltpu.make_async_remote_copy(
            src_ref=kk.at[core, x, y],
            dst_ref=kk.at[core, x, y],
            send_sem=bsend.at[7 + k - 1],
            recv_sem=kysem,
            device_id={"scan": chip(x, y + k, core)},
            device_id_type=MESH,
        )
        copy.start()
        ky_copies.append(copy)

    pltpu.make_async_copy(kk.at[0, 0, pl.ds(0, 7)], kk.at[0, 0, pl.ds(0, 7)], kysem).wait()
    kx_copies = []
    for k in range(1, side):
        copy = pltpu.make_async_remote_copy(
            src_ref=kk.at[core, x],
            dst_ref=kk.at[core, x],
            send_sem=bsend.at[14 + k - 1],
            recv_sem=kxsem,
            device_id={"scan": chip(x + k, y, core)},
            device_id_type=MESH,
        )
        copy.start()
        kx_copies.append(copy)
    pieces = []
    for j in (3, 1, 2, 0):
        t1[j].wait_recv()
        lo = JITTER + STRIP * j
        grad[:, lo : lo + STRIP, own_cols] += t1_in[j]
        if j == 3:
            t8.wait_recv()
            grad[:, STEP : STEP + JITTER, own_cols] += t8_in[...]
        if j in (1, 2):
            far_final[j - 1].wait_recv()
            grad[:, lo : lo + STRIP, own_cols] += far_in[j - 1]
        slot = (j - q + SPLIT) % SPLIT
        copy = pltpu.make_async_remote_copy(
            src_ref=grad.at[:, pl.ds(lo, STRIP), own_cols],
            dst_ref=piece.at[slot],
            send_sem=bsend.at[23 + j],
            recv_sem=psem.at[slot],
            device_id={"scan": first + j},
            device_id_type=MESH,
        )
        pl.when(q != j)(copy.start)
        pieces.append((copy, q != j))

    piece[0] = grad[:, pl.ds(mult(JITTER + STRIP * q, 8), STRIP), own_cols]

    pltpu.make_async_copy(kk.at[0, pl.ds(0, 7)], kk.at[0, pl.ds(0, 7)], kxsem).wait()
    ks_copy = msg.make(kk.at[core], kk.at[core], sibling)
    ks_copy.start()

    for k in range(SPLIT):
        if k > 0:
            pltpu.make_async_copy(piece.at[k], piece.at[k], psem.at[k]).wait()
        source = (q - k + SPLIT) % SPLIT
        at = pl.ds(mult(768 * (source // 2) + OWN * (source % 2), LANES), OWN)
        dobj[:, :, at] += piece[k]
    lit = illum[0]
    g_re, g_im = dobj[0], dobj[1]
    o_re, o_im = obj[0], obj[1]
    d_re, d_im = g_re / (lit + 1.0), g_im / (lit + 1.0)
    s_uu = jnp.sum((d_re * d_re + d_im * d_im) * lit)
    s_uc = jnp.sum(d_re * g_re + d_im * g_im)
    dobj[0] = d_re
    dobj[1] = d_im

    ks_copy.wait_recv()
    for at_band in range(PATCH // 8):
        for at_lane in range(2):
            xx = (at_band // 16) * 4 + (at_band % 2) * 2 + at_lane
            yy = (at_band // 2) % 8
            rows = slice(ZTOP + 8 * at_band, ZTOP + 8 * at_band + 8)
            cols = slice(LANES * at_lane, LANES * at_lane + LANES)
            kpad[0, rows, cols] = kk[0, xx, yy]
            kpad[1, rows, cols] = kk[1, xx, yy]
    for line in range(3):
        spread(n, kpad, place, metas, line)
    d_re, d_im = dobj[0], dobj[1]
    s_uv = jnp.sum(
        place[0] * (d_re * o_re + d_im * o_im) - place[1] * (d_re * o_im - d_im * o_re)
    )

    at = lax.broadcasted_iota(jnp.int32, (8, LANES), 1)
    own_sums = jnp.zeros((8, LANES), F32)
    for i, value in enumerate((s_uu, s_uv, jnp.sum(s_vv), s_uc, jnp.sum(s_vc))):
        own_sums = jnp.where(at == i, value, own_sums)
    vec[...] = own_sums
    v1_copies = []
    for k in range(1, 2 * side):
        copy = pltpu.make_async_remote_copy(
            src_ref=vec.at[pl.ds(0, 1)],
            dst_ref=vec1.at[pl.ds(k - 1, 1)],
            send_sem=bsend.at[27 + k - 1],
            recv_sem=v1sem,
            device_id={"scan": chip(x, y + k // 2, (core + k) % 2)},
            device_id_type=MESH,
        )
        copy.start()
        v1_copies.append(copy)
    pltpu.make_async_copy(vec1.at[pl.ds(0, 15)], vec1.at[pl.ds(0, 15)], v1sem).wait()
    for copy in v1_copies:
        copy.wait_send()
    vec[...] = own_sums + jnp.sum(vec1[0:15, :], 0, keepdims=True)
    v2_copies = []
    for k in range(1, side):
        copy = pltpu.make_async_remote_copy(
            src_ref=vec.at[pl.ds(0, 1)],
            dst_ref=vec2.at[pl.ds(k - 1, 1)],
            send_sem=bsend.at[42 + k - 1],
            recv_sem=v2sem,
            device_id={"scan": chip(x + k, y, core)},
            device_id_type=MESH,
        )
        copy.start()
        v2_copies.append(copy)
    for at_lane in range(2):
        source = chip((x % 2) * 4 + core * 2 + at_lane, y, x // 4)
        arrived = pltpu.make_async_copy(dp_in.at[at_lane], dp_in.at[at_lane], dpsem.at[at_lane])
        pl.when(source != me)(arrived.wait)
    pltpu.make_async_copy(vec2.at[pl.ds(0, 7)], vec2.at[pl.ds(0, 7)], v2sem).wait()
    totals = vec[...] + jnp.sum(vec2[0:7, :], 0, keepdims=True)
    uu, uv, vv, uc, vc = (totals[0:1, i : i + 1] for i in range(5))
    a = 1.1 * uu + 1e-06
    d = 1.1 * vv + 1e-06
    det = a * d - uv * uv
    rate_obj = (uc * d - uv * vc) / det
    rate_probe = (a * vc - uv * uc) / det
    for part in range(2):
        new_obj[part] = obj[part] + rate_obj * dobj[part]
        for at_lane in range(2):
            cols = slice(LANES * at_lane, LANES * at_lane + LANES)
            new_probe[part, :, cols] = probe[part, out_mode, pl.ds(mult(8 * out_band, 8), 8), cols] + rate_probe * dp_in[at_lane, part]

    msg.drain()
    for copy in y_copies + ky_copies + kx_copies + v2_copies:
        copy.wait_send()
    for copy, when in dp_sends + pieces:
        pl.when(when)(copy.wait_send)


def step(n, offsets, live, meta, obj, probe, amps, cos, sin):
    vmem = pl.BlockSpec(memory_space=pltpu.VMEM)
    smem = pl.BlockSpec(memory_space=pltpu.SMEM)
    hbm = pl.BlockSpec(memory_space=pl.ANY)
    dma = pltpu.SemaphoreType.DMA
    columns = obj.shape[2]

    def f32(*shape):
        return pltpu.VMEM(shape, F32)

    return pl.pallas_call(
        functools.partial(step_kernel, n),
        out_shape=(
            jax.ShapeDtypeStruct((2, STRIP, columns), F32),
            jax.ShapeDtypeStruct((2, 8, PATCH), F32),
        ),
        in_specs=[smem, smem, vmem, vmem, hbm, hbm, vmem, vmem],
        out_specs=[vmem] * 2,
        scratch_shapes=[
            pltpu.VMEM((4 * SPLIT, 8, LANES), jnp.int32),
            pltpu.SMEM((4 * SPLIT, 8, LANES), jnp.int32),
            f32(2, MODES, PATCH, PATCH),
            f32(SPLIT, PATCH, PATCH),
            f32(2, ROWS + 16, WIN),
            f32(2, 2, STRIP, OWN),
            f32(2, ROWS + 16, WIN),
            f32(2, PATCH, PATCH),
            f32(2, PATCH, PATCH),
            f32(PATCH, PATCH),
            f32(2 * MODES + 1, PATCH, PATCH),
            pltpu.VMEM((2 * PATCH, 2 * PATCH), BF16),
            pltpu.VMEM((2 * PATCH, 2 * PATCH), BF16),
            *[pltpu.VMEM((2 * PATCH, PATCH), BF16) for m in range(MODES)],
            *[pltpu.VMEM((PATCH, 2 * PATCH), BF16) for m in range(MODES)],
            *[f32(PATCH, 2 * PATCH) for m in range(MODES)],
            f32(2, 8, 8, 5, 8, LANES),
            f32(2, ROWS, LANES),
            f32(2, STRIP, OWN),
            f32(4, 2, STRIP, OWN),
            f32(2, JITTER, OWN),
            f32(2, 2, STRIP, OWN),
            f32(2, 2, STRIP, OWN),
            f32(4, 2, STRIP, OWN),
            f32(8, 8, 5, 8, LANES),
            f32(8, 8, 5, 8, LANES),
            f32(7, 4, 5, 8, LANES),
            f32(7, 4, 5, 8, LANES),
            f32(7, 5, 8, LANES),
            f32(4, 2, STRIP, OWN),
            f32(2, 2, STRIP, OWN),
            f32(5, 8, LANES),
            f32(2, 2, 8, LANES),
            f32(2, 2, 8, LANES),
            f32(2, 8, LANES),
            f32(8, LANES),
            f32(2, 8, 8, 8, LANES),
            f32(2, KROWS, KCOLS),
            f32(1, STRIP, columns),
            f32(2, STRIP, columns),
            f32(2, STRIP, columns),
            f32(8, LANES),
            f32(16, LANES),
            f32(8, LANES),
            dma((48,)),
            dma((48,)),
            dma,
            dma,
            dma,
            dma,
            dma,
            dma((50,)),
            dma((2,)),
            dma((4,)),
            dma((2,)),
            dma((40,)),
            dma((4,)),
            dma((4,)),
            dma((2,)),
            dma((3,)),
            dma,
            dma,
            dma,
            dma((6,)),
        ],
        compiler_params=pltpu.CompilerParams(collective_id=0, has_side_effects=True),
        name="step",
    )(offsets, live, meta, obj, probe, amps, cos, sin)


def tables(length):
    numbers = np.arange(length, dtype=np.int64)
    angles = (numbers[:, None] * numbers[None, :] % length).astype(np.float32)
    angles = angles * np.float32(2.0 * math.pi / length)
    scaling = np.float32(1.0 / math.sqrt(length))
    return tuple(jnp.asarray(f(angles) * scaling).astype(BF16) for f in (np.cos, np.sin))


def on_device(n, object_field, probe_field, amplitudes, offsets, live_counts):
    probe = probe_field.reshape(2, MODES, PATCH, PATCH)
    meta = jnp.concatenate([offsets.reshape(-1), live_counts])
    meta = jnp.broadcast_to(jnp.pad(meta, (0, LANES - meta.shape[0]))[None], (8, LANES))
    cos, sin = tables(PATCH)
    return step(n, offsets, live_counts, meta, object_field, probe, amplitudes, cos, sin)


def solution(mesh):
    groups_scan = ("groups", "scan")
    placed = (
        P(None, groups_scan, None),
        P(None, "groups", None),
        P(groups_scan, None, None),
        P(groups_scan, None),
        P(groups_scan),
    )
    return jax.shard_map(
        functools.partial(on_device, mesh.shape["scan"]),
        mesh=mesh,
        in_specs=placed,
        out_specs=(P(None, groups_scan, None), P(None, groups_scan, None)),
        check_vma=False,
    )
```

```python
import functools
import math

import jax
import jax.numpy as jnp
import numpy as np
from jax import lax
from jax.experimental import pallas as pl
from jax.experimental.pallas import tpu as pltpu
from jax.sharding import PartitionSpec as P

MESH = pl.DeviceIdType.MESH
SPLIT = 4
JITTER = 8
STEP = 96
PATCH = 256
MODES = 4
STRIP = 24
LANES = 128
OWN = 512
WIN = 640
ROWS = JITTER + 2 * STEP + 72
ZTOP = 104
KROWS = 408
KCOLS = 384
F32 = jnp.float32
BF16 = jnp.bfloat16


def mult(value, of):
    return pl.multiple_of(value, of)


class Messages:
    def __init__(self, send, recv):
        self.send, self.recv, self.count, self.open = send, recv, 0, []

    def make(self, src, dst, scan, when=None):
        at = self.count
        self.count += 1
        self.last = self.recv.at[at]
        copy = pltpu.make_async_remote_copy(
            src_ref=src,
            dst_ref=dst,
            send_sem=self.send.at[at],
            recv_sem=self.recv.at[at],
            device_id={"scan": scan},
            device_id_type=MESH,
        )
        self.open.append((copy, when))
        return copy

    def drain(self):
        for copy, when in self.open:
            if when is None:
                copy.wait_send()
            else:
                pl.when(when)(copy.wait_send)
        self.open = []


def greet(peers):
    barrier = pltpu.get_barrier_semaphore()
    for peer in peers:
        pl.semaphore_signal(barrier, inc=1, device_id={"scan": peer}, device_id_type=MESH)
    pl.semaphore_wait(barrier, len(peers))


def long_way(me, step):
    line, at, q = me // 16, (me // SPLIT) % 4, me % SPLIT
    scale = 16

    def device(at_line, at_row):
        return (at_line + 8) % 8 * scale + (at_row + 8) % 4 * SPLIT + q

    def turn(row):
        row = (row + 8) % 4
        return jnp.where(jnp.logical_or(row == 0, row == 3), 0, 1)

    relay = device(line, at - step)
    origin = device(line, at + step)
    target = device(line + step * turn(at), at - step)
    source = device(line - step * turn(at + step), at + step)
    return relay, origin, target, source


def spread(n, kernel_pad, out, metas, line):
    me = lax.axis_index("scan")
    q = me % SPLIT
    line = line + jnp.where(q == SPLIT - 1, 1, 0)
    there = me // SPLIT - 2 + line
    inside = jnp.logical_and(there >= 0, there < n // SPLIT)
    start = mult(STRIP * q + STEP * (2 - line) - JITTER + ZTOP, 8)
    parts = out.shape[0]
    tall = STRIP + 2 * JITTER

    def one(col, carry):
        slot = line * SPLIT + col // SPLIT
        place = col % SPLIT
        top = metas[slot, 0, 2 * place]
        left = metas[slot, 0, 2 * place + 1]
        weight = jnp.where(jnp.logical_and(inside, place < metas[slot, 0, 8]), 1.0, 0.0).astype(F32)
        ahead = jnp.clip(STEP * there - top + JITTER, 0, 2 * JITTER)
        base = mult((STEP * col + 40) // LANES * LANES, LANES)
        shift = jnp.clip(left - base, 0, LANES)
        for part in range(parts):
            value = kernel_pad[part, pl.ds(start, tall), :]
            value = pltpu.roll(value, (tall - ahead) % tall, 0)[0:STRIP]
            value = pltpu.roll(value, shift, 1) * weight
            out[part, :, pl.ds(base, KCOLS)] += value
        return carry

    lax.fori_loop(0, 16, one, 0, unroll=4)


def step_kernel(
    n, offsets, live, obj, probe_hbm, amps_hbm, cos, sin, obj_step, probe_out, rates,
    meta, metas_in, metas, probe, amps, win, relay_in, grad, patch, share, bright, sums9, ta, tb,
    w0, w1, w2, w3, h0, h1, h2, h3, f0, f1, f2, f3,
    q_in, sib_in, t2_in, t1_in, t8_in, back_in, far_in, piece, q_sib, acc, minus_in, plus_in, y_in, hold_t1, hold_far,
    tile, dp, dp_in, kmine, ksib, kk, kpad, illum, place, dobj, vec, vec1, vec2,
    send, recv, ysem, kysem, kxsem, v1sem, v2sem, bsend, dpsem, psem, lsem,
    gsend, ownsem, aheadsem, relaysem, finalsem, tailsem, mrecv, msem, holdsem,
):
    me = lax.axis_index("scan")
    q = me % SPLIT
    core = me % 2
    first = me - q
    row = me // SPLIT
    rows_all = n // SPLIT
    up = (me - SPLIT + n) % n
    down = (me + SPLIT) % n
    sibling = me + 1 - 2 * core
    side = 8
    x, y = me // (2 * side), (me // 2) % side
    msg = Messages(send, recv)

    def chip(at_x, at_y, at_core):
        return ((at_x % side) * side + at_y % side) * 2 + at_core

    def columns(quarter):
        return pl.ds(mult(768 * (quarter // 2) + OWN * (quarter % 2), LANES), OWN)

    def rows(start, size):
        return pl.ds(mult(start, 8), size)

    lanes = lax.broadcasted_iota(jnp.int32, (8, LANES), 1)
    facts = jnp.where(lanes == 2 * SPLIT, live[0], 0)
    for p in range(SPLIT):
        for i in range(2):
            facts = jnp.where(lanes == 2 * p + i, offsets[i, p], facts)
    meta[...] = facts
    load_probe = pltpu.make_async_copy(probe_hbm, probe, lsem.at[0])
    load_probe.start()
    load_amps = pltpu.make_async_copy(amps_hbm, amps, lsem.at[1])
    load_amps.start()
    peers = [(first + SPLIT * e + k + 2 * n) % n for e in (-2, -1, 1, 2) for k in range(SPLIT)]
    peers += [chip(x + k, y, cc) for k in range(1, side) for cc in range(2)]
    peers += [chip(x, y + k, cc) for k in range(1, side) for cc in range(2)]
    peers += [sibling]
    greet(peers)

    sends = []

    def put(src, dst, recv_sem, there, when=None):
        copy = pltpu.make_async_remote_copy(
            src_ref=src,
            dst_ref=dst,
            send_sem=gsend.at[len(sends)],
            recv_sem=recv_sem,
            device_id={"scan": there},
            device_id_type=MESH,
        )
        sends.append((copy, when))
        if when is None:
            copy.start()
        else:
            pl.when(when)(copy.start)

    def landing(quarter, start, size=STRIP):
        return win.at[:, rows(start, size), pl.ds(mult(LANES * (quarter % 2), LANES), OWN)]

    for e in (-1, 0, 1, 2):
        for k in range(SPLIT):
            if e or k:
                there = (first + SPLIT * e + (q + k) % SPLIT + n) % n
                put(meta, metas_in.at[(2 - e) * SPLIT + q], mrecv, there)
    relay, origin, target, source = long_way(me, -1)
    middle = jnp.logical_or(q == 1, q == 2)
    middle_at = jnp.clip(q - 1, 0, 1)
    around = [(q + k) % SPLIT for k in range(SPLIT)]
    for there in around:
        block = obj.at[:, :, columns(there)]
        put(block, relay_in.at[middle_at], relaysem.at[middle_at], relay - q + there, when=middle)
        put(block, landing(there, JITTER + STEP + STRIP * q), aheadsem.at[q], (first - SPLIT + there + n) % n)
    for there in around[1:]:
        block = obj.at[:, :, columns(there)]
        put(block, landing(there, JITTER + STRIP * q), ownsem.at[q], first + there)
    for there in around:
        block = obj.at[:, pl.ds(STRIP - JITTER, JITTER), columns(there)]
        put(block, landing(there, 0, JITTER), tailsem, (first + SPLIT + there) % n, when=q == SPLIT - 1)
    own_at = mult(LANES * core, LANES)
    own_cols = pl.ds(own_at, OWN)
    sib_cols = pl.ds(mult(OWN * (1 - core), LANES), LANES)
    win[:, rows(JITTER + STRIP * q, STRIP), own_cols] = obj[:, :, columns(q)]
    metas_in[2 * SPLIT + q] = facts

    c, s = cos[...], sin[...]
    ta[0:256, 0:256] = c
    ta[0:256, 256:512] = s
    ta[256:512, 0:256] = -s
    ta[256:512, 256:512] = c
    tb[0:256, 0:256] = c
    tb[0:256, 256:512] = -s
    tb[256:512, 0:256] = s
    tb[256:512, 256:512] = c
    grad[...] = jnp.zeros_like(grad)
    sums9[...] = jnp.zeros_like(sums9)
    kpad[...] = jnp.zeros_like(kpad)
    illum[...] = jnp.zeros_like(illum)
    place[...] = jnp.zeros_like(place)
    dobj[...] = jnp.zeros_like(dobj)
    win[:, ROWS:, :] = jnp.zeros((2, 16, WIN), F32)
    load_probe.wait()
    light = jnp.zeros((PATCH, PATCH), F32)
    for m in range(MODES):
        light = light + (probe[0, m] * probe[0, m] + probe[1, m] * probe[1, m])
    kpad[0, ZTOP : ZTOP + PATCH, 0:PATCH] = light

    def arrived(ref, sem):
        return pltpu.make_async_copy(ref, ref, sem)

    def border(start, size):
        mine = pl.ds(mult(LANES * core + 384 * (1 - core), LANES), LANES)
        src = win.at[:, pl.ds(start, size), mine]
        dst = win.at[:, pl.ds(start, size), pl.ds(mult(OWN * core, LANES), LANES)]
        copy = msg.make(src, dst, sibling)
        copy.start()
        return copy

    def far_on(j):
        arrived(relay_in.at[j - 1], relaysem.at[j - 1]).wait()
        put(relay_in.at[j - 1], landing(q, JITTER + 2 * STEP + STRIP * j), finalsem.at[j], target)

    for j in range(SPLIT):
        pl.when(q != j)(arrived(landing(q, JITTER + STRIP * j), ownsem.at[j]).wait)
        if j == 0:
            arrived(landing(q, JITTER + STEP), aheadsem.at[0]).wait()
            put(landing(q, JITTER + STEP), landing(q, JITTER + 2 * STEP), finalsem.at[0], up)
            far_on(1)
        if j == 1:
            far_on(2)
    borders = [border(JITTER, STEP)]
    arrived(landing(q, 0, JITTER), tailsem).wait()
    borders.append(border(0, JITTER))
    for j in range(1, SPLIT):
        arrived(landing(q, JITTER + STEP + STRIP * j), aheadsem.at[j]).wait()
    borders.append(border(JITTER + STEP, STEP))
    for j in range(3):
        arrived(landing(q, JITTER + 2 * STEP + STRIP * j), finalsem.at[j]).wait()
    borders.append(border(JITTER + 2 * STEP, 72))
    arrived(metas_in.at[pl.ds(0, 15)], mrecv).wait()
    to_smem = pltpu.make_async_copy(metas_in, metas, msem)
    to_smem.start()
    load_amps.wait()
    for copy in borders:
        copy.wait_recv()

    def clear_outside(ref):
        @pl.when(row == 0)
        def _():
            ref[:, 0:JITTER, :] = jnp.zeros((2, JITTER, WIN), F32)

        @pl.when(row == rows_all - 1)
        def _():
            ref[:, JITTER + STEP : JITTER + 2 * STEP, :] = jnp.zeros((2, STEP, WIN), F32)

        @pl.when(row >= rows_all - 2)
        def _():
            ref[:, JITTER + 2 * STEP : ROWS, :] = jnp.zeros((2, 72, WIN), F32)

    msg.drain()
    for copy, when in sends:
        if when is None:
            copy.wait_send()
        else:
            pl.when(when)(copy.wait_send)
    clear_outside(win)

    wave, half_done, far = (w0, w1, w2, w3), (h0, h1, h2, h3), (f0, f1, f2, f3)
    chunk = 32
    chunks = PATCH // chunk
    slab = chunk + 2 * JITTER

    def visit(p, carry):
        ahead = jnp.clip(offsets[0, p] - (STEP * row - JITTER), 0, 2 * JITTER)
        base = mult((STEP * p + 40) // LANES * LANES, LANES)
        shift = jnp.clip(offsets[1, p] - STEP * SPLIT * q - base, 0, LANES)
        weight = jnp.where(p < live[0], 1.0, 0.0).astype(F32)
        steps = [slice(i * chunk, (i + 1) * chunk) for i in range(chunks)]
        lows = [slice(PATCH + i * chunk, PATCH + (i + 1) * chunk) for i in range(chunks)]
        left_half, right_half = slice(0, PATCH), slice(PATCH, 2 * PATCH)

        def across(table, m):
            z = jnp.dot(table[...], wave[m][...], preferred_element_type=F32)
            half_done[m][:, left_half] = z[left_half].astype(BF16)
            half_done[m][:, right_half] = z[right_half].astype(BF16)

        def along(table, m):
            far[m][...] = jnp.dot(half_done[m][...], table[...], preferred_element_type=F32)

        for i, at in enumerate(steps):
            for part in range(2):
                v = win[part, i * chunk : i * chunk + slab, pl.ds(base, KCOLS)]
                v = pltpu.roll(v, (slab - ahead) % slab, 0)[0:chunk]
                patch[part, at, :] = pltpu.roll(v, KCOLS - shift, 1)[:, 0:PATCH]
        for m in range(MODES):
            for at, low in zip(steps, lows):
                pr, pi = probe[0, m, at, :], probe[1, m, at, :]
                o_re, o_im = patch[0, at, :], patch[1, at, :]
                wave[m][at, :] = (pr * o_re - pi * o_im).astype(BF16)
                wave[m][low, :] = (pr * o_im + pi * o_re).astype(BF16)
            across(ta, m)
        for m in range(MODES):
            along(tb, m)
            for at in steps:
                fr, fi = far[m][at, left_half], far[m][at, right_half]
                power = fr * fr + fi * fi
                bright[at, :] = power if m == 0 else bright[at, :] + power
        for m in range(MODES):
            for at, low in zip(steps, lows):
                if m == 0:
                    root = jnp.maximum(jnp.sqrt(bright[at, :]), 0.5)
                    factor = (amps[p, at, :] / root - 1.0) * weight
                    bright[at, :] = factor
                else:
                    factor = bright[at, :]
                wave[m][at, :] = (far[m][at, left_half] * factor).astype(BF16)
                wave[m][low, :] = (far[m][at, right_half] * factor).astype(BF16)
            across(tb, m)
        for m in range(MODES):
            along(ta, m)
            for at in steps:
                pr, pi = probe[0, m, at, :], probe[1, m, at, :]
                o_re, o_im = patch[0, at, :], patch[1, at, :]
                cr, ci = far[m][at, left_half], far[m][at, right_half]
                g_re = pr * cr + pi * ci
                g_im = pr * ci - pi * cr
                if m > 0:
                    g_re = g_re + share[0, at, :]
                    g_im = g_im + share[1, at, :]
                share[0, at, :] = g_re
                share[1, at, :] = g_im
                sums9[m, at, :] += o_re * cr + o_im * ci
                sums9[MODES + m, at, :] += o_re * ci - o_im * cr
        blank = jnp.zeros((chunk, KCOLS - PATCH), F32)
        below = jnp.zeros((2 * JITTER, KCOLS), F32)
        for i, at in enumerate(steps):
            o_re, o_im = patch[0, at, :], patch[1, at, :]
            sums9[2 * MODES, at, :] += (o_re * o_re + o_im * o_im) * weight
            for part in range(2):
                v = pltpu.roll(jnp.concatenate([share[part, at, :], blank], 1), shift, 1)
                v = pltpu.roll(jnp.concatenate([v, below], 0), ahead, 0)
                grad[part, i * chunk : i * chunk + slab, pl.ds(base, KCOLS)] += v
        return carry

    lax.fori_loop(0, SPLIT, visit, 0)
    clear_outside(grad)

    to_sib = msg.make(grad.at[:, pl.ds(0, ROWS), sib_cols], sib_in, sibling)
    to_sib.start()
    for at_band in range(PATCH // 8):
        yy = (at_band // 2) % 8
        for at_lane in range(2):
            xx = (at_band // 16) * 4 + (at_band % 2) * 2 + at_lane
            at_rows = slice(8 * at_band, 8 * at_band + 8)
            at_cols = slice(LANES * at_lane, LANES * at_lane + LANES)
            for k in range(2):
                for i, m in enumerate((2 * k, 2 * k + 1, MODES + 2 * k, MODES + 2 * k + 1, 8)):
                    q_in[k, xx, yy, i] = sums9[m, at_rows, at_cols]
    chunks = [(x + k) % side for k in (4, 5, 3, 6, 2, 7, 1, 0)]
    q_copies = []
    for at in chunks:
        copy = msg.make(q_in.at[1 - core, at], q_sib.at[at], sibling)
        copy.start()
        q_copies.append(copy)
    relay, origin, target, source = long_way(me, 1)

    band = (x // 4) * 16 + y * 2 + (x // 2) % 2
    lane = x % 2
    out_mode = x // 2
    out_band = (x % 2) * 16 + y * 2 + core
    p_tile = probe[:, pl.ds(2 * core, 2), pl.ds(mult(8 * band, 8), 8), pl.ds(mult(LANES * lane, LANES), LANES)]

    to_sib.wait_recv()
    edge = pl.ds(mult(LANES * core + 384 * (1 - core), LANES), LANES)
    grad[:, 0:ROWS, edge] += sib_in[...]

    def sums(start):
        return grad.at[:, pl.ds(start, STRIP), own_cols]

    def add_sibling(i):
        q_copies[i].wait_recv()
        acc[chunks[i]] = q_in[core, chunks[i]] + q_sib[chunks[i]]

    halves = side // 2

    def send_chain(way, i):
        which = (i % 2 if way < 0 else 1 - i % 2) * halves
        reach = (4 if i % 2 == 0 else 3) - i // 2
        dest = (x + way * reach + side) % side
        copy = msg.make(
            acc.at[dest, pl.ds(which, halves)],
            (minus_in if way < 0 else plus_in).at[i],
            chip(x + way + side, y, core),
        )
        copy.start()
        return copy

    chains = {}
    add_sibling(0)
    chains[-1, 0], chains[1, 0] = send_chain(-1, 0), send_chain(1, 0)
    add_sibling(1)
    chains[-1, 1] = send_chain(-1, 1)
    add_sibling(2)
    chains[1, 1] = send_chain(1, 1)
    far_out = []
    for j in (1, 2):
        copy = msg.make(sums(JITTER + 2 * STEP + STRIP * j), back_in.at[j - 1], relay)
        copy.start()
        far_out.append(copy)
    t2 = msg.make(sums(JITTER + 2 * STEP), t2_in, down)
    t2.start()
    t8 = msg.make(grad.at[:, pl.ds(0, JITTER), own_cols], t8_in, up)
    t8.start()

    at_row = (me // SPLIT) % 4
    crossing = at_row == 3
    holder = at_row == 0
    turning = jnp.logical_or(at_row == 1, at_row == 2)
    far_holder = at_row <= 1
    below = x * 2 * side + (at_row + 1) % 4 * SPLIT + q
    beside = chip(x + 1, y, core)

    def start_t1(j):
        src = sums(JITTER + STEP + STRIP * j)
        t1[j] = msg.make(src, t1_in.at[j], below, when=jnp.logical_not(crossing))
        final_sem = msg.last
        pl.when(jnp.logical_not(crossing))(t1[j].start)
        copy = msg.make(src, hold_t1.at[j], below, when=crossing)
        pl.when(crossing)(copy.start)
        held.append((copy, holder, hold_t1.at[j], t1_in.at[j], final_sem))

    def pass_far(j):
        there = x * 2 * side + (at_row + 3) % 4 * SPLIT + q
        final = msg.make(back_in.at[j], far_in.at[j], there, when=jnp.logical_not(turning))
        final_sem = msg.last
        pl.when(jnp.logical_not(turning))(final.start)
        copy = msg.make(back_in.at[j], hold_far.at[j], there, when=turning)
        pl.when(turning)(copy.start)
        held.append((copy, far_holder, hold_far.at[j], far_in.at[j], final_sem))
        return final

    def release(i):
        copy, here, src, dst, final_sem = held[i]
        pl.when(here)(copy.wait_recv)
        onward = pltpu.make_async_remote_copy(
            src_ref=src,
            dst_ref=dst,
            send_sem=holdsem.at[i],
            recv_sem=final_sem,
            device_id={"scan": beside},
            device_id_type=MESH,
        )
        pl.when(here)(onward.start)
        msg.open.append((onward, here))

    t1, held = {}, []
    start_t1(3)
    for i in range(3, 8):
        add_sibling(i)

    def x_step(i):
        for way, arrived in ((-1, minus_in), (1, plus_in)):
            which = (i % 2 if way < 0 else 1 - i % 2) * halves
            reach = (4 if i % 2 == 0 else 3) - 1 - i // 2
            dest = (x + way * reach + side) % side
            chains[way, i].wait_recv()
            acc[dest, which : which + halves] += arrived[i]
            if reach > 0:
                chains[way, i + 2] = send_chain(way, i + 2)

    to_smem.wait()
    x_step(0)
    start_t1(1)
    spread(n, kpad.at[pl.ds(0, 1)], illum, metas, 0)
    x_step(1)
    start_t1(2)
    spread(n, kpad.at[pl.ds(0, 1)], illum, metas, 1)
    x_step(2)
    t2.wait_recv()
    grad[:, JITTER + STEP : JITTER + STEP + STRIP, own_cols] += t2_in[...]
    x_step(3)
    far_final = []
    for j in range(2):
        far_out[j].wait_recv()
        far_final.append(pass_far(j))
    x_step(4)
    spread(n, kpad.at[pl.ds(0, 1)], illum, metas, 2)
    x_step(5)
    x_step(6)

    y_copies = []
    for k in range(1, side):
        copy = pltpu.make_async_remote_copy(
            src_ref=acc.at[x, (y + k) % side],
            dst_ref=y_in.at[k - 1],
            send_sem=bsend.at[k - 1],
            recv_sem=ysem,
            device_id={"scan": chip(x, y + k, core)},
            device_id_type=MESH,
        )
        copy.start()
        y_copies.append(copy)
    start_t1(0)
    for i in range(3):
        release(i)
    pltpu.make_async_copy(y_in, y_in, ysem).wait()
    tile[...] = acc[x, y] + jnp.sum(y_in[...], 0)
    norm = tile[4]
    inverse = norm + 1.0
    k_re = jnp.zeros((8, LANES), F32)
    k_im = jnp.zeros((8, LANES), F32)
    s_vv = jnp.zeros((8, LANES), F32)
    s_vc = jnp.zeros((8, LANES), F32)
    for m in range(2):
        g_re, g_im = tile[m], tile[2 + m]
        d_re, d_im = g_re / inverse, g_im / inverse
        dp[m, 0] = d_re
        dp[m, 1] = d_im
        p_re, p_im = p_tile[0, m], p_tile[1, m]
        k_re = k_re + (p_re * d_re + p_im * d_im)
        k_im = k_im + (p_re * d_im - p_im * d_re)
        s_vv = s_vv + (d_re * d_re + d_im * d_im) * norm
        s_vc = s_vc + (d_re * g_re + d_im * g_im)
    kmine[0] = k_re
    kmine[1] = k_im
    k_copy = msg.make(kmine.at[1 - core], ksib, sibling)
    k_copy.start()

    dp_sends = []
    for m in range(2):
        dest = chip(2 * (2 * core + m) + x // 4, y, (x // 2) % 2)
        away = dest != me
        copy = pltpu.make_async_remote_copy(
            src_ref=dp.at[m],
            dst_ref=dp_in.at[lane],
            send_sem=bsend.at[21 + m],
            recv_sem=dpsem.at[lane],
            device_id={"scan": dest},
            device_id_type=MESH,
        )
        pl.when(away)(copy.start)
        dp_sends.append((copy, away))

        @pl.when(jnp.logical_not(away))
        def _():
            dp_in[lane] = dp[m]

    k_copy.wait_recv()
    kk[core, x, y] = kmine[core] + ksib[...]
    ky_copies = []
    for k in range(1, side):
        copy = pltpu.make_async_remote_copy(
            src_ref=kk.at[core, x, y],
            dst_ref=kk.at[core, x, y],
            send_sem=bsend.at[7 + k - 1],
            recv_sem=kysem,
            device_id={"scan": chip(x, y + k, core)},
            device_id_type=MESH,
        )
        copy.start()
        ky_copies.append(copy)

    for i in range(3, 6):
        release(i)
    pltpu.make_async_copy(kk.at[0, 0, pl.ds(0, 7)], kk.at[0, 0, pl.ds(0, 7)], kysem).wait()
    kx_copies = []
    for k in range(1, side):
        copy = pltpu.make_async_remote_copy(
            src_ref=kk.at[core, x],
            dst_ref=kk.at[core, x],
            send_sem=bsend.at[14 + k - 1],
            recv_sem=kxsem,
            device_id={"scan": chip(x + k, y, core)},
            device_id_type=MESH,
        )
        copy.start()
        kx_copies.append(copy)
    pieces = []
    for j in (3, 1, 2, 0):
        t1[j].wait_recv()
        lo = JITTER + STRIP * j
        grad[:, lo : lo + STRIP, own_cols] += t1_in[j]
        if j == 3:
            t8.wait_recv()
            grad[:, STEP : STEP + JITTER, own_cols] += t8_in[...]
        if j in (1, 2):
            far_final[j - 1].wait_recv()
            grad[:, lo : lo + STRIP, own_cols] += far_in[j - 1]
        slot = (j - q + SPLIT) % SPLIT
        copy = pltpu.make_async_remote_copy(
            src_ref=grad.at[:, pl.ds(lo, STRIP), own_cols],
            dst_ref=piece.at[slot],
            send_sem=bsend.at[23 + j],
            recv_sem=psem.at[slot],
            device_id={"scan": first + j},
            device_id_type=MESH,
        )
        pl.when(q != j)(copy.start)
        pieces.append((copy, q != j))

    piece[0] = grad[:, pl.ds(mult(JITTER + STRIP * q, 8), STRIP), own_cols]

    pltpu.make_async_copy(kk.at[0, pl.ds(0, 7)], kk.at[0, pl.ds(0, 7)], kxsem).wait()
    ks_copy = msg.make(kk.at[core], kk.at[core], sibling)
    ks_copy.start()

    for k in range(SPLIT):
        if k > 0:
            pltpu.make_async_copy(piece.at[k], piece.at[k], psem.at[k]).wait()
        source = (q - k + SPLIT) % SPLIT
        at = pl.ds(mult(768 * (source // 2) + OWN * (source % 2), LANES), OWN)
        dobj[:, :, at] += piece[k]
    lit = illum[0]
    g_re, g_im = dobj[0], dobj[1]
    o_re, o_im = obj[0], obj[1]
    d_re, d_im = g_re / (lit + 1.0), g_im / (lit + 1.0)
    s_uu = jnp.sum((d_re * d_re + d_im * d_im) * lit)
    s_uc = jnp.sum(d_re * g_re + d_im * g_im)
    dobj[0] = d_re
    dobj[1] = d_im

    ks_copy.wait_recv()
    for at_band in range(PATCH // 8):
        for at_lane in range(2):
            xx = (at_band // 16) * 4 + (at_band % 2) * 2 + at_lane
            yy = (at_band // 2) % 8
            rows = slice(ZTOP + 8 * at_band, ZTOP + 8 * at_band + 8)
            cols = slice(LANES * at_lane, LANES * at_lane + LANES)
            kpad[0, rows, cols] = kk[0, xx, yy]
            kpad[1, rows, cols] = kk[1, xx, yy]
    for line in range(3):
        spread(n, kpad, place, metas, line)
    d_re, d_im = dobj[0], dobj[1]
    s_uv = jnp.sum(
        place[0] * (d_re * o_re + d_im * o_im) - place[1] * (d_re * o_im - d_im * o_re)
    )

    at = lax.broadcasted_iota(jnp.int32, (8, LANES), 1)
    own_sums = jnp.zeros((8, LANES), F32)
    for i, value in enumerate((s_uu, s_uv, jnp.sum(s_vv), s_uc, jnp.sum(s_vc))):
        own_sums = jnp.where(at == i, value, own_sums)
    vec[...] = own_sums
    v1_copies = []
    for k in range(1, 2 * side):
        copy = pltpu.make_async_remote_copy(
            src_ref=vec.at[pl.ds(0, 1)],
            dst_ref=vec1.at[pl.ds(k - 1, 1)],
            send_sem=bsend.at[27 + k - 1],
            recv_sem=v1sem,
            device_id={"scan": chip(x, y + k // 2, (core + k) % 2)},
            device_id_type=MESH,
        )
        copy.start()
        v1_copies.append(copy)
    pltpu.make_async_copy(vec1.at[pl.ds(0, 15)], vec1.at[pl.ds(0, 15)], v1sem).wait()
    for copy in v1_copies:
        copy.wait_send()
    vec[...] = own_sums + jnp.sum(vec1[0:15, :], 0, keepdims=True)
    v2_copies = []
    for k in range(1, side):
        copy = pltpu.make_async_remote_copy(
            src_ref=vec.at[pl.ds(0, 1)],
            dst_ref=vec2.at[pl.ds(k - 1, 1)],
            send_sem=bsend.at[42 + k - 1],
            recv_sem=v2sem,
            device_id={"scan": chip(x + k, y, core)},
            device_id_type=MESH,
        )
        copy.start()
        v2_copies.append(copy)
    for at_lane in range(2):
        source = chip((x % 2) * 4 + core * 2 + at_lane, y, x // 4)
        arrived = pltpu.make_async_copy(dp_in.at[at_lane], dp_in.at[at_lane], dpsem.at[at_lane])
        pl.when(source != me)(arrived.wait)
    pltpu.make_async_copy(vec2.at[pl.ds(0, 7)], vec2.at[pl.ds(0, 7)], v2sem).wait()
    totals = vec[...] + jnp.sum(vec2[0:7, :], 0, keepdims=True)
    uu, uv, vv, uc, vc = (totals[0:1, i : i + 1] for i in range(5))
    a = 1.1 * uu + 1e-06
    d = 1.1 * vv + 1e-06
    det = a * d - uv * uv
    rate_obj = (uc * d - uv * vc) / det
    rate_probe = (a * vc - uv * uc) / det
    at = lax.broadcasted_iota(jnp.int32, (8, LANES), 1)
    rates[...] = jnp.where(at == 0, rate_obj, rate_probe)
    obj_step[...] = dobj[...]
    for part in range(2):
        for at_lane in range(2):
            cols = slice(LANES * at_lane, LANES * at_lane + LANES)
            probe_out[0, part, :, cols] = dp_in[at_lane, part]
            probe_out[1, part, :, cols] = probe[part, out_mode, pl.ds(mult(8 * out_band, 8), 8), cols]

    msg.drain()
    for copy in y_copies + ky_copies + kx_copies + v2_copies:
        copy.wait_send()
    for copy, when in dp_sends + pieces:
        pl.when(when)(copy.wait_send)


def finish_kernel(obj, obj_step, probe_out, rates, new_obj, new_probe):
    rate_obj, rate_probe = rates[0:1, 0:1], rates[0:1, 1:2]
    for part in range(2):
        new_obj[part] = obj[part] + rate_obj * obj_step[part]
        new_probe[part] = probe_out[1, part] + rate_probe * probe_out[0, part]


def finish(obj, obj_step, probe_out, rates):
    vmem = pl.BlockSpec(memory_space=pltpu.VMEM)
    return pl.pallas_call(
        finish_kernel,
        out_shape=(
            jax.ShapeDtypeStruct(obj.shape, F32),
            jax.ShapeDtypeStruct(probe_out.shape[1:], F32),
        ),
        in_specs=[vmem] * 4,
        out_specs=[vmem] * 2,
        name="finish",
    )(obj, obj_step, probe_out, rates)


def step(n, offsets, live, obj, probe, amps, cos, sin):
    vmem = pl.BlockSpec(memory_space=pltpu.VMEM)
    smem = pl.BlockSpec(memory_space=pltpu.SMEM)
    hbm = pl.BlockSpec(memory_space=pl.ANY)
    dma = pltpu.SemaphoreType.DMA
    columns = obj.shape[2]

    def f32(*shape):
        return pltpu.VMEM(shape, F32)

    return pl.pallas_call(
        functools.partial(step_kernel, n),
        out_shape=(
            jax.ShapeDtypeStruct((2, STRIP, columns), F32),
            jax.ShapeDtypeStruct((2, 2, 8, PATCH), F32),
            jax.ShapeDtypeStruct((8, LANES), F32),
        ),
        in_specs=[smem, smem, vmem, hbm, hbm, vmem, vmem],
        out_specs=[vmem] * 3,
        scratch_shapes=[
            pltpu.VMEM((8, LANES), jnp.int32),
            pltpu.VMEM((4 * SPLIT, 8, LANES), jnp.int32),
            pltpu.SMEM((4 * SPLIT, 8, LANES), jnp.int32),
            f32(2, MODES, PATCH, PATCH),
            f32(SPLIT, PATCH, PATCH),
            f32(2, ROWS + 16, WIN),
            f32(2, 2, STRIP, OWN),
            f32(2, ROWS + 16, WIN),
            f32(2, PATCH, PATCH),
            f32(2, PATCH, PATCH),
            f32(PATCH, PATCH),
            f32(2 * MODES + 1, PATCH, PATCH),
            pltpu.VMEM((2 * PATCH, 2 * PATCH), BF16),
            pltpu.VMEM((2 * PATCH, 2 * PATCH), BF16),
            *[pltpu.VMEM((2 * PATCH, PATCH), BF16) for m in range(MODES)],
            *[pltpu.VMEM((PATCH, 2 * PATCH), BF16) for m in range(MODES)],
            *[f32(PATCH, 2 * PATCH) for m in range(MODES)],
            f32(2, 8, 8, 5, 8, LANES),
            f32(2, ROWS, LANES),
            f32(2, STRIP, OWN),
            f32(4, 2, STRIP, OWN),
            f32(2, JITTER, OWN),
            f32(2, 2, STRIP, OWN),
            f32(2, 2, STRIP, OWN),
            f32(4, 2, STRIP, OWN),
            f32(8, 8, 5, 8, LANES),
            f32(8, 8, 5, 8, LANES),
            f32(7, 4, 5, 8, LANES),
            f32(7, 4, 5, 8, LANES),
            f32(7, 5, 8, LANES),
            f32(4, 2, STRIP, OWN),
            f32(2, 2, STRIP, OWN),
            f32(5, 8, LANES),
            f32(2, 2, 8, LANES),
            f32(2, 2, 8, LANES),
            f32(2, 8, LANES),
            f32(8, LANES),
            f32(2, 8, 8, 8, LANES),
            f32(2, KROWS, KCOLS),
            f32(1, STRIP, columns),
            f32(2, STRIP, columns),
            f32(2, STRIP, columns),
            f32(8, LANES),
            f32(16, LANES),
            f32(8, LANES),
            dma((48,)),
            dma((48,)),
            dma,
            dma,
            dma,
            dma,
            dma,
            dma((50,)),
            dma((2,)),
            dma((4,)),
            dma((2,)),
            dma((40,)),
            dma((4,)),
            dma((4,)),
            dma((2,)),
            dma((3,)),
            dma,
            dma,
            dma,
            dma((6,)),
        ],
        compiler_params=pltpu.CompilerParams(collective_id=0, has_side_effects=True),
        name="step",
    )(offsets, live, obj, probe, amps, cos, sin)


def tables(length):
    numbers = np.arange(length, dtype=np.int64)
    angles = (numbers[:, None] * numbers[None, :] % length).astype(np.float32)
    angles = angles * np.float32(2.0 * math.pi / length)
    scaling = np.float32(1.0 / math.sqrt(length))
    return tuple(jnp.asarray(f(angles) * scaling).astype(BF16) for f in (np.cos, np.sin))


def on_device(n, object_field, probe_field, amplitudes, offsets, live_counts):
    probe = probe_field.reshape(2, MODES, PATCH, PATCH)
    cos, sin = tables(PATCH)
    updates = step(n, offsets.T, live_counts, object_field, probe, amplitudes, cos, sin)
    return finish(object_field, *updates)


def solution(mesh):
    groups_scan = ("groups", "scan")
    placed = (
        P(None, groups_scan, None),
        P(None, "groups", None),
        P(groups_scan, None, None),
        P(groups_scan, None),
        P(groups_scan),
    )
    return jax.shard_map(
        functools.partial(on_device, mesh.shape["scan"]),
        mesh=mesh,
        in_specs=placed,
        out_specs=(P(None, groups_scan, None), P(None, groups_scan, None)),
        check_vma=False,
    )
```

```python
import functools
import math

import jax
import jax.numpy as jnp
import numpy as np
from jax import lax
from jax.experimental import pallas as pl
from jax.experimental.pallas import tpu as pltpu
from jax.sharding import PartitionSpec as P

MESH = pl.DeviceIdType.MESH
SPLIT = 4
JITTER = 8
STEP = 96
PATCH = 256
MODES = 4
STRIP = 24
LANES = 128
OWN = 512
WIN = 640
ROWS = JITTER + 2 * STEP + 72
ZTOP = 104
KROWS = 408
KCOLS = 384
F32 = jnp.float32
BF16 = jnp.bfloat16


def mult(value, of):
    return pl.multiple_of(value, of)


class Messages:
    def __init__(self, send, recv):
        self.send, self.recv, self.count, self.open = send, recv, 0, []

    def make(self, src, dst, scan, when=None):
        at = self.count
        self.count += 1
        self.last = self.recv.at[at]
        copy = pltpu.make_async_remote_copy(
            src_ref=src,
            dst_ref=dst,
            send_sem=self.send.at[at],
            recv_sem=self.recv.at[at],
            device_id={"scan": scan},
            device_id_type=MESH,
        )
        self.open.append((copy, when))
        return copy

    def drain(self):
        for copy, when in self.open:
            if when is None:
                copy.wait_send()
            else:
                pl.when(when)(copy.wait_send)
        self.open = []


def greet(peers):
    barrier = pltpu.get_barrier_semaphore()
    for peer in peers:
        pl.semaphore_signal(barrier, inc=1, device_id={"scan": peer}, device_id_type=MESH)
    pl.semaphore_wait(barrier, len(peers))


def long_way(me, step):
    line, at, q = me // 16, (me // SPLIT) % 4, me % SPLIT
    scale = 16

    def device(at_line, at_row):
        return (at_line + 8) % 8 * scale + (at_row + 8) % 4 * SPLIT + q

    def turn(row):
        row = (row + 8) % 4
        return jnp.where(jnp.logical_or(row == 0, row == 3), 0, 1)

    relay = device(line, at - step)
    origin = device(line, at + step)
    target = device(line + step * turn(at), at - step)
    source = device(line - step * turn(at + step), at + step)
    return relay, origin, target, source


def spread(n, kernel_pad, out, metas, line):
    me = lax.axis_index("scan")
    q = me % SPLIT
    line = line + jnp.where(q == SPLIT - 1, 1, 0)
    there = me // SPLIT - 2 + line
    inside = jnp.logical_and(there >= 0, there < n // SPLIT)
    start = mult(STRIP * q + STEP * (2 - line) - JITTER + ZTOP, 8)
    parts = out.shape[0]
    tall = STRIP + 2 * JITTER

    def one(col, carry):
        slot = line * SPLIT + col // SPLIT
        place = col % SPLIT
        top = metas[slot, 0, 2 * place]
        left = metas[slot, 0, 2 * place + 1]
        weight = jnp.where(jnp.logical_and(inside, place < metas[slot, 0, 8]), 1.0, 0.0).astype(F32)
        ahead = jnp.clip(STEP * there - top + JITTER, 0, 2 * JITTER)
        base = mult((STEP * col + 40) // LANES * LANES, LANES)
        shift = jnp.clip(left - base, 0, LANES)
        for part in range(parts):
            value = kernel_pad[part, pl.ds(start, tall), :]
            value = pltpu.roll(value, (tall - ahead) % tall, 0)[0:STRIP]
            value = pltpu.roll(value, shift, 1) * weight
            out[part, :, pl.ds(base, KCOLS)] += value
        return carry

    lax.fori_loop(0, 16, one, 0, unroll=4)


def step_kernel(
    n, offsets, live, obj, probe_hbm, amps_hbm, cos, sin, obj_step, probe_out, rates,
    meta, metas_in, metas, probe, amps, win, relay_in, grad, patch, share, bright, sums9, ta, tb,
    w0, w1, w2, w3, h0, h1, h2, h3, f0, f1, f2, f3,
    q_in, sib_in, t2_in, t1_in, t8_in, back_in, far_in, piece, q_sib, acc, minus_in, plus_in, y_in, hold_t1, hold_far,
    tile, dp, dp_in, kmine, ksib, kk, kpad, illum, place, dobj, vec, vec1, vec2,
    send, recv, ysem, kysem, kxsem, v1sem, v2sem, bsend, dpsem, psem, lsem,
    gsend, ownsem, aheadsem, relaysem, finalsem, tailsem, mrecv, msem, holdsem,
):
    me = lax.axis_index("scan")
    q = me % SPLIT
    core = me % 2
    first = me - q
    row = me // SPLIT
    rows_all = n // SPLIT
    up = (me - SPLIT + n) % n
    down = (me + SPLIT) % n
    sibling = me + 1 - 2 * core
    side = 8
    x, y = me // (2 * side), (me // 2) % side
    msg = Messages(send, recv)

    def chip(at_x, at_y, at_core):
        return ((at_x % side) * side + at_y % side) * 2 + at_core

    def columns(quarter):
        return pl.ds(mult(768 * (quarter // 2) + OWN * (quarter % 2), LANES), OWN)

    def rows(start, size):
        return pl.ds(mult(start, 8), size)

    lanes = lax.broadcasted_iota(jnp.int32, (8, LANES), 1)
    facts = jnp.where(lanes == 2 * SPLIT, live[0], 0)
    for p in range(SPLIT):
        for i in range(2):
            facts = jnp.where(lanes == 2 * p + i, offsets[i, p], facts)
    meta[...] = facts
    load_probe = pltpu.make_async_copy(probe_hbm, probe, lsem.at[0])
    load_probe.start()
    load_amps = pltpu.make_async_copy(amps_hbm, amps, lsem.at[1])
    load_amps.start()
    peers = [(first + SPLIT * e + k + 2 * n) % n for e in (-2, -1, 1, 2) for k in range(SPLIT)]
    peers += [chip(x + k, y, cc) for k in range(1, side) for cc in range(2)]
    peers += [chip(x, y + k, cc) for k in range(1, side) for cc in range(2)]
    peers += [sibling]
    def clear_outside(ref):
        @pl.when(row == 0)
        def _():
            ref[:, 0:JITTER, :] = jnp.zeros((2, JITTER, WIN), F32)

        @pl.when(row == rows_all - 1)
        def _():
            ref[:, JITTER + STEP : JITTER + 2 * STEP, :] = jnp.zeros((2, STEP, WIN), F32)

        @pl.when(row >= rows_all - 2)
        def _():
            ref[:, JITTER + 2 * STEP : ROWS, :] = jnp.zeros((2, 72, WIN), F32)

    clear_outside(win)
    metas_in[...] = jnp.zeros_like(metas_in)
    greet(peers)

    sends = []

    def put(src, dst, recv_sem, there, when=None):
        copy = pltpu.make_async_remote_copy(
            src_ref=src,
            dst_ref=dst,
            send_sem=gsend.at[len(sends)],
            recv_sem=recv_sem,
            device_id={"scan": there},
            device_id_type=MESH,
        )
        sends.append((copy, when))
        if when is None:
            copy.start()
        else:
            pl.when(when)(copy.start)

    def landing(quarter, start, size=STRIP):
        return win.at[:, rows(start, size), pl.ds(mult(LANES * (quarter % 2), LANES), OWN)]

    for e in (-1, 0, 1, 2):
        for k in range(SPLIT):
            if e or k:
                there = (first + SPLIT * e + (q + k) % SPLIT + n) % n
                to = row + e
                known = jnp.logical_and(to >= 0, to < rows_all)
                slot = (2 - e) * SPLIT + q
                put(meta, metas_in.at[slot], mrecv.at[slot], there, when=known)
    relay, origin, target, source = long_way(me, -1)
    above1, above2 = row >= 1, row >= 2
    below1, below2 = row <= rows_all - 2, row <= rows_all - 3
    middle = jnp.logical_and(jnp.logical_or(q == 1, q == 2), above2)
    passing = origin // SPLIT >= 2
    middle_at = jnp.clip(q - 1, 0, 1)
    around = [(q + k) % SPLIT for k in range(SPLIT)]
    for there in around:
        block = obj.at[:, :, columns(there)]
        put(block, relay_in.at[middle_at], relaysem.at[middle_at], relay - q + there, when=middle)
        put(block, landing(there, JITTER + STEP + STRIP * q), aheadsem.at[q], (first - SPLIT + there + n) % n, when=above1)
    for there in around[1:]:
        block = obj.at[:, :, columns(there)]
        put(block, landing(there, JITTER + STRIP * q), ownsem.at[q], first + there)
    for there in around:
        block = obj.at[:, pl.ds(STRIP - JITTER, JITTER), columns(there)]
        put(block, landing(there, 0, JITTER), tailsem, (first + SPLIT + there) % n, when=jnp.logical_and(q == SPLIT - 1, below1))
    own_at = mult(LANES * core, LANES)
    own_cols = pl.ds(own_at, OWN)
    sib_cols = pl.ds(mult(OWN * (1 - core), LANES), LANES)
    win[:, rows(JITTER + STRIP * q, STRIP), own_cols] = obj[:, :, columns(q)]
    metas_in[2 * SPLIT + q] = facts

    c, s = cos[...], sin[...]
    ta[0:256, 0:256] = c
    ta[0:256, 256:512] = s
    ta[256:512, 0:256] = -s
    ta[256:512, 256:512] = c
    tb[0:256, 0:256] = c
    tb[0:256, 256:512] = -s
    tb[256:512, 0:256] = s
    tb[256:512, 256:512] = c
    grad[...] = jnp.zeros_like(grad)
    sums9[...] = jnp.zeros_like(sums9)
    kpad[...] = jnp.zeros_like(kpad)
    illum[...] = jnp.zeros_like(illum)
    place[...] = jnp.zeros_like(place)
    dobj[...] = jnp.zeros_like(dobj)
    win[:, ROWS:, :] = jnp.zeros((2, 16, WIN), F32)
    load_probe.wait()
    light = jnp.zeros((PATCH, PATCH), F32)
    for m in range(MODES):
        light = light + (probe[0, m] * probe[0, m] + probe[1, m] * probe[1, m])
    kpad[0, ZTOP : ZTOP + PATCH, 0:PATCH] = light

    def arrived(ref, sem):
        return pltpu.make_async_copy(ref, ref, sem)

    def border(start, size):
        mine = pl.ds(mult(LANES * core + 384 * (1 - core), LANES), LANES)
        src = win.at[:, pl.ds(start, size), mine]
        dst = win.at[:, pl.ds(start, size), pl.ds(mult(OWN * core, LANES), LANES)]
        copy = msg.make(src, dst, sibling)
        copy.start()
        return copy

    def far_on(j):
        pl.when(passing)(arrived(relay_in.at[j - 1], relaysem.at[j - 1]).wait)
        put(relay_in.at[j - 1], landing(q, JITTER + 2 * STEP + STRIP * j), finalsem.at[j], target, when=passing)

    for j in range(SPLIT):
        pl.when(q != j)(arrived(landing(q, JITTER + STRIP * j), ownsem.at[j]).wait)
        if j == 0:
            pl.when(below1)(arrived(landing(q, JITTER + STEP), aheadsem.at[0]).wait)
            onward = jnp.logical_and(above1, below1)
            put(landing(q, JITTER + STEP), landing(q, JITTER + 2 * STEP), finalsem.at[0], up, when=onward)
            far_on(1)
        if j == 1:
            far_on(2)
    borders = [border(JITTER, STEP)]
    pl.when(above1)(arrived(landing(q, 0, JITTER), tailsem).wait)
    borders.append(border(0, JITTER))
    for j in range(1, SPLIT):
        pl.when(below1)(arrived(landing(q, JITTER + STEP + STRIP * j), aheadsem.at[j]).wait)
    borders.append(border(JITTER + STEP, STEP))
    for j in range(3):
        pl.when(below2)(arrived(landing(q, JITTER + 2 * STEP + STRIP * j), finalsem.at[j]).wait)
    borders.append(border(JITTER + 2 * STEP, 72))
    for line in range(4):
        there = row - 2 + line
        known = jnp.logical_and(there >= 0, there < rows_all)
        for at in range(SPLIT):
            slot = line * SPLIT + at
            other = known if line != 2 else q != at
            pl.when(other)(arrived(metas_in.at[slot], mrecv.at[slot]).wait)
    to_smem = pltpu.make_async_copy(metas_in, metas, msem)
    to_smem.start()
    load_amps.wait()
    for copy in borders:
        copy.wait_recv()

    msg.drain()
    for copy, when in sends:
        if when is None:
            copy.wait_send()
        else:
            pl.when(when)(copy.wait_send)

    wave, half_done, far = (w0, w1, w2, w3), (h0, h1, h2, h3), (f0, f1, f2, f3)
    chunk = 32
    chunks = PATCH // chunk
    slab = chunk + 2 * JITTER

    def visit(p, carry):
        ahead = jnp.clip(offsets[0, p] - (STEP * row - JITTER), 0, 2 * JITTER)
        base = mult((STEP * p + 40) // LANES * LANES, LANES)
        shift = jnp.clip(offsets[1, p] - STEP * SPLIT * q - base, 0, LANES)
        weight = jnp.where(p < live[0], 1.0, 0.0).astype(F32)
        steps = [slice(i * chunk, (i + 1) * chunk) for i in range(chunks)]
        lows = [slice(PATCH + i * chunk, PATCH + (i + 1) * chunk) for i in range(chunks)]
        left_half, right_half = slice(0, PATCH), slice(PATCH, 2 * PATCH)

        def across(table, m):
            z = jnp.dot(table[...], wave[m][...], preferred_element_type=F32)
            half_done[m][:, left_half] = z[left_half].astype(BF16)
            half_done[m][:, right_half] = z[right_half].astype(BF16)

        def along(table, m):
            far[m][...] = jnp.dot(half_done[m][...], table[...], preferred_element_type=F32)

        for i, at in enumerate(steps):
            for part in range(2):
                v = win[part, i * chunk : i * chunk + slab, pl.ds(base, KCOLS)]
                v = pltpu.roll(v, (slab - ahead) % slab, 0)[0:chunk]
                patch[part, at, :] = pltpu.roll(v, KCOLS - shift, 1)[:, 0:PATCH]
        for m in range(MODES):
            for at, low in zip(steps, lows):
                pr, pi = probe[0, m, at, :], probe[1, m, at, :]
                o_re, o_im = patch[0, at, :], patch[1, at, :]
                wave[m][at, :] = (pr * o_re - pi * o_im).astype(BF16)
                wave[m][low, :] = (pr * o_im + pi * o_re).astype(BF16)
            across(ta, m)
        for m in range(MODES):
            along(tb, m)
            for at in steps:
                fr, fi = far[m][at, left_half], far[m][at, right_half]
                power = fr * fr + fi * fi
                bright[at, :] = power if m == 0 else bright[at, :] + power
        for m in range(MODES):
            for at, low in zip(steps, lows):
                if m == 0:
                    root = jnp.maximum(jnp.sqrt(bright[at, :]), 0.5)
                    factor = (amps[p, at, :] / root - 1.0) * weight
                    bright[at, :] = factor
                else:
                    factor = bright[at, :]
                wave[m][at, :] = (far[m][at, left_half] * factor).astype(BF16)
                wave[m][low, :] = (far[m][at, right_half] * factor).astype(BF16)
            across(tb, m)
        for m in range(MODES):
            along(ta, m)
            for at in steps:
                pr, pi = probe[0, m, at, :], probe[1, m, at, :]
                o_re, o_im = patch[0, at, :], patch[1, at, :]
                cr, ci = far[m][at, left_half], far[m][at, right_half]
                g_re = pr * cr + pi * ci
                g_im = pr * ci - pi * cr
                if m > 0:
                    g_re = g_re + share[0, at, :]
                    g_im = g_im + share[1, at, :]
                share[0, at, :] = g_re
                share[1, at, :] = g_im
                sums9[m, at, :] += o_re * cr + o_im * ci
                sums9[MODES + m, at, :] += o_re * ci - o_im * cr
        blank = jnp.zeros((chunk, KCOLS - PATCH), F32)
        below = jnp.zeros((2 * JITTER, KCOLS), F32)
        for i, at in enumerate(steps):
            o_re, o_im = patch[0, at, :], patch[1, at, :]
            sums9[2 * MODES, at, :] += (o_re * o_re + o_im * o_im) * weight
            for part in range(2):
                v = pltpu.roll(jnp.concatenate([share[part, at, :], blank], 1), shift, 1)
                v = pltpu.roll(jnp.concatenate([v, below], 0), ahead, 0)
                grad[part, i * chunk : i * chunk + slab, pl.ds(base, KCOLS)] += v
        return carry

    lax.fori_loop(0, SPLIT, visit, 0)
    clear_outside(grad)

    to_sib = msg.make(grad.at[:, pl.ds(0, ROWS), sib_cols], sib_in, sibling)
    to_sib.start()
    for at_band in range(PATCH // 8):
        yy = (at_band // 2) % 8
        for at_lane in range(2):
            xx = (at_band // 16) * 4 + (at_band % 2) * 2 + at_lane
            at_rows = slice(8 * at_band, 8 * at_band + 8)
            at_cols = slice(LANES * at_lane, LANES * at_lane + LANES)
            for k in range(2):
                for i, m in enumerate((2 * k, 2 * k + 1, MODES + 2 * k, MODES + 2 * k + 1, 8)):
                    q_in[k, xx, yy, i] = sums9[m, at_rows, at_cols]
    chunks = [(x + k) % side for k in (4, 5, 3, 6, 2, 7, 1, 0)]
    q_copies = []
    for at in chunks:
        copy = msg.make(q_in.at[1 - core, at], q_sib.at[at], sibling)
        copy.start()
        q_copies.append(copy)
    relay, origin, target, source = long_way(me, 1)

    band = (x // 4) * 16 + y * 2 + (x // 2) % 2
    lane = x % 2
    out_mode = x // 2
    out_band = (x % 2) * 16 + y * 2 + core
    p_tile = probe[:, pl.ds(2 * core, 2), pl.ds(mult(8 * band, 8), 8), pl.ds(mult(LANES * lane, LANES), LANES)]

    to_sib.wait_recv()
    edge = pl.ds(mult(LANES * core + 384 * (1 - core), LANES), LANES)
    grad[:, 0:ROWS, edge] += sib_in[...]

    def sums(start):
        return grad.at[:, pl.ds(start, STRIP), own_cols]

    def add_sibling(i):
        q_copies[i].wait_recv()
        acc[chunks[i]] = q_in[core, chunks[i]] + q_sib[chunks[i]]

    halves = side // 2

    def send_chain(way, i):
        which = (i % 2 if way < 0 else 1 - i % 2) * halves
        reach = (4 if i % 2 == 0 else 3) - i // 2
        dest = (x + way * reach + side) % side
        copy = msg.make(
            acc.at[dest, pl.ds(which, halves)],
            (minus_in if way < 0 else plus_in).at[i],
            chip(x + way + side, y, core),
        )
        copy.start()
        return copy

    chains = {}
    add_sibling(0)
    chains[-1, 0], chains[1, 0] = send_chain(-1, 0), send_chain(1, 0)
    add_sibling(1)
    chains[-1, 1] = send_chain(-1, 1)
    add_sibling(2)
    chains[1, 1] = send_chain(1, 1)
    far_out = []
    for j in (1, 2):
        copy = msg.make(sums(JITTER + 2 * STEP + STRIP * j), back_in.at[j - 1], relay)
        copy.start()
        far_out.append(copy)
    t2 = msg.make(sums(JITTER + 2 * STEP), t2_in, down)
    t2.start()
    t8 = msg.make(grad.at[:, pl.ds(0, JITTER), own_cols], t8_in, up)
    t8.start()

    at_row = (me // SPLIT) % 4
    crossing = at_row == 3
    holder = at_row == 0
    turning = jnp.logical_or(at_row == 1, at_row == 2)
    far_holder = at_row <= 1
    below = x * 2 * side + (at_row + 1) % 4 * SPLIT + q
    beside = chip(x + 1, y, core)

    def start_t1(j):
        src = sums(JITTER + STEP + STRIP * j)
        t1[j] = msg.make(src, t1_in.at[j], below, when=jnp.logical_not(crossing))
        final_sem = msg.last
        pl.when(jnp.logical_not(crossing))(t1[j].start)
        copy = msg.make(src, hold_t1.at[j], below, when=crossing)
        pl.when(crossing)(copy.start)
        held.append((copy, holder, hold_t1.at[j], t1_in.at[j], final_sem))

    def pass_far(j):
        there = x * 2 * side + (at_row + 3) % 4 * SPLIT + q
        final = msg.make(back_in.at[j], far_in.at[j], there, when=jnp.logical_not(turning))
        final_sem = msg.last
        pl.when(jnp.logical_not(turning))(final.start)
        copy = msg.make(back_in.at[j], hold_far.at[j], there, when=turning)
        pl.when(turning)(copy.start)
        held.append((copy, far_holder, hold_far.at[j], far_in.at[j], final_sem))
        return final

    def release(i):
        copy, here, src, dst, final_sem = held[i]
        pl.when(here)(copy.wait_recv)
        onward = pltpu.make_async_remote_copy(
            src_ref=src,
            dst_ref=dst,
            send_sem=holdsem.at[i],
            recv_sem=final_sem,
            device_id={"scan": beside},
            device_id_type=MESH,
        )
        pl.when(here)(onward.start)
        msg.open.append((onward, here))

    t1, held = {}, []
    start_t1(3)
    for i in range(3, 8):
        add_sibling(i)

    def x_step(i):
        for way, arrived in ((-1, minus_in), (1, plus_in)):
            which = (i % 2 if way < 0 else 1 - i % 2) * halves
            reach = (4 if i % 2 == 0 else 3) - 1 - i // 2
            dest = (x + way * reach + side) % side
            chains[way, i].wait_recv()
            acc[dest, which : which + halves] += arrived[i]
            if reach > 0:
                chains[way, i + 2] = send_chain(way, i + 2)

    to_smem.wait()
    x_step(0)
    start_t1(1)
    spread(n, kpad.at[pl.ds(0, 1)], illum, metas, 0)
    x_step(1)
    start_t1(2)
    spread(n, kpad.at[pl.ds(0, 1)], illum, metas, 1)
    x_step(2)
    t2.wait_recv()
    grad[:, JITTER + STEP : JITTER + STEP + STRIP, own_cols] += t2_in[...]
    x_step(3)
    far_final = []
    for j in range(2):
        far_out[j].wait_recv()
        far_final.append(pass_far(j))
    x_step(4)
    spread(n, kpad.at[pl.ds(0, 1)], illum, metas, 2)
    x_step(5)
    x_step(6)

    y_copies = []
    for k in range(1, side):
        copy = pltpu.make_async_remote_copy(
            src_ref=acc.at[x, (y + k) % side],
            dst_ref=y_in.at[k - 1],
            send_sem=bsend.at[k - 1],
            recv_sem=ysem,
            device_id={"scan": chip(x, y + k, core)},
            device_id_type=MESH,
        )
        copy.start()
        y_copies.append(copy)
    start_t1(0)
    for i in range(3):
        release(i)
    pltpu.make_async_copy(y_in, y_in, ysem).wait()
    tile[...] = acc[x, y] + jnp.sum(y_in[...], 0)
    norm = tile[4]
    inverse = norm + 1.0
    k_re = jnp.zeros((8, LANES), F32)
    k_im = jnp.zeros((8, LANES), F32)
    s_vv = jnp.zeros((8, LANES), F32)
    s_vc = jnp.zeros((8, LANES), F32)
    for m in range(2):
        g_re, g_im = tile[m], tile[2 + m]
        d_re, d_im = g_re / inverse, g_im / inverse
        dp[m, 0] = d_re
        dp[m, 1] = d_im
        p_re, p_im = p_tile[0, m], p_tile[1, m]
        k_re = k_re + (p_re * d_re + p_im * d_im)
        k_im = k_im + (p_re * d_im - p_im * d_re)
        s_vv = s_vv + (d_re * d_re + d_im * d_im) * norm
        s_vc = s_vc + (d_re * g_re + d_im * g_im)
    kmine[0] = k_re
    kmine[1] = k_im
    k_copy = msg.make(kmine.at[1 - core], ksib, sibling)
    k_copy.start()

    dp_sends = []
    for m in range(2):
        dest = chip(2 * (2 * core + m) + x // 4, y, (x // 2) % 2)
        away = dest != me
        copy = pltpu.make_async_remote_copy(
            src_ref=dp.at[m],
            dst_ref=dp_in.at[lane],
            send_sem=bsend.at[21 + m],
            recv_sem=dpsem.at[lane],
            device_id={"scan": dest},
            device_id_type=MESH,
        )
        pl.when(away)(copy.start)
        dp_sends.append((copy, away))

        @pl.when(jnp.logical_not(away))
        def _():
            dp_in[lane] = dp[m]

    k_copy.wait_recv()
    kk[core, x, y] = kmine[core] + ksib[...]
    ky_copies = []
    for k in range(1, side):
        copy = pltpu.make_async_remote_copy(
            src_ref=kk.at[core, x, y],
            dst_ref=kk.at[core, x, y],
            send_sem=bsend.at[7 + k - 1],
            recv_sem=kysem,
            device_id={"scan": chip(x, y + k, core)},
            device_id_type=MESH,
        )
        copy.start()
        ky_copies.append(copy)

    for i in range(3, 6):
        release(i)
    pltpu.make_async_copy(kk.at[0, 0, pl.ds(0, 7)], kk.at[0, 0, pl.ds(0, 7)], kysem).wait()
    kx_copies = []
    for k in range(1, side):
        copy = pltpu.make_async_remote_copy(
            src_ref=kk.at[core, x],
            dst_ref=kk.at[core, x],
            send_sem=bsend.at[14 + k - 1],
            recv_sem=kxsem,
            device_id={"scan": chip(x + k, y, core)},
            device_id_type=MESH,
        )
        copy.start()
        kx_copies.append(copy)
    pieces = []
    for j in (3, 1, 2, 0):
        t1[j].wait_recv()
        lo = JITTER + STRIP * j
        grad[:, lo : lo + STRIP, own_cols] += t1_in[j]
        if j == 3:
            t8.wait_recv()
            grad[:, STEP : STEP + JITTER, own_cols] += t8_in[...]
        if j in (1, 2):
            far_final[j - 1].wait_recv()
            grad[:, lo : lo + STRIP, own_cols] += far_in[j - 1]
        slot = (j - q + SPLIT) % SPLIT
        copy = pltpu.make_async_remote_copy(
            src_ref=grad.at[:, pl.ds(lo, STRIP), own_cols],
            dst_ref=piece.at[slot],
            send_sem=bsend.at[23 + j],
            recv_sem=psem.at[slot],
            device_id={"scan": first + j},
            device_id_type=MESH,
        )
        pl.when(q != j)(copy.start)
        pieces.append((copy, q != j))

    piece[0] = grad[:, pl.ds(mult(JITTER + STRIP * q, 8), STRIP), own_cols]

    pltpu.make_async_copy(kk.at[0, pl.ds(0, 7)], kk.at[0, pl.ds(0, 7)], kxsem).wait()
    ks_copy = msg.make(kk.at[core], kk.at[core], sibling)
    ks_copy.start()

    for k in range(SPLIT):
        if k > 0:
            pltpu.make_async_copy(piece.at[k], piece.at[k], psem.at[k]).wait()
        source = (q - k + SPLIT) % SPLIT
        at = pl.ds(mult(768 * (source // 2) + OWN * (source % 2), LANES), OWN)
        dobj[:, :, at] += piece[k]
    lit = illum[0]
    g_re, g_im = dobj[0], dobj[1]
    o_re, o_im = obj[0], obj[1]
    d_re, d_im = g_re / (lit + 1.0), g_im / (lit + 1.0)
    s_uu = jnp.sum((d_re * d_re + d_im * d_im) * lit)
    s_uc = jnp.sum(d_re * g_re + d_im * g_im)
    dobj[0] = d_re
    dobj[1] = d_im

    ks_copy.wait_recv()
    for at_band in range(PATCH // 8):
        for at_lane in range(2):
            xx = (at_band // 16) * 4 + (at_band % 2) * 2 + at_lane
            yy = (at_band // 2) % 8
            rows = slice(ZTOP + 8 * at_band, ZTOP + 8 * at_band + 8)
            cols = slice(LANES * at_lane, LANES * at_lane + LANES)
            kpad[0, rows, cols] = kk[0, xx, yy]
            kpad[1, rows, cols] = kk[1, xx, yy]
    for line in range(3):
        spread(n, kpad, place, metas, line)
    d_re, d_im = dobj[0], dobj[1]
    s_uv = jnp.sum(
        place[0] * (d_re * o_re + d_im * o_im) - place[1] * (d_re * o_im - d_im * o_re)
    )

    at = lax.broadcasted_iota(jnp.int32, (8, LANES), 1)
    own_sums = jnp.zeros((8, LANES), F32)
    for i, value in enumerate((s_uu, s_uv, jnp.sum(s_vv), s_uc, jnp.sum(s_vc))):
        own_sums = jnp.where(at == i, value, own_sums)
    vec[...] = own_sums
    v1_copies = []
    for k in range(1, 2 * side):
        copy = pltpu.make_async_remote_copy(
            src_ref=vec.at[pl.ds(0, 1)],
            dst_ref=vec1.at[pl.ds(k - 1, 1)],
            send_sem=bsend.at[27 + k - 1],
            recv_sem=v1sem,
            device_id={"scan": chip(x, y + k // 2, (core + k) % 2)},
            device_id_type=MESH,
        )
        copy.start()
        v1_copies.append(copy)
    pltpu.make_async_copy(vec1.at[pl.ds(0, 15)], vec1.at[pl.ds(0, 15)], v1sem).wait()
    for copy in v1_copies:
        copy.wait_send()
    vec[...] = own_sums + jnp.sum(vec1[0:15, :], 0, keepdims=True)
    v2_copies = []
    for k in range(1, side):
        copy = pltpu.make_async_remote_copy(
            src_ref=vec.at[pl.ds(0, 1)],
            dst_ref=vec2.at[pl.ds(k - 1, 1)],
            send_sem=bsend.at[42 + k - 1],
            recv_sem=v2sem,
            device_id={"scan": chip(x + k, y, core)},
            device_id_type=MESH,
        )
        copy.start()
        v2_copies.append(copy)
    for at_lane in range(2):
        source = chip((x % 2) * 4 + core * 2 + at_lane, y, x // 4)
        arrived = pltpu.make_async_copy(dp_in.at[at_lane], dp_in.at[at_lane], dpsem.at[at_lane])
        pl.when(source != me)(arrived.wait)
    pltpu.make_async_copy(vec2.at[pl.ds(0, 7)], vec2.at[pl.ds(0, 7)], v2sem).wait()
    totals = vec[...] + jnp.sum(vec2[0:7, :], 0, keepdims=True)
    uu, uv, vv, uc, vc = (totals[0:1, i : i + 1] for i in range(5))
    a = 1.1 * uu + 1e-06
    d = 1.1 * vv + 1e-06
    det = a * d - uv * uv
    rate_obj = (uc * d - uv * vc) / det
    rate_probe = (a * vc - uv * uc) / det
    at = lax.broadcasted_iota(jnp.int32, (8, LANES), 1)
    rates[...] = jnp.where(at == 0, rate_obj, rate_probe)
    obj_step[...] = dobj[...]
    for part in range(2):
        for at_lane in range(2):
            cols = slice(LANES * at_lane, LANES * at_lane + LANES)
            probe_out[0, part, :, cols] = dp_in[at_lane, part]
            probe_out[1, part, :, cols] = probe[part, out_mode, pl.ds(mult(8 * out_band, 8), 8), cols]

    msg.drain()
    for copy in y_copies + ky_copies + kx_copies + v2_copies:
        copy.wait_send()
    for copy, when in dp_sends + pieces:
        pl.when(when)(copy.wait_send)


def finish_kernel(obj, obj_step, probe_out, rates, new_obj, new_probe):
    rate_obj, rate_probe = rates[0:1, 0:1], rates[0:1, 1:2]
    for part in range(2):
        new_obj[part] = obj[part] + rate_obj * obj_step[part]
        new_probe[part] = probe_out[1, part] + rate_probe * probe_out[0, part]


def finish(obj, obj_step, probe_out, rates):
    vmem = pl.BlockSpec(memory_space=pltpu.VMEM)
    return pl.pallas_call(
        finish_kernel,
        out_shape=(
            jax.ShapeDtypeStruct(obj.shape, F32),
            jax.ShapeDtypeStruct(probe_out.shape[1:], F32),
        ),
        in_specs=[vmem] * 4,
        out_specs=[vmem] * 2,
        name="finish",
    )(obj, obj_step, probe_out, rates)


def step(n, offsets, live, obj, probe, amps, cos, sin):
    vmem = pl.BlockSpec(memory_space=pltpu.VMEM)
    smem = pl.BlockSpec(memory_space=pltpu.SMEM)
    hbm = pl.BlockSpec(memory_space=pl.ANY)
    dma = pltpu.SemaphoreType.DMA
    columns = obj.shape[2]

    def f32(*shape):
        return pltpu.VMEM(shape, F32)

    return pl.pallas_call(
        functools.partial(step_kernel, n),
        out_shape=(
            jax.ShapeDtypeStruct((2, STRIP, columns), F32),
            jax.ShapeDtypeStruct((2, 2, 8, PATCH), F32),
            jax.ShapeDtypeStruct((8, LANES), F32),
        ),
        in_specs=[smem, smem, vmem, hbm, hbm, vmem, vmem],
        out_specs=[vmem] * 3,
        scratch_shapes=[
            pltpu.VMEM((8, LANES), jnp.int32),
            pltpu.VMEM((4 * SPLIT, 8, LANES), jnp.int32),
            pltpu.SMEM((4 * SPLIT, 8, LANES), jnp.int32),
            f32(2, MODES, PATCH, PATCH),
            f32(SPLIT, PATCH, PATCH),
            f32(2, ROWS + 16, WIN),
            f32(2, 2, STRIP, OWN),
            f32(2, ROWS + 16, WIN),
            f32(2, PATCH, PATCH),
            f32(2, PATCH, PATCH),
            f32(PATCH, PATCH),
            f32(2 * MODES + 1, PATCH, PATCH),
            pltpu.VMEM((2 * PATCH, 2 * PATCH), BF16),
            pltpu.VMEM((2 * PATCH, 2 * PATCH), BF16),
            *[pltpu.VMEM((2 * PATCH, PATCH), BF16) for m in range(MODES)],
            *[pltpu.VMEM((PATCH, 2 * PATCH), BF16) for m in range(MODES)],
            *[f32(PATCH, 2 * PATCH) for m in range(MODES)],
            f32(2, 8, 8, 5, 8, LANES),
            f32(2, ROWS, LANES),
            f32(2, STRIP, OWN),
            f32(4, 2, STRIP, OWN),
            f32(2, JITTER, OWN),
            f32(2, 2, STRIP, OWN),
            f32(2, 2, STRIP, OWN),
            f32(4, 2, STRIP, OWN),
            f32(8, 8, 5, 8, LANES),
            f32(8, 8, 5, 8, LANES),
            f32(7, 4, 5, 8, LANES),
            f32(7, 4, 5, 8, LANES),
            f32(7, 5, 8, LANES),
            f32(4, 2, STRIP, OWN),
            f32(2, 2, STRIP, OWN),
            f32(5, 8, LANES),
            f32(2, 2, 8, LANES),
            f32(2, 2, 8, LANES),
            f32(2, 8, LANES),
            f32(8, LANES),
            f32(2, 8, 8, 8, LANES),
            f32(2, KROWS, KCOLS),
            f32(1, STRIP, columns),
            f32(2, STRIP, columns),
            f32(2, STRIP, columns),
            f32(8, LANES),
            f32(16, LANES),
            f32(8, LANES),
            dma((48,)),
            dma((48,)),
            dma,
            dma,
            dma,
            dma,
            dma,
            dma((50,)),
            dma((2,)),
            dma((4,)),
            dma((2,)),
            dma((40,)),
            dma((4,)),
            dma((4,)),
            dma((2,)),
            dma((3,)),
            dma,
            dma((16,)),
            dma,
            dma((6,)),
        ],
        compiler_params=pltpu.CompilerParams(collective_id=0, has_side_effects=True),
        name="step",
    )(offsets, live, obj, probe, amps, cos, sin)


def tables(length):
    numbers = np.arange(length, dtype=np.int64)
    angles = (numbers[:, None] * numbers[None, :] % length).astype(np.float32)
    angles = angles * np.float32(2.0 * math.pi / length)
    scaling = np.float32(1.0 / math.sqrt(length))
    return tuple(jnp.asarray(f(angles) * scaling).astype(BF16) for f in (np.cos, np.sin))


def on_device(n, object_field, probe_field, amplitudes, offsets, live_counts):
    probe = probe_field.reshape(2, MODES, PATCH, PATCH)
    cos, sin = tables(PATCH)
    updates = step(n, offsets.T, live_counts, object_field, probe, amplitudes, cos, sin)
    return finish(object_field, *updates)


def solution(mesh):
    groups_scan = ("groups", "scan")
    placed = (
        P(None, groups_scan, None),
        P(None, "groups", None),
        P(groups_scan, None, None),
        P(groups_scan, None),
        P(groups_scan),
    )
    return jax.shard_map(
        functools.partial(on_device, mesh.shape["scan"]),
        mesh=mesh,
        in_specs=placed,
        out_specs=(P(None, groups_scan, None), P(None, groups_scan, None)),
        check_vma=False,
    )
```

```python
import functools
import math

import jax
import jax.numpy as jnp
import numpy as np
from jax import lax
from jax.experimental import pallas as pl
from jax.experimental.pallas import tpu as pltpu
from jax.sharding import PartitionSpec as P

MESH = pl.DeviceIdType.MESH
SPLIT = 4
JITTER = 8
STEP = 96
PATCH = 256
MODES = 4
STRIP = 24
LANES = 128
OWN = 512
WIN = 640
ROWS = JITTER + 2 * STEP + 72
ZTOP = 104
KROWS = 408
KCOLS = 384
F32 = jnp.float32
BF16 = jnp.bfloat16


def mult(value, of):
    return pl.multiple_of(value, of)


class Messages:
    def __init__(self, send, recv):
        self.send, self.recv, self.count, self.open = send, recv, 0, []

    def make(self, src, dst, scan, when=None):
        at = self.count
        self.count += 1
        self.last = self.recv.at[at]
        copy = pltpu.make_async_remote_copy(
            src_ref=src,
            dst_ref=dst,
            send_sem=self.send.at[at],
            recv_sem=self.recv.at[at],
            device_id={"scan": scan},
            device_id_type=MESH,
        )
        self.open.append((copy, when))
        return copy

    def drain(self):
        for copy, when in self.open:
            if when is None:
                copy.wait_send()
            else:
                pl.when(when)(copy.wait_send)
        self.open = []


def greet(peers):
    barrier = pltpu.get_barrier_semaphore()
    for peer in peers:
        pl.semaphore_signal(barrier, inc=1, device_id={"scan": peer}, device_id_type=MESH)
    pl.semaphore_wait(barrier, len(peers))


def long_way(me, step):
    line, at, q = me // 16, (me // SPLIT) % 4, me % SPLIT
    scale = 16

    def device(at_line, at_row):
        return (at_line + 8) % 8 * scale + (at_row + 8) % 4 * SPLIT + q

    def turn(row):
        row = (row + 8) % 4
        return jnp.where(jnp.logical_or(row == 0, row == 3), 0, 1)

    relay = device(line, at - step)
    origin = device(line, at + step)
    target = device(line + step * turn(at), at - step)
    source = device(line - step * turn(at + step), at + step)
    return relay, origin, target, source


def spread(n, kernel_pad, out, metas, line):
    me = lax.axis_index("scan")
    q = me % SPLIT
    line = line + jnp.where(q == SPLIT - 1, 1, 0)
    there = me // SPLIT - 2 + line
    inside = jnp.logical_and(there >= 0, there < n // SPLIT)
    start = mult(STRIP * q + STEP * (2 - line) - JITTER + ZTOP, 8)
    parts = out.shape[0]
    tall = STRIP + 2 * JITTER

    def one(col, carry):
        slot = line * SPLIT + col // SPLIT
        place = col % SPLIT
        top = metas[slot, 0, 2 * place]
        left = metas[slot, 0, 2 * place + 1]
        weight = jnp.where(jnp.logical_and(inside, place < metas[slot, 0, 8]), 1.0, 0.0).astype(F32)
        ahead = jnp.clip(STEP * there - top + JITTER, 0, 2 * JITTER)
        base = mult((STEP * col + 40) // LANES * LANES, LANES)
        shift = jnp.clip(left - base, 0, LANES)
        for part in range(parts):
            value = kernel_pad[part, pl.ds(start, tall), :]
            value = pltpu.roll(value, (tall - ahead) % tall, 0)[0:STRIP]
            value = pltpu.roll(value, shift, 1) * weight
            out[part, :, pl.ds(base, KCOLS)] += value
        return carry

    lax.fori_loop(0, 16, one, 0, unroll=4)


def collect(n, strip, out, metas, line):
    me = lax.axis_index("scan")
    q = me % SPLIT
    line = line + jnp.where(q == SPLIT - 1, 1, 0)
    there = me // SPLIT - 2 + line
    inside = jnp.logical_and(there >= 0, there < n // SPLIT)
    start = mult(STRIP * q + STEP * (2 - line) - JITTER + ZTOP, 8)
    tall = STRIP + 2 * JITTER

    def one(col, carry):
        slot = line * SPLIT + col // SPLIT
        place = col % SPLIT
        top = metas[slot, 0, 2 * place]
        left = metas[slot, 0, 2 * place + 1]
        weight = jnp.where(jnp.logical_and(inside, place < metas[slot, 0, 8]), 1.0, 0.0).astype(F32)
        ahead = jnp.clip(STEP * there - top + JITTER, 0, 2 * JITTER)
        base = mult((STEP * col + 40) // LANES * LANES, LANES)
        shift = jnp.clip(left - base, 0, LANES)
        below = jnp.zeros((2 * JITTER, PATCH), F32)
        for part in range(2):
            value = strip[part, :, pl.ds(base, KCOLS)]
            value = pltpu.roll(value, (KCOLS - shift) % KCOLS, 1)[:, 0:PATCH] * weight
            value = pltpu.roll(jnp.concatenate([value, below], 0), ahead, 0)
            out[part, pl.ds(start, tall), :] += value
        return carry

    lax.fori_loop(0, 16, one, 0, unroll=4)


def step_kernel(
    n, offsets, live, obj, probe_hbm, amps_hbm, cos, sin, obj_step, probe_out, rates,
    meta, metas_in, metas, probe, amps, win, relay_in, grad, patch, share, bright, sums9, ta, tb,
    w0, w1, w2, w3, h0, h1, h2, h3, f0, f1, f2, f3,
    q_in, sib_in, t2_in, t1_in, t8_in, back_in, far_in, piece, q_sib, acc, minus_in, plus_in, y_in, hold_t1, hold_far,
    tile, dp, dp_in, kmine, ksib, kk, kpad, illum, place, dobj, cross, cross_in, vec, vec1, vec2,
    send, recv, ysem, kysem, kxsem, v1sem, v2sem, bsend, dpsem, psem, lsem,
    gsend, ownsem, aheadsem, relaysem, finalsem, tailsem, mrecv, msem, holdsem,
):
    me = lax.axis_index("scan")
    q = me % SPLIT
    core = me % 2
    first = me - q
    row = me // SPLIT
    rows_all = n // SPLIT
    up = (me - SPLIT + n) % n
    down = (me + SPLIT) % n
    sibling = me + 1 - 2 * core
    side = 8
    x, y = me // (2 * side), (me // 2) % side
    msg = Messages(send, recv)

    def chip(at_x, at_y, at_core):
        return ((at_x % side) * side + at_y % side) * 2 + at_core

    def columns(quarter):
        return pl.ds(mult(768 * (quarter // 2) + OWN * (quarter % 2), LANES), OWN)

    def rows(start, size):
        return pl.ds(mult(start, 8), size)

    lanes = lax.broadcasted_iota(jnp.int32, (8, LANES), 1)
    facts = jnp.where(lanes == 2 * SPLIT, live[0], 0)
    for p in range(SPLIT):
        for i in range(2):
            facts = jnp.where(lanes == 2 * p + i, offsets[i, p], facts)
    meta[...] = facts
    load_probe = pltpu.make_async_copy(probe_hbm, probe, lsem.at[0])
    load_probe.start()
    load_amps = pltpu.make_async_copy(amps_hbm, amps, lsem.at[1])
    load_amps.start()
    peers = [(first + SPLIT * e + k + 2 * n) % n for e in (-2, -1, 1, 2) for k in range(SPLIT)]
    peers += [chip(x + k, y, cc) for k in range(1, side) for cc in range(2)]
    peers += [chip(x, y + k, cc) for k in range(1, side) for cc in range(2)]
    peers += [sibling]
    def clear_outside(ref):
        @pl.when(row == 0)
        def _():
            ref[:, 0:JITTER, :] = jnp.zeros((2, JITTER, WIN), F32)

        @pl.when(row == rows_all - 1)
        def _():
            ref[:, JITTER + STEP : JITTER + 2 * STEP, :] = jnp.zeros((2, STEP, WIN), F32)

        @pl.when(row >= rows_all - 2)
        def _():
            ref[:, JITTER + 2 * STEP : ROWS, :] = jnp.zeros((2, 72, WIN), F32)

    clear_outside(win)
    metas_in[...] = jnp.zeros_like(metas_in)
    greet(peers)

    sends = []

    def put(src, dst, recv_sem, there, when=None):
        copy = pltpu.make_async_remote_copy(
            src_ref=src,
            dst_ref=dst,
            send_sem=gsend.at[len(sends)],
            recv_sem=recv_sem,
            device_id={"scan": there},
            device_id_type=MESH,
        )
        sends.append((copy, when))
        if when is None:
            copy.start()
        else:
            pl.when(when)(copy.start)

    def landing(quarter, start, size=STRIP):
        return win.at[:, rows(start, size), pl.ds(mult(LANES * (quarter % 2), LANES), OWN)]

    for e in (-1, 0, 1, 2):
        for k in range(SPLIT):
            if e or k:
                there = (first + SPLIT * e + (q + k) % SPLIT + n) % n
                to = row + e
                known = jnp.logical_and(to >= 0, to < rows_all)
                slot = (2 - e) * SPLIT + q
                put(meta, metas_in.at[slot], mrecv.at[slot], there, when=known)
    relay, origin, target, source = long_way(me, -1)
    above1, above2 = row >= 1, row >= 2
    below1, below2 = row <= rows_all - 2, row <= rows_all - 3
    middle = jnp.logical_and(jnp.logical_or(q == 1, q == 2), above2)
    passing = origin // SPLIT >= 2
    middle_at = jnp.clip(q - 1, 0, 1)
    around = [(q + k) % SPLIT for k in range(SPLIT)]
    for there in around:
        block = obj.at[:, :, columns(there)]
        put(block, relay_in.at[middle_at], relaysem.at[middle_at], relay - q + there, when=middle)
        put(block, landing(there, JITTER + STEP + STRIP * q), aheadsem.at[q], (first - SPLIT + there + n) % n, when=above1)
    for there in around[1:]:
        block = obj.at[:, :, columns(there)]
        put(block, landing(there, JITTER + STRIP * q), ownsem.at[q], first + there)
    for there in around:
        block = obj.at[:, pl.ds(STRIP - JITTER, JITTER), columns(there)]
        put(block, landing(there, 0, JITTER), tailsem, (first + SPLIT + there) % n, when=jnp.logical_and(q == SPLIT - 1, below1))
    own_at = mult(LANES * core, LANES)
    own_cols = pl.ds(own_at, OWN)
    sib_cols = pl.ds(mult(OWN * (1 - core), LANES), LANES)
    win[:, rows(JITTER + STRIP * q, STRIP), own_cols] = obj[:, :, columns(q)]
    metas_in[2 * SPLIT + q] = facts

    c, s = cos[...], sin[...]
    ta[0:256, 0:256] = c
    ta[0:256, 256:512] = s
    ta[256:512, 0:256] = -s
    ta[256:512, 256:512] = c
    tb[0:256, 0:256] = c
    tb[0:256, 256:512] = -s
    tb[256:512, 0:256] = s
    tb[256:512, 256:512] = c
    grad[...] = jnp.zeros_like(grad)
    sums9[...] = jnp.zeros_like(sums9)
    kpad[...] = jnp.zeros_like(kpad)
    illum[...] = jnp.zeros_like(illum)
    cross[...] = jnp.zeros_like(cross)
    dobj[...] = jnp.zeros_like(dobj)
    win[:, ROWS:, :] = jnp.zeros((2, 16, WIN), F32)
    load_probe.wait()
    light = jnp.zeros((PATCH, PATCH), F32)
    for m in range(MODES):
        light = light + (probe[0, m] * probe[0, m] + probe[1, m] * probe[1, m])
    kpad[0, ZTOP : ZTOP + PATCH, 0:PATCH] = light

    def arrived(ref, sem):
        return pltpu.make_async_copy(ref, ref, sem)

    def border(start, size):
        mine = pl.ds(mult(LANES * core + 384 * (1 - core), LANES), LANES)
        src = win.at[:, pl.ds(start, size), mine]
        dst = win.at[:, pl.ds(start, size), pl.ds(mult(OWN * core, LANES), LANES)]
        copy = msg.make(src, dst, sibling)
        copy.start()
        return copy

    def far_on(j):
        pl.when(passing)(arrived(relay_in.at[j - 1], relaysem.at[j - 1]).wait)
        put(relay_in.at[j - 1], landing(q, JITTER + 2 * STEP + STRIP * j), finalsem.at[j], target, when=passing)

    for j in range(SPLIT):
        pl.when(q != j)(arrived(landing(q, JITTER + STRIP * j), ownsem.at[j]).wait)
        if j == 0:
            pl.when(below1)(arrived(landing(q, JITTER + STEP), aheadsem.at[0]).wait)
            onward = jnp.logical_and(above1, below1)
            put(landing(q, JITTER + STEP), landing(q, JITTER + 2 * STEP), finalsem.at[0], up, when=onward)
            far_on(1)
        if j == 1:
            far_on(2)
    borders = [border(JITTER, STEP)]
    pl.when(above1)(arrived(landing(q, 0, JITTER), tailsem).wait)
    borders.append(border(0, JITTER))
    for j in range(1, SPLIT):
        pl.when(below1)(arrived(landing(q, JITTER + STEP + STRIP * j), aheadsem.at[j]).wait)
    borders.append(border(JITTER + STEP, STEP))
    for j in range(3):
        pl.when(below2)(arrived(landing(q, JITTER + 2 * STEP + STRIP * j), finalsem.at[j]).wait)
    borders.append(border(JITTER + 2 * STEP, 72))
    for line in range(4):
        there = row - 2 + line
        known = jnp.logical_and(there >= 0, there < rows_all)
        for at in range(SPLIT):
            slot = line * SPLIT + at
            other = known if line != 2 else q != at
            pl.when(other)(arrived(metas_in.at[slot], mrecv.at[slot]).wait)
    to_smem = pltpu.make_async_copy(metas_in, metas, msem)
    to_smem.start()
    load_amps.wait()
    for copy in borders:
        copy.wait_recv()

    msg.drain()
    for copy, when in sends:
        if when is None:
            copy.wait_send()
        else:
            pl.when(when)(copy.wait_send)

    wave, half_done, far = (w0, w1, w2, w3), (h0, h1, h2, h3), (f0, f1, f2, f3)
    chunk = 32
    chunks = PATCH // chunk
    slab = chunk + 2 * JITTER

    def visit(p, carry):
        ahead = jnp.clip(offsets[0, p] - (STEP * row - JITTER), 0, 2 * JITTER)
        base = mult((STEP * p + 40) // LANES * LANES, LANES)
        shift = jnp.clip(offsets[1, p] - STEP * SPLIT * q - base, 0, LANES)
        weight = jnp.where(p < live[0], 1.0, 0.0).astype(F32)
        steps = [slice(i * chunk, (i + 1) * chunk) for i in range(chunks)]
        lows = [slice(PATCH + i * chunk, PATCH + (i + 1) * chunk) for i in range(chunks)]
        left_half, right_half = slice(0, PATCH), slice(PATCH, 2 * PATCH)

        def across(table, m):
            z = jnp.dot(table[...], wave[m][...], preferred_element_type=F32)
            half_done[m][:, left_half] = z[left_half].astype(BF16)
            half_done[m][:, right_half] = z[right_half].astype(BF16)

        def along(table, m):
            far[m][...] = jnp.dot(half_done[m][...], table[...], preferred_element_type=F32)

        for i, at in enumerate(steps):
            for part in range(2):
                v = win[part, i * chunk : i * chunk + slab, pl.ds(base, KCOLS)]
                v = pltpu.roll(v, (slab - ahead) % slab, 0)[0:chunk]
                patch[part, at, :] = pltpu.roll(v, KCOLS - shift, 1)[:, 0:PATCH]
        for m in range(MODES):
            for at, low in zip(steps, lows):
                pr, pi = probe[0, m, at, :], probe[1, m, at, :]
                o_re, o_im = patch[0, at, :], patch[1, at, :]
                wave[m][at, :] = (pr * o_re - pi * o_im).astype(BF16)
                wave[m][low, :] = (pr * o_im + pi * o_re).astype(BF16)
            across(ta, m)
        for m in range(MODES):
            along(tb, m)
            for at in steps:
                fr, fi = far[m][at, left_half], far[m][at, right_half]
                power = fr * fr + fi * fi
                bright[at, :] = power if m == 0 else bright[at, :] + power
        for m in range(MODES):
            for at, low in zip(steps, lows):
                if m == 0:
                    root = jnp.maximum(jnp.sqrt(bright[at, :]), 0.5)
                    factor = (amps[p, at, :] / root - 1.0) * weight
                    bright[at, :] = factor
                else:
                    factor = bright[at, :]
                wave[m][at, :] = (far[m][at, left_half] * factor).astype(BF16)
                wave[m][low, :] = (far[m][at, right_half] * factor).astype(BF16)
            across(tb, m)
        for m in range(MODES):
            along(ta, m)
            for at in steps:
                pr, pi = probe[0, m, at, :], probe[1, m, at, :]
                o_re, o_im = patch[0, at, :], patch[1, at, :]
                cr, ci = far[m][at, left_half], far[m][at, right_half]
                g_re = pr * cr + pi * ci
                g_im = pr * ci - pi * cr
                if m > 0:
                    g_re = g_re + share[0, at, :]
                    g_im = g_im + share[1, at, :]
                share[0, at, :] = g_re
                share[1, at, :] = g_im
                sums9[m, at, :] += o_re * cr + o_im * ci
                sums9[MODES + m, at, :] += o_re * ci - o_im * cr
        blank = jnp.zeros((chunk, KCOLS - PATCH), F32)
        below = jnp.zeros((2 * JITTER, KCOLS), F32)
        for i, at in enumerate(steps):
            o_re, o_im = patch[0, at, :], patch[1, at, :]
            sums9[2 * MODES, at, :] += (o_re * o_re + o_im * o_im) * weight
            for part in range(2):
                v = pltpu.roll(jnp.concatenate([share[part, at, :], blank], 1), shift, 1)
                v = pltpu.roll(jnp.concatenate([v, below], 0), ahead, 0)
                grad[part, i * chunk : i * chunk + slab, pl.ds(base, KCOLS)] += v
        return carry

    lax.fori_loop(0, SPLIT, visit, 0)
    clear_outside(grad)

    for at_band in range(PATCH // 8):
        yy = (at_band // 2) % 8
        for at_lane in range(2):
            xx = (at_band // 16) * 4 + (at_band % 2) * 2 + at_lane
            at_rows = slice(8 * at_band, 8 * at_band + 8)
            at_cols = slice(LANES * at_lane, LANES * at_lane + LANES)
            for k in range(2):
                for i, m in enumerate((2 * k, 2 * k + 1, MODES + 2 * k, MODES + 2 * k + 1, 8)):
                    q_in[k, xx, yy, i] = sums9[m, at_rows, at_cols]
    chunks = [(x + k) % side for k in (4, 5, 3, 6, 2, 7, 1, 0)]
    q_copies = []
    for at in chunks:
        copy = msg.make(q_in.at[1 - core, at], q_sib.at[at], sibling)
        copy.start()
        q_copies.append(copy)
        if not q_copies[1:]:
            to_sib = msg.make(grad.at[:, pl.ds(0, ROWS), sib_cols], sib_in, sibling)
            to_sib.start()
    relay, origin, target, source = long_way(me, 1)

    band = (x // 4) * 16 + y * 2 + (x // 2) % 2
    lane = x % 2
    out_mode = x // 2
    out_band = (x % 2) * 16 + y * 2 + core
    p_tile = probe[:, pl.ds(2 * core, 2), pl.ds(mult(8 * band, 8), 8), pl.ds(mult(LANES * lane, LANES), LANES)]

    def sums(start):
        return grad.at[:, pl.ds(start, STRIP), own_cols]

    def add_sibling(i):
        q_copies[i].wait_recv()
        acc[chunks[i]] = q_in[core, chunks[i]] + q_sib[chunks[i]]

    halves = side // 2

    def send_chain(way, i):
        which = (i % 2 if way < 0 else 1 - i % 2) * halves
        reach = (4 if i % 2 == 0 else 3) - i // 2
        dest = (x + way * reach + side) % side
        copy = msg.make(
            acc.at[dest, pl.ds(which, halves)],
            (minus_in if way < 0 else plus_in).at[i],
            chip(x + way + side, y, core),
        )
        copy.start()
        return copy

    chains = {}
    add_sibling(0)
    chains[-1, 0], chains[1, 0] = send_chain(-1, 0), send_chain(1, 0)
    add_sibling(1)
    chains[-1, 1] = send_chain(-1, 1)
    add_sibling(2)
    chains[1, 1] = send_chain(1, 1)
    to_sib.wait_recv()
    edge = pl.ds(mult(LANES * core + 384 * (1 - core), LANES), LANES)
    grad[:, 0:ROWS, edge] += sib_in[...]

    far_out = []
    for j in (1, 2):
        copy = msg.make(sums(JITTER + 2 * STEP + STRIP * j), back_in.at[j - 1], relay)
        copy.start()
        far_out.append(copy)
    t2 = msg.make(sums(JITTER + 2 * STEP), t2_in, down)
    t2.start()
    t8 = msg.make(grad.at[:, pl.ds(0, JITTER), own_cols], t8_in, up)
    t8.start()

    at_row = (me // SPLIT) % 4
    crossing = at_row == 3
    holder = at_row == 0
    turning = jnp.logical_or(at_row == 1, at_row == 2)
    far_holder = at_row <= 1
    below = x * 2 * side + (at_row + 1) % 4 * SPLIT + q
    beside = chip(x + 1, y, core)

    def start_t1(j):
        src = sums(JITTER + STEP + STRIP * j)
        t1[j] = msg.make(src, t1_in.at[j], below, when=jnp.logical_not(crossing))
        final_sem = msg.last
        pl.when(jnp.logical_not(crossing))(t1[j].start)
        copy = msg.make(src, hold_t1.at[j], below, when=crossing)
        pl.when(crossing)(copy.start)
        held.append((copy, holder, hold_t1.at[j], t1_in.at[j], final_sem))

    def pass_far(j):
        there = x * 2 * side + (at_row + 3) % 4 * SPLIT + q
        final = msg.make(back_in.at[j], far_in.at[j], there, when=jnp.logical_not(turning))
        final_sem = msg.last
        pl.when(jnp.logical_not(turning))(final.start)
        copy = msg.make(back_in.at[j], hold_far.at[j], there, when=turning)
        pl.when(turning)(copy.start)
        held.append((copy, far_holder, hold_far.at[j], far_in.at[j], final_sem))
        return final

    def release(i):
        copy, here, src, dst, final_sem = held[i]
        pl.when(here)(copy.wait_recv)
        onward = pltpu.make_async_remote_copy(
            src_ref=src,
            dst_ref=dst,
            send_sem=holdsem.at[i],
            recv_sem=final_sem,
            device_id={"scan": beside},
            device_id_type=MESH,
        )
        pl.when(here)(onward.start)
        msg.open.append((onward, here))

    t1, held = {}, []
    start_t1(3)
    for i in range(3, 8):
        add_sibling(i)

    def x_step(i):
        for way, arrived in ((-1, minus_in), (1, plus_in)):
            which = (i % 2 if way < 0 else 1 - i % 2) * halves
            reach = (4 if i % 2 == 0 else 3) - 1 - i // 2
            dest = (x + way * reach + side) % side
            chains[way, i].wait_recv()
            acc[dest, which : which + halves] += arrived[i]
            if reach > 0:
                chains[way, i + 2] = send_chain(way, i + 2)

    to_smem.wait()
    x_step(0)
    start_t1(1)
    spread(n, kpad, illum, metas, 0)
    x_step(1)
    start_t1(2)
    spread(n, kpad, illum, metas, 1)
    x_step(2)
    t2.wait_recv()
    grad[:, JITTER + STEP : JITTER + STEP + STRIP, own_cols] += t2_in[...]
    x_step(3)
    far_final = []
    for j in range(2):
        far_out[j].wait_recv()
        far_final.append(pass_far(j))
    x_step(4)
    spread(n, kpad, illum, metas, 2)
    x_step(5)
    x_step(6)

    y_copies = []
    for k in range(1, side):
        copy = pltpu.make_async_remote_copy(
            src_ref=acc.at[x, (y + k) % side],
            dst_ref=y_in.at[k - 1],
            send_sem=bsend.at[k - 1],
            recv_sem=ysem,
            device_id={"scan": chip(x, y + k, core)},
            device_id_type=MESH,
        )
        copy.start()
        y_copies.append(copy)
    start_t1(0)
    for i in range(3):
        release(i)
    pltpu.make_async_copy(y_in, y_in, ysem).wait()
    tile[...] = acc[x, y] + jnp.sum(y_in[...], 0)
    norm = tile[4]
    inverse = norm + 1.0
    k_re = jnp.zeros((8, LANES), F32)
    k_im = jnp.zeros((8, LANES), F32)
    s_vv = jnp.zeros((8, LANES), F32)
    s_vc = jnp.zeros((8, LANES), F32)
    for m in range(2):
        g_re, g_im = tile[m], tile[2 + m]
        d_re, d_im = g_re / inverse, g_im / inverse
        dp[m, 0] = d_re
        dp[m, 1] = d_im
        p_re, p_im = p_tile[0, m], p_tile[1, m]
        k_re = k_re + (p_re * d_re + p_im * d_im)
        k_im = k_im + (p_re * d_im - p_im * d_re)
        s_vv = s_vv + (d_re * d_re + d_im * d_im) * norm
        s_vc = s_vc + (d_re * g_re + d_im * g_im)
    kmine[0] = k_re
    kmine[1] = k_im
    k_copy = msg.make(kmine.at[1 - core], ksib, sibling)
    k_copy.start()

    dp_sends = []
    for m in range(2):
        dest = chip(2 * (2 * core + m) + x // 4, y, (x // 2) % 2)
        away = dest != me
        copy = pltpu.make_async_remote_copy(
            src_ref=dp.at[m],
            dst_ref=dp_in.at[lane],
            send_sem=bsend.at[21 + m],
            recv_sem=dpsem.at[lane],
            device_id={"scan": dest},
            device_id_type=MESH,
        )
        pl.when(away)(copy.start)
        dp_sends.append((copy, away))

        @pl.when(jnp.logical_not(away))
        def _():
            dp_in[lane] = dp[m]

    k_copy.wait_recv()
    kk[core, x, y] = kmine[core] + ksib[...]
    ky_copies = []
    for k in range(1, side):
        copy = pltpu.make_async_remote_copy(
            src_ref=kk.at[core, x, y],
            dst_ref=kk.at[core, x, y],
            send_sem=bsend.at[7 + k - 1],
            recv_sem=kysem,
            device_id={"scan": chip(x, y + k, core)},
            device_id_type=MESH,
        )
        copy.start()
        ky_copies.append(copy)

    for i in range(3, 6):
        release(i)
    pltpu.make_async_copy(kk.at[0, 0, pl.ds(0, 7)], kk.at[0, 0, pl.ds(0, 7)], kysem).wait()
    kx_copies = []
    for k in range(1, side):
        copy = pltpu.make_async_remote_copy(
            src_ref=kk.at[core, x],
            dst_ref=kk.at[core, x],
            send_sem=bsend.at[14 + k - 1],
            recv_sem=kxsem,
            device_id={"scan": chip(x + k, y, core)},
            device_id_type=MESH,
        )
        copy.start()
        kx_copies.append(copy)
    pieces = []
    for j in (3, 1, 2, 0):
        t1[j].wait_recv()
        lo = JITTER + STRIP * j
        grad[:, lo : lo + STRIP, own_cols] += t1_in[j]
        if j == 3:
            t8.wait_recv()
            grad[:, STEP : STEP + JITTER, own_cols] += t8_in[...]
        if j in (1, 2):
            far_final[j - 1].wait_recv()
            grad[:, lo : lo + STRIP, own_cols] += far_in[j - 1]
        slot = (j - q + SPLIT) % SPLIT
        copy = pltpu.make_async_remote_copy(
            src_ref=grad.at[:, pl.ds(lo, STRIP), own_cols],
            dst_ref=piece.at[slot],
            send_sem=bsend.at[23 + j],
            recv_sem=psem.at[slot],
            device_id={"scan": first + j},
            device_id_type=MESH,
        )
        pl.when(q != j)(copy.start)
        pieces.append((copy, q != j))

    piece[0] = grad[:, pl.ds(mult(JITTER + STRIP * q, 8), STRIP), own_cols]

    for k in range(SPLIT):
        if k > 0:
            pltpu.make_async_copy(piece.at[k], piece.at[k], psem.at[k]).wait()
        source = (q - k + SPLIT) % SPLIT
        at = pl.ds(mult(768 * (source // 2) + OWN * (source % 2), LANES), OWN)
        dobj[:, :, at] += piece[k]
    lit = illum[0]
    g_re, g_im = dobj[0], dobj[1]
    o_re, o_im = obj[0], obj[1]
    d_re, d_im = g_re / (lit + 1.0), g_im / (lit + 1.0)
    s_uu = jnp.sum((d_re * d_re + d_im * d_im) * lit)
    s_uc = jnp.sum(d_re * g_re + d_im * g_im)
    dobj[0] = d_re
    dobj[1] = d_im

    place[0] = d_re * o_re + d_im * o_im
    place[1] = d_re * o_im - d_im * o_re
    for line in range(3):
        collect(n, place, cross, metas, line)
    cross_copy = msg.make(cross.at[1 - core, pl.ds(ZTOP, PATCH)], cross_in, sibling)
    cross_copy.start()
    pltpu.make_async_copy(kk.at[0, pl.ds(0, 7)], kk.at[0, pl.ds(0, 7)], kxsem).wait()
    cross_copy.wait_recv()
    product = jnp.zeros((8, LANES), F32)
    for at_band in range(PATCH // 8):
        for at_lane in range(2):
            xx = (at_band // 16) * 4 + (at_band % 2) * 2 + at_lane
            yy = (at_band // 2) % 8
            rows_at = slice(8 * at_band, 8 * at_band + 8)
            cols = slice(LANES * at_lane, LANES * at_lane + LANES)
            both = cross[core, ZTOP + 8 * at_band : ZTOP + 8 * at_band + 8, cols] + cross_in[rows_at, cols]
            product = product + kk[core, xx, yy] * both
    s_uv = jnp.sum(product) * jnp.where(core == 0, 1.0, -1.0).astype(F32)

    at = lax.broadcasted_iota(jnp.int32, (8, LANES), 1)
    own_sums = jnp.zeros((8, LANES), F32)
    for i, value in enumerate((s_uu, s_uv, jnp.sum(s_vv), s_uc, jnp.sum(s_vc))):
        own_sums = jnp.where(at == i, value, own_sums)
    vec[...] = own_sums
    v1_copies = []
    for k in range(1, 2 * side):
        copy = pltpu.make_async_remote_copy(
            src_ref=vec.at[pl.ds(0, 1)],
            dst_ref=vec1.at[pl.ds(k - 1, 1)],
            send_sem=bsend.at[27 + k - 1],
            recv_sem=v1sem,
            device_id={"scan": chip(x, y + k // 2, (core + k) % 2)},
            device_id_type=MESH,
        )
        copy.start()
        v1_copies.append(copy)
    pltpu.make_async_copy(vec1.at[pl.ds(0, 15)], vec1.at[pl.ds(0, 15)], v1sem).wait()
    for copy in v1_copies:
        copy.wait_send()
    vec[...] = own_sums + jnp.sum(vec1[0:15, :], 0, keepdims=True)
    v2_copies = []
    for k in range(1, side):
        copy = pltpu.make_async_remote_copy(
            src_ref=vec.at[pl.ds(0, 1)],
            dst_ref=vec2.at[pl.ds(k - 1, 1)],
            send_sem=bsend.at[42 + k - 1],
            recv_sem=v2sem,
            device_id={"scan": chip(x + k, y, core)},
            device_id_type=MESH,
        )
        copy.start()
        v2_copies.append(copy)
    for at_lane in range(2):
        source = chip((x % 2) * 4 + core * 2 + at_lane, y, x // 4)
        arrived = pltpu.make_async_copy(dp_in.at[at_lane], dp_in.at[at_lane], dpsem.at[at_lane])
        pl.when(source != me)(arrived.wait)
    pltpu.make_async_copy(vec2.at[pl.ds(0, 7)], vec2.at[pl.ds(0, 7)], v2sem).wait()
    totals = vec[...] + jnp.sum(vec2[0:7, :], 0, keepdims=True)
    uu, uv, vv, uc, vc = (totals[0:1, i : i + 1] for i in range(5))
    a = 1.1 * uu + 1e-06
    d = 1.1 * vv + 1e-06
    det = a * d - uv * uv
    rate_obj = (uc * d - uv * vc) / det
    rate_probe = (a * vc - uv * uc) / det
    at = lax.broadcasted_iota(jnp.int32, (8, LANES), 1)
    rates[...] = jnp.where(at == 0, rate_obj, rate_probe)
    obj_step[...] = dobj[...]
    for part in range(2):
        for at_lane in range(2):
            cols = slice(LANES * at_lane, LANES * at_lane + LANES)
            probe_out[0, part, :, cols] = dp_in[at_lane, part]
            probe_out[1, part, :, cols] = probe[part, out_mode, pl.ds(mult(8 * out_band, 8), 8), cols]

    msg.drain()
    for copy in y_copies + ky_copies + kx_copies + v2_copies:
        copy.wait_send()
    for copy, when in dp_sends + pieces:
        pl.when(when)(copy.wait_send)


def finish_kernel(obj, obj_step, probe_out, rates, new_obj, new_probe):
    rate_obj, rate_probe = rates[0:1, 0:1], rates[0:1, 1:2]
    for part in range(2):
        new_obj[part] = obj[part] + rate_obj * obj_step[part]
        new_probe[part] = probe_out[1, part] + rate_probe * probe_out[0, part]


def finish(obj, obj_step, probe_out, rates):
    vmem = pl.BlockSpec(memory_space=pltpu.VMEM)
    return pl.pallas_call(
        finish_kernel,
        out_shape=(
            jax.ShapeDtypeStruct(obj.shape, F32),
            jax.ShapeDtypeStruct(probe_out.shape[1:], F32),
        ),
        in_specs=[vmem] * 4,
        out_specs=[vmem] * 2,
        name="finish",
    )(obj, obj_step, probe_out, rates)


def step(n, offsets, live, obj, probe, amps, cos, sin):
    vmem = pl.BlockSpec(memory_space=pltpu.VMEM)
    smem = pl.BlockSpec(memory_space=pltpu.SMEM)
    hbm = pl.BlockSpec(memory_space=pl.ANY)
    dma = pltpu.SemaphoreType.DMA
    columns = obj.shape[2]

    def f32(*shape):
        return pltpu.VMEM(shape, F32)

    return pl.pallas_call(
        functools.partial(step_kernel, n),
        out_shape=(
            jax.ShapeDtypeStruct((2, STRIP, columns), F32),
            jax.ShapeDtypeStruct((2, 2, 8, PATCH), F32),
            jax.ShapeDtypeStruct((8, LANES), F32),
        ),
        in_specs=[smem, smem, vmem, hbm, hbm, vmem, vmem],
        out_specs=[vmem] * 3,
        scratch_shapes=[
            pltpu.VMEM((8, LANES), jnp.int32),
            pltpu.VMEM((4 * SPLIT, 8, LANES), jnp.int32),
            pltpu.SMEM((4 * SPLIT, 8, LANES), jnp.int32),
            f32(2, MODES, PATCH, PATCH),
            f32(SPLIT, PATCH, PATCH),
            f32(2, ROWS + 16, WIN),
            f32(2, 2, STRIP, OWN),
            f32(2, ROWS + 16, WIN),
            f32(2, PATCH, PATCH),
            f32(2, PATCH, PATCH),
            f32(PATCH, PATCH),
            f32(2 * MODES + 1, PATCH, PATCH),
            pltpu.VMEM((2 * PATCH, 2 * PATCH), BF16),
            pltpu.VMEM((2 * PATCH, 2 * PATCH), BF16),
            *[pltpu.VMEM((2 * PATCH, PATCH), BF16) for m in range(MODES)],
            *[pltpu.VMEM((PATCH, 2 * PATCH), BF16) for m in range(MODES)],
            *[f32(PATCH, 2 * PATCH) for m in range(MODES)],
            f32(2, 8, 8, 5, 8, LANES),
            f32(2, ROWS, LANES),
            f32(2, STRIP, OWN),
            f32(4, 2, STRIP, OWN),
            f32(2, JITTER, OWN),
            f32(2, 2, STRIP, OWN),
            f32(2, 2, STRIP, OWN),
            f32(4, 2, STRIP, OWN),
            f32(8, 8, 5, 8, LANES),
            f32(8, 8, 5, 8, LANES),
            f32(7, 4, 5, 8, LANES),
            f32(7, 4, 5, 8, LANES),
            f32(7, 5, 8, LANES),
            f32(4, 2, STRIP, OWN),
            f32(2, 2, STRIP, OWN),
            f32(5, 8, LANES),
            f32(2, 2, 8, LANES),
            f32(2, 2, 8, LANES),
            f32(2, 8, LANES),
            f32(8, LANES),
            f32(2, 8, 8, 8, LANES),
            f32(1, KROWS, KCOLS),
            f32(1, STRIP, columns),
            f32(2, STRIP, columns),
            f32(2, STRIP, columns),
            f32(2, KROWS, PATCH),
            f32(PATCH, PATCH),
            f32(8, LANES),
            f32(16, LANES),
            f32(8, LANES),
            dma((48,)),
            dma((48,)),
            dma,
            dma,
            dma,
            dma,
            dma,
            dma((50,)),
            dma((2,)),
            dma((4,)),
            dma((2,)),
            dma((40,)),
            dma((4,)),
            dma((4,)),
            dma((2,)),
            dma((3,)),
            dma,
            dma((16,)),
            dma,
            dma((6,)),
        ],
        compiler_params=pltpu.CompilerParams(collective_id=0, has_side_effects=True),
        name="step",
    )(offsets, live, obj, probe, amps, cos, sin)


def tables(length):
    numbers = np.arange(length, dtype=np.int64)
    angles = (numbers[:, None] * numbers[None, :] % length).astype(np.float32)
    angles = angles * np.float32(2.0 * math.pi / length)
    scaling = np.float32(1.0 / math.sqrt(length))
    return tuple(jnp.asarray(f(angles) * scaling).astype(BF16) for f in (np.cos, np.sin))


def on_device(n, object_field, probe_field, amplitudes, offsets, live_counts):
    probe = probe_field.reshape(2, MODES, PATCH, PATCH)
    cos, sin = tables(PATCH)
    updates = step(n, offsets.T, live_counts, object_field, probe, amplitudes, cos, sin)
    return finish(object_field, *updates)


def solution(mesh):
    groups_scan = ("groups", "scan")
    placed = (
        P(None, groups_scan, None),
        P(None, "groups", None),
        P(groups_scan, None, None),
        P(groups_scan, None),
        P(groups_scan),
    )
    return jax.shard_map(
        functools.partial(on_device, mesh.shape["scan"]),
        mesh=mesh,
        in_specs=placed,
        out_specs=(P(None, groups_scan, None), P(None, groups_scan, None)),
        check_vma=False,
    )
```

```python
import functools
import math

import jax
import jax.numpy as jnp
import numpy as np
from jax import lax
from jax.experimental import pallas as pl
from jax.experimental.pallas import tpu as pltpu
from jax.sharding import PartitionSpec as P

MESH = pl.DeviceIdType.MESH
SPLIT = 4
JITTER = 8
STEP = 96
PATCH = 256
MODES = 4
STRIP = 24
LANES = 128
OWN = 512
WIN = 640
ROWS = JITTER + 2 * STEP + 72
ZTOP = 104
KROWS = 408
KCOLS = 384
F32 = jnp.float32
BF16 = jnp.bfloat16


def mult(value, of):
    return pl.multiple_of(value, of)


class Messages:
    def __init__(self, send, recv):
        self.send, self.recv, self.count, self.open = send, recv, 0, []

    def make(self, src, dst, scan, when=None):
        at = self.count
        self.count += 1
        self.last = self.recv.at[at]
        copy = pltpu.make_async_remote_copy(
            src_ref=src,
            dst_ref=dst,
            send_sem=self.send.at[at],
            recv_sem=self.recv.at[at],
            device_id={"scan": scan},
            device_id_type=MESH,
        )
        self.open.append((copy, when))
        return copy

    def drain(self):
        for copy, when in self.open:
            if when is None:
                copy.wait_send()
            else:
                pl.when(when)(copy.wait_send)
        self.open = []


def greet(peers):
    barrier = pltpu.get_barrier_semaphore()
    for peer in peers:
        pl.semaphore_signal(barrier, inc=1, device_id={"scan": peer}, device_id_type=MESH)
    pl.semaphore_wait(barrier, len(peers))


def long_way(me, step):
    line, at, q = me // 16, (me // SPLIT) % 4, me % SPLIT
    scale = 16

    def device(at_line, at_row):
        return (at_line + 8) % 8 * scale + (at_row + 8) % 4 * SPLIT + q

    def turn(row):
        row = (row + 8) % 4
        return jnp.where(jnp.logical_or(row == 0, row == 3), 0, 1)

    relay = device(line, at - step)
    origin = device(line, at + step)
    target = device(line + step * turn(at), at - step)
    source = device(line - step * turn(at + step), at + step)
    return relay, origin, target, source


def spread(n, kernel_pad, out, metas, line):
    me = lax.axis_index("scan")
    q = me % SPLIT
    line = line + jnp.where(q == SPLIT - 1, 1, 0)
    there = me // SPLIT - 2 + line
    inside = jnp.logical_and(there >= 0, there < n // SPLIT)
    start = mult(STRIP * q + STEP * (2 - line) - JITTER + ZTOP, 8)
    parts = out.shape[0]
    tall = STRIP + 2 * JITTER

    def one(col, carry):
        slot = line * SPLIT + col // SPLIT
        place = col % SPLIT
        top = metas[slot, 0, 2 * place]
        left = metas[slot, 0, 2 * place + 1]
        weight = jnp.where(jnp.logical_and(inside, place < metas[slot, 0, 8]), 1.0, 0.0).astype(F32)
        ahead = jnp.clip(STEP * there - top + JITTER, 0, 2 * JITTER)
        base = mult((STEP * col + 40) // LANES * LANES, LANES)
        shift = jnp.clip(left - base, 0, LANES)
        for part in range(parts):
            value = kernel_pad[part, pl.ds(start, tall), :]
            value = pltpu.roll(value, (tall - ahead) % tall, 0)[0:STRIP]
            value = pltpu.roll(value, shift, 1) * weight
            out[part, :, pl.ds(base, KCOLS)] += value
        return carry

    lax.fori_loop(0, 16, one, 0, unroll=4)


def collect(n, strip, out, metas, line):
    me = lax.axis_index("scan")
    q = me % SPLIT
    line = line + jnp.where(q == SPLIT - 1, 1, 0)
    there = me // SPLIT - 2 + line
    inside = jnp.logical_and(there >= 0, there < n // SPLIT)
    start = mult(STRIP * q + STEP * (2 - line) - JITTER + ZTOP, 8)
    tall = STRIP + 2 * JITTER

    def one(col, carry):
        slot = line * SPLIT + col // SPLIT
        place = col % SPLIT
        top = metas[slot, 0, 2 * place]
        left = metas[slot, 0, 2 * place + 1]
        weight = jnp.where(jnp.logical_and(inside, place < metas[slot, 0, 8]), 1.0, 0.0).astype(F32)
        ahead = jnp.clip(STEP * there - top + JITTER, 0, 2 * JITTER)
        base = mult((STEP * col + 40) // LANES * LANES, LANES)
        shift = jnp.clip(left - base, 0, LANES)
        below = jnp.zeros((2 * JITTER, PATCH), F32)
        for part in range(2):
            value = strip[part, :, pl.ds(base, KCOLS)]
            value = pltpu.roll(value, (KCOLS - shift) % KCOLS, 1)[:, 0:PATCH] * weight
            value = pltpu.roll(jnp.concatenate([value, below], 0), ahead, 0)
            out[part, pl.ds(start, tall), :] += value
        return carry

    lax.fori_loop(0, 16, one, 0, unroll=4)


def step_kernel(
    n, offsets, live, obj, probe_hbm, amps_hbm, cos, sin, obj_step, probe_out, rates,
    meta, metas_in, metas, probe, amps, win, relay_in, grad, patch, share, bright, sums9, ta, tb,
    w0, w1, w2, w3, h0, h1, h2, h3, f0, f1, f2, f3,
    q_in, sib_in, t2_in, t1_in, t8_in, back_in, far_in, piece, q_sib, acc, minus_in, plus_in, y_in, hold_t1, hold_far,
    tile, dp, dp_in, kmine, ksib, kk, kpad, illum, place, dobj, cross, cross_in, vec, vec1, vec2,
    send, recv, ysem, kysem, kxsem, v1sem, v2sem, bsend, dpsem, psem, lsem,
    gsend, ownsem, aheadsem, relaysem, finalsem, tailsem, mrecv, msem, holdsem,
):
    me = lax.axis_index("scan")
    q = me % SPLIT
    core = me % 2
    first = me - q
    row = me // SPLIT
    rows_all = n // SPLIT
    up = (me - SPLIT + n) % n
    down = (me + SPLIT) % n
    sibling = me + 1 - 2 * core
    side = 8
    x, y = me // (2 * side), (me // 2) % side
    msg = Messages(send, recv)

    def chip(at_x, at_y, at_core):
        return ((at_x % side) * side + at_y % side) * 2 + at_core

    def columns(quarter):
        return pl.ds(mult(768 * (quarter // 2) + OWN * (quarter % 2), LANES), OWN)

    def rows(start, size):
        return pl.ds(mult(start, 8), size)

    lanes = lax.broadcasted_iota(jnp.int32, (8, LANES), 1)
    facts = jnp.where(lanes == 2 * SPLIT, live[0], 0)
    for p in range(SPLIT):
        for i in range(2):
            facts = jnp.where(lanes == 2 * p + i, offsets[i, p], facts)
    meta[...] = facts
    load_probe = pltpu.make_async_copy(probe_hbm, probe, lsem.at[0])
    load_probe.start()
    load_amps = pltpu.make_async_copy(amps_hbm, amps, lsem.at[1])
    load_amps.start()
    peers = [(first + SPLIT * e + k + 2 * n) % n for e in (-2, -1, 1, 2) for k in range(SPLIT)]
    peers += [chip(x + k, y, cc) for k in range(1, side) for cc in range(2)]
    peers += [chip(x, y + k, cc) for k in range(1, side) for cc in range(2)]
    peers += [sibling]
    def clear_outside(ref):
        @pl.when(row == 0)
        def _():
            ref[:, 0:JITTER, :] = jnp.zeros((2, JITTER, WIN), F32)

        @pl.when(row == rows_all - 1)
        def _():
            ref[:, JITTER + STEP : JITTER + 2 * STEP, :] = jnp.zeros((2, STEP, WIN), F32)

        @pl.when(row >= rows_all - 2)
        def _():
            ref[:, JITTER + 2 * STEP : ROWS, :] = jnp.zeros((2, 72, WIN), F32)

    clear_outside(win)
    metas_in[...] = jnp.zeros_like(metas_in)
    greet(peers)

    sends = []

    def put(src, dst, recv_sem, there, when=None):
        copy = pltpu.make_async_remote_copy(
            src_ref=src,
            dst_ref=dst,
            send_sem=gsend.at[len(sends)],
            recv_sem=recv_sem,
            device_id={"scan": there},
            device_id_type=MESH,
        )
        sends.append((copy, when))
        if when is None:
            copy.start()
        else:
            pl.when(when)(copy.start)

    def landing(quarter, start, size=STRIP):
        return win.at[:, rows(start, size), pl.ds(mult(LANES * (quarter % 2), LANES), OWN)]

    for e in (-1, 0, 1, 2):
        for k in range(SPLIT):
            if e or k:
                there = (first + SPLIT * e + (q + k) % SPLIT + n) % n
                to = row + e
                known = jnp.logical_and(to >= 0, to < rows_all)
                slot = (2 - e) * SPLIT + q
                put(meta, metas_in.at[slot], mrecv.at[slot], there, when=known)
    relay, origin, target, source = long_way(me, -1)
    above1, above2 = row >= 1, row >= 2
    below1, below2 = row <= rows_all - 2, row <= rows_all - 3
    middle = jnp.logical_and(jnp.logical_or(q == 1, q == 2), above2)
    passing = origin // SPLIT >= 2
    middle_at = jnp.clip(q - 1, 0, 1)
    around = [(q + k) % SPLIT for k in range(SPLIT)]
    for there in around:
        block = obj.at[:, :, columns(there)]
        put(block, relay_in.at[middle_at], relaysem.at[middle_at], relay - q + there, when=middle)
        put(block, landing(there, JITTER + STEP + STRIP * q), aheadsem.at[q], (first - SPLIT + there + n) % n, when=above1)
    for there in around[1:]:
        block = obj.at[:, :, columns(there)]
        put(block, landing(there, JITTER + STRIP * q), ownsem.at[q], first + there)
    for there in around:
        block = obj.at[:, pl.ds(STRIP - JITTER, JITTER), columns(there)]
        put(block, landing(there, 0, JITTER), tailsem, (first + SPLIT + there) % n, when=jnp.logical_and(q == SPLIT - 1, below1))
    own_at = mult(LANES * core, LANES)
    own_cols = pl.ds(own_at, OWN)
    sib_cols = pl.ds(mult(OWN * (1 - core), LANES), LANES)
    win[:, rows(JITTER + STRIP * q, STRIP), own_cols] = obj[:, :, columns(q)]
    metas_in[2 * SPLIT + q] = facts

    c, s = cos[...], sin[...]
    ta[0:256, 0:256] = c
    ta[0:256, 256:512] = s
    ta[256:512, 0:256] = -s
    ta[256:512, 256:512] = c
    tb[0:256, 0:256] = c
    tb[0:256, 256:512] = -s
    tb[256:512, 0:256] = s
    tb[256:512, 256:512] = c
    grad[...] = jnp.zeros_like(grad)
    sums9[...] = jnp.zeros_like(sums9)
    kpad[...] = jnp.zeros_like(kpad)
    illum[...] = jnp.zeros_like(illum)
    cross[...] = jnp.zeros_like(cross)
    dobj[...] = jnp.zeros_like(dobj)
    win[:, ROWS:, :] = jnp.zeros((2, 16, WIN), F32)
    load_probe.wait()
    light = jnp.zeros((PATCH, PATCH), F32)
    for m in range(MODES):
        light = light + (probe[0, m] * probe[0, m] + probe[1, m] * probe[1, m])
    kpad[0, ZTOP : ZTOP + PATCH, 0:PATCH] = light

    def arrived(ref, sem):
        return pltpu.make_async_copy(ref, ref, sem)

    def border(start, size):
        mine = pl.ds(mult(LANES * core + 384 * (1 - core), LANES), LANES)
        src = win.at[:, pl.ds(start, size), mine]
        dst = win.at[:, pl.ds(start, size), pl.ds(mult(OWN * core, LANES), LANES)]
        copy = msg.make(src, dst, sibling)
        copy.start()
        return copy

    def far_on(j):
        pl.when(passing)(arrived(relay_in.at[j - 1], relaysem.at[j - 1]).wait)
        put(relay_in.at[j - 1], landing(q, JITTER + 2 * STEP + STRIP * j), finalsem.at[j], target, when=passing)

    for j in range(SPLIT):
        pl.when(q != j)(arrived(landing(q, JITTER + STRIP * j), ownsem.at[j]).wait)
        if j == 0:
            pl.when(below1)(arrived(landing(q, JITTER + STEP), aheadsem.at[0]).wait)
            onward = jnp.logical_and(above1, below1)
            put(landing(q, JITTER + STEP), landing(q, JITTER + 2 * STEP), finalsem.at[0], up, when=onward)
            far_on(1)
        if j == 1:
            far_on(2)
    borders = [border(JITTER, STEP)]
    pl.when(above1)(arrived(landing(q, 0, JITTER), tailsem).wait)
    borders.append(border(0, JITTER))
    for j in range(1, SPLIT):
        pl.when(below1)(arrived(landing(q, JITTER + STEP + STRIP * j), aheadsem.at[j]).wait)
    borders.append(border(JITTER + STEP, STEP))
    for j in range(3):
        pl.when(below2)(arrived(landing(q, JITTER + 2 * STEP + STRIP * j), finalsem.at[j]).wait)
    borders.append(border(JITTER + 2 * STEP, 72))
    for line in range(4):
        there = row - 2 + line
        known = jnp.logical_and(there >= 0, there < rows_all)
        for at in range(SPLIT):
            slot = line * SPLIT + at
            other = known if line != 2 else q != at
            pl.when(other)(arrived(metas_in.at[slot], mrecv.at[slot]).wait)
    to_smem = pltpu.make_async_copy(metas_in, metas, msem)
    to_smem.start()
    load_amps.wait()
    for copy in borders:
        copy.wait_recv()

    msg.drain()
    for copy, when in sends:
        if when is None:
            copy.wait_send()
        else:
            pl.when(when)(copy.wait_send)

    wave, half_done, far = (w0, w1, w2, w3), (h0, h1, h2, h3), (f0, f1, f2, f3)
    chunk = 32
    chunks = PATCH // chunk
    slab = chunk + 2 * JITTER

    def visit(p, carry):
        ahead = jnp.clip(offsets[0, p] - (STEP * row - JITTER), 0, 2 * JITTER)
        base = mult((STEP * p + 40) // LANES * LANES, LANES)
        shift = jnp.clip(offsets[1, p] - STEP * SPLIT * q - base, 0, LANES)
        weight = jnp.where(p < live[0], 1.0, 0.0).astype(F32)
        steps = [slice(i * chunk, (i + 1) * chunk) for i in range(chunks)]
        lows = [slice(PATCH + i * chunk, PATCH + (i + 1) * chunk) for i in range(chunks)]
        left_half, right_half = slice(0, PATCH), slice(PATCH, 2 * PATCH)

        def across(table, m):
            z = jnp.dot(table[...], wave[m][...], preferred_element_type=F32)
            half_done[m][:, left_half] = z[left_half].astype(BF16)
            half_done[m][:, right_half] = z[right_half].astype(BF16)

        def along(table, m):
            far[m][...] = jnp.dot(half_done[m][...], table[...], preferred_element_type=F32)

        for i, at in enumerate(steps):
            for part in range(2):
                v = win[part, i * chunk : i * chunk + slab, pl.ds(base, KCOLS)]
                v = pltpu.roll(v, (slab - ahead) % slab, 0)[0:chunk]
                patch[part, at, :] = pltpu.roll(v, KCOLS - shift, 1)[:, 0:PATCH]
        for m in range(MODES):
            for at, low in zip(steps, lows):
                pr, pi = probe[0, m, at, :], probe[1, m, at, :]
                o_re, o_im = patch[0, at, :], patch[1, at, :]
                wave[m][at, :] = (pr * o_re - pi * o_im).astype(BF16)
                wave[m][low, :] = (pr * o_im + pi * o_re).astype(BF16)
            across(ta, m)
        for m in range(MODES):
            along(tb, m)
            for at in steps:
                fr, fi = far[m][at, left_half], far[m][at, right_half]
                power = fr * fr + fi * fi
                bright[at, :] = power if m == 0 else bright[at, :] + power
        for m in range(MODES):
            for at, low in zip(steps, lows):
                if m == 0:
                    root = jnp.maximum(jnp.sqrt(bright[at, :]), 0.5)
                    factor = (amps[p, at, :] / root - 1.0) * weight
                    bright[at, :] = factor
                else:
                    factor = bright[at, :]
                wave[m][at, :] = (far[m][at, left_half] * factor).astype(BF16)
                wave[m][low, :] = (far[m][at, right_half] * factor).astype(BF16)
            across(tb, m)
        for m in range(MODES):
            along(ta, m)
            for at in steps:
                pr, pi = probe[0, m, at, :], probe[1, m, at, :]
                o_re, o_im = patch[0, at, :], patch[1, at, :]
                cr, ci = far[m][at, left_half], far[m][at, right_half]
                g_re = pr * cr + pi * ci
                g_im = pr * ci - pi * cr
                if m > 0:
                    g_re = g_re + share[0, at, :]
                    g_im = g_im + share[1, at, :]
                share[0, at, :] = g_re
                share[1, at, :] = g_im
                sums9[m, at, :] += o_re * cr + o_im * ci
                sums9[MODES + m, at, :] += o_re * ci - o_im * cr
        blank = jnp.zeros((chunk, KCOLS - PATCH), F32)
        below = jnp.zeros((2 * JITTER, KCOLS), F32)
        for i, at in enumerate(steps):
            o_re, o_im = patch[0, at, :], patch[1, at, :]
            sums9[2 * MODES, at, :] += (o_re * o_re + o_im * o_im) * weight
            for part in range(2):
                v = pltpu.roll(jnp.concatenate([share[part, at, :], blank], 1), shift, 1)
                v = pltpu.roll(jnp.concatenate([v, below], 0), ahead, 0)
                grad[part, i * chunk : i * chunk + slab, pl.ds(base, KCOLS)] += v
        return carry

    lax.fori_loop(0, SPLIT, visit, 0)
    clear_outside(grad)

    for at_band in range(PATCH // 8):
        yy = (at_band // 2) % 8
        for at_lane in range(2):
            xx = (at_band // 16) * 4 + (at_band % 2) * 2 + at_lane
            at_rows = slice(8 * at_band, 8 * at_band + 8)
            at_cols = slice(LANES * at_lane, LANES * at_lane + LANES)
            for k in range(2):
                for i, m in enumerate((2 * k, 2 * k + 1, MODES + 2 * k, MODES + 2 * k + 1, 8)):
                    q_in[k, xx, yy, i] = sums9[m, at_rows, at_cols]
    chunks = [(x + k) % side for k in (4, 5, 3, 6, 2, 7, 1, 0)]
    q_copies = []
    for at in chunks:
        copy = msg.make(q_in.at[1 - core, at], q_sib.at[at], sibling)
        copy.start()
        q_copies.append(copy)
        if not q_copies[1:]:
            to_sib = msg.make(grad.at[:, pl.ds(0, ROWS), sib_cols], sib_in, sibling)
            to_sib.start()
    relay, origin, target, source = long_way(me, 1)

    band = (x // 4) * 16 + y * 2 + (x // 2) % 2
    lane = x % 2
    out_mode = x // 2
    out_band = (x % 2) * 16 + y * 2 + core
    p_tile = probe[:, pl.ds(2 * core, 2), pl.ds(mult(8 * band, 8), 8), pl.ds(mult(LANES * lane, LANES), LANES)]

    def sums(start):
        return grad.at[:, pl.ds(start, STRIP), own_cols]

    def add_sibling(i):
        q_copies[i].wait_recv()
        acc[chunks[i]] = q_in[core, chunks[i]] + q_sib[chunks[i]]

    halves = side // 2

    def send_chain(way, i):
        which = (i % 2 if way < 0 else 1 - i % 2) * halves
        reach = (4 if i % 2 == 0 else 3) - i // 2
        dest = (x + way * reach + side) % side
        copy = msg.make(
            acc.at[dest, pl.ds(which, halves)],
            (minus_in if way < 0 else plus_in).at[i],
            chip(x + way + side, y, core),
        )
        copy.start()
        return copy

    chains = {}
    add_sibling(0)
    chains[-1, 0], chains[1, 0] = send_chain(-1, 0), send_chain(1, 0)
    add_sibling(1)
    chains[-1, 1] = send_chain(-1, 1)
    add_sibling(2)
    chains[1, 1] = send_chain(1, 1)
    to_sib.wait_recv()
    edge = pl.ds(mult(LANES * core + 384 * (1 - core), LANES), LANES)
    grad[:, 0:ROWS, edge] += sib_in[...]

    far_out = []
    for j in (1, 2):
        copy = msg.make(sums(JITTER + 2 * STEP + STRIP * j), back_in.at[j - 1], relay)
        copy.start()
        far_out.append(copy)
    t2 = msg.make(sums(JITTER + 2 * STEP), t2_in, down)
    t2.start()
    t8 = msg.make(grad.at[:, pl.ds(0, JITTER), own_cols], t8_in, up)
    t8.start()

    at_row = (me // SPLIT) % 4
    crossing = at_row == 3
    holder = at_row == 0
    turning = jnp.logical_or(at_row == 1, at_row == 2)
    far_holder = at_row <= 1
    below = x * 2 * side + (at_row + 1) % 4 * SPLIT + q
    beside = chip(x + 1, y, core)

    def start_t1(j):
        src = sums(JITTER + STEP + STRIP * j)
        t1[j] = msg.make(src, t1_in.at[j], below, when=jnp.logical_not(crossing))
        final_sem = msg.last
        pl.when(jnp.logical_not(crossing))(t1[j].start)
        copy = msg.make(src, hold_t1.at[j], below, when=crossing)
        pl.when(crossing)(copy.start)
        held.append((copy, holder, hold_t1.at[j], t1_in.at[j], final_sem))

    def pass_far(j):
        there = x * 2 * side + (at_row + 3) % 4 * SPLIT + q
        final = msg.make(back_in.at[j], far_in.at[j], there, when=jnp.logical_not(turning))
        final_sem = msg.last
        pl.when(jnp.logical_not(turning))(final.start)
        copy = msg.make(back_in.at[j], hold_far.at[j], there, when=turning)
        pl.when(turning)(copy.start)
        held.append((copy, far_holder, hold_far.at[j], far_in.at[j], final_sem))
        return final

    def release(i):
        copy, here, src, dst, final_sem = held[i]
        pl.when(here)(copy.wait_recv)
        onward = pltpu.make_async_remote_copy(
            src_ref=src,
            dst_ref=dst,
            send_sem=holdsem.at[i],
            recv_sem=final_sem,
            device_id={"scan": beside},
            device_id_type=MESH,
        )
        pl.when(here)(onward.start)
        msg.open.append((onward, here))

    t1, held = {}, []
    start_t1(3)
    for i in range(3, 8):
        add_sibling(i)

    def x_step(i):
        for way, arrived in ((-1, minus_in), (1, plus_in)):
            which = (i % 2 if way < 0 else 1 - i % 2) * halves
            reach = (4 if i % 2 == 0 else 3) - 1 - i // 2
            dest = (x + way * reach + side) % side
            chains[way, i].wait_recv()
            acc[dest, which : which + halves] += arrived[i]
            if reach > 0:
                chains[way, i + 2] = send_chain(way, i + 2)

    to_smem.wait()
    x_step(0)
    start_t1(1)
    spread(n, kpad, illum, metas, 0)
    x_step(1)
    start_t1(2)
    spread(n, kpad, illum, metas, 1)
    x_step(2)
    t2.wait_recv()
    grad[:, JITTER + STEP : JITTER + STEP + STRIP, own_cols] += t2_in[...]
    x_step(3)
    far_final = []
    for j in range(2):
        far_out[j].wait_recv()
        far_final.append(pass_far(j))
    x_step(4)
    spread(n, kpad, illum, metas, 2)
    x_step(5)
    x_step(6)

    y_copies = []
    for k in range(1, side):
        copy = pltpu.make_async_remote_copy(
            src_ref=acc.at[x, (y + k) % side],
            dst_ref=y_in.at[k - 1],
            send_sem=bsend.at[k - 1],
            recv_sem=ysem,
            device_id={"scan": chip(x, y + k, core)},
            device_id_type=MESH,
        )
        copy.start()
        y_copies.append(copy)
    start_t1(0)
    for i in range(3):
        release(i)
    pltpu.make_async_copy(y_in, y_in, ysem).wait()
    release(3)
    release(4)
    tile[...] = acc[x, y] + jnp.sum(y_in[...], 0)
    norm = tile[4]
    inverse = norm + 1.0
    k_re = jnp.zeros((8, LANES), F32)
    k_im = jnp.zeros((8, LANES), F32)
    s_vv = jnp.zeros((8, LANES), F32)
    s_vc = jnp.zeros((8, LANES), F32)
    for m in range(2):
        g_re, g_im = tile[m], tile[2 + m]
        d_re, d_im = g_re / inverse, g_im / inverse
        dp[m, 0] = d_re
        dp[m, 1] = d_im
        p_re, p_im = p_tile[0, m], p_tile[1, m]
        k_re = k_re + (p_re * d_re + p_im * d_im)
        k_im = k_im + (p_re * d_im - p_im * d_re)
        s_vv = s_vv + (d_re * d_re + d_im * d_im) * norm
        s_vc = s_vc + (d_re * g_re + d_im * g_im)
    kmine[0] = k_re
    kmine[1] = k_im
    k_copy = msg.make(kmine.at[1 - core], ksib, sibling)
    k_copy.start()

    dp_sends = []
    for m in range(2):
        dest = chip(2 * (2 * core + m) + x // 4, y, (x // 2) % 2)
        away = dest != me
        copy = pltpu.make_async_remote_copy(
            src_ref=dp.at[m],
            dst_ref=dp_in.at[lane],
            send_sem=bsend.at[21 + m],
            recv_sem=dpsem.at[lane],
            device_id={"scan": dest},
            device_id_type=MESH,
        )
        pl.when(away)(copy.start)
        dp_sends.append((copy, away))

        @pl.when(jnp.logical_not(away))
        def _():
            dp_in[lane] = dp[m]

    k_copy.wait_recv()
    kk[core, x, y] = kmine[core] + ksib[...]
    ky_copies = []
    for k in range(1, side):
        copy = pltpu.make_async_remote_copy(
            src_ref=kk.at[core, x, y],
            dst_ref=kk.at[core, x, y],
            send_sem=bsend.at[7 + k - 1],
            recv_sem=kysem,
            device_id={"scan": chip(x, y + k, core)},
            device_id_type=MESH,
        )
        copy.start()
        ky_copies.append(copy)

    release(5)
    pltpu.make_async_copy(kk.at[0, 0, pl.ds(0, 7)], kk.at[0, 0, pl.ds(0, 7)], kysem).wait()
    kx_copies = []
    for k in range(1, side):
        copy = pltpu.make_async_remote_copy(
            src_ref=kk.at[core, x],
            dst_ref=kk.at[core, x],
            send_sem=bsend.at[14 + k - 1],
            recv_sem=kxsem,
            device_id={"scan": chip(x + k, y, core)},
            device_id_type=MESH,
        )
        copy.start()
        kx_copies.append(copy)
    pieces = []
    for j in (3, 1, 2, 0):
        t1[j].wait_recv()
        lo = JITTER + STRIP * j
        grad[:, lo : lo + STRIP, own_cols] += t1_in[j]
        if j == 3:
            t8.wait_recv()
            grad[:, STEP : STEP + JITTER, own_cols] += t8_in[...]
        if j in (1, 2):
            far_final[j - 1].wait_recv()
            grad[:, lo : lo + STRIP, own_cols] += far_in[j - 1]
        slot = (j - q + SPLIT) % SPLIT
        copy = pltpu.make_async_remote_copy(
            src_ref=grad.at[:, pl.ds(lo, STRIP), own_cols],
            dst_ref=piece.at[slot],
            send_sem=bsend.at[23 + j],
            recv_sem=psem.at[slot],
            device_id={"scan": first + j},
            device_id_type=MESH,
        )
        pl.when(q != j)(copy.start)
        pieces.append((copy, q != j))

    piece[0] = grad[:, pl.ds(mult(JITTER + STRIP * q, 8), STRIP), own_cols]

    for k in range(SPLIT):
        if k > 0:
            pltpu.make_async_copy(piece.at[k], piece.at[k], psem.at[k]).wait()
        source = (q - k + SPLIT) % SPLIT
        at = pl.ds(mult(768 * (source // 2) + OWN * (source % 2), LANES), OWN)
        dobj[:, :, at] += piece[k]
    lit = illum[0]
    g_re, g_im = dobj[0], dobj[1]
    o_re, o_im = obj[0], obj[1]
    d_re, d_im = g_re / (lit + 1.0), g_im / (lit + 1.0)
    s_uu = jnp.sum((d_re * d_re + d_im * d_im) * lit)
    s_uc = jnp.sum(d_re * g_re + d_im * g_im)
    dobj[0] = d_re
    dobj[1] = d_im

    place[0] = d_re * o_re + d_im * o_im
    place[1] = d_re * o_im - d_im * o_re
    for line in range(3):
        collect(n, place, cross, metas, line)
    cross_copy = msg.make(cross.at[1 - core, pl.ds(ZTOP, PATCH)], cross_in, sibling)
    cross_copy.start()
    pltpu.make_async_copy(kk.at[0, pl.ds(0, 7)], kk.at[0, pl.ds(0, 7)], kxsem).wait()
    cross_copy.wait_recv()
    product = jnp.zeros((8, LANES), F32)
    for at_band in range(PATCH // 8):
        for at_lane in range(2):
            xx = (at_band // 16) * 4 + (at_band % 2) * 2 + at_lane
            yy = (at_band // 2) % 8
            rows_at = slice(8 * at_band, 8 * at_band + 8)
            cols = slice(LANES * at_lane, LANES * at_lane + LANES)
            both = cross[core, ZTOP + 8 * at_band : ZTOP + 8 * at_band + 8, cols] + cross_in[rows_at, cols]
            product = product + kk[core, xx, yy] * both
    s_uv = jnp.sum(product) * jnp.where(core == 0, 1.0, -1.0).astype(F32)

    at = lax.broadcasted_iota(jnp.int32, (8, LANES), 1)
    own_sums = jnp.zeros((8, LANES), F32)
    for i, value in enumerate((s_uu, s_uv, jnp.sum(s_vv), s_uc, jnp.sum(s_vc))):
        own_sums = jnp.where(at == i, value, own_sums)
    vec[...] = own_sums
    v1_copies = []
    for k in range(1, 2 * side):
        copy = pltpu.make_async_remote_copy(
            src_ref=vec.at[pl.ds(0, 1)],
            dst_ref=vec1.at[pl.ds(k - 1, 1)],
            send_sem=bsend.at[27 + k - 1],
            recv_sem=v1sem,
            device_id={"scan": chip(x, y + k // 2, (core + k) % 2)},
            device_id_type=MESH,
        )
        copy.start()
        v1_copies.append(copy)
    pltpu.make_async_copy(vec1.at[pl.ds(0, 15)], vec1.at[pl.ds(0, 15)], v1sem).wait()
    for copy in v1_copies:
        copy.wait_send()
    vec[...] = own_sums + jnp.sum(vec1[0:15, :], 0, keepdims=True)
    v2_copies = []
    for k in range(1, side):
        copy = pltpu.make_async_remote_copy(
            src_ref=vec.at[pl.ds(0, 1)],
            dst_ref=vec2.at[pl.ds(k - 1, 1)],
            send_sem=bsend.at[42 + k - 1],
            recv_sem=v2sem,
            device_id={"scan": chip(x + k, y, core)},
            device_id_type=MESH,
        )
        copy.start()
        v2_copies.append(copy)
    for at_lane in range(2):
        source = chip((x % 2) * 4 + core * 2 + at_lane, y, x // 4)
        arrived = pltpu.make_async_copy(dp_in.at[at_lane], dp_in.at[at_lane], dpsem.at[at_lane])
        pl.when(source != me)(arrived.wait)
    pltpu.make_async_copy(vec2.at[pl.ds(0, 7)], vec2.at[pl.ds(0, 7)], v2sem).wait()
    totals = vec[...] + jnp.sum(vec2[0:7, :], 0, keepdims=True)
    uu, uv, vv, uc, vc = (totals[0:1, i : i + 1] for i in range(5))
    a = 1.1 * uu + 1e-06
    d = 1.1 * vv + 1e-06
    det = a * d - uv * uv
    rate_obj = (uc * d - uv * vc) / det
    rate_probe = (a * vc - uv * uc) / det
    at = lax.broadcasted_iota(jnp.int32, (8, LANES), 1)
    rates[...] = jnp.where(at == 0, rate_obj, rate_probe)
    obj_step[...] = dobj[...]
    for part in range(2):
        for at_lane in range(2):
            cols = slice(LANES * at_lane, LANES * at_lane + LANES)
            probe_out[0, part, :, cols] = dp_in[at_lane, part]
            probe_out[1, part, :, cols] = probe[part, out_mode, pl.ds(mult(8 * out_band, 8), 8), cols]

    msg.drain()
    for copy in y_copies + ky_copies + kx_copies + v2_copies:
        copy.wait_send()
    for copy, when in dp_sends + pieces:
        pl.when(when)(copy.wait_send)


def finish_kernel(obj, obj_step, probe_out, rates, new_obj, new_probe):
    rate_obj, rate_probe = rates[0:1, 0:1], rates[0:1, 1:2]
    for part in range(2):
        new_obj[part] = obj[part] + rate_obj * obj_step[part]
        new_probe[part] = probe_out[1, part] + rate_probe * probe_out[0, part]


def finish(obj, obj_step, probe_out, rates):
    vmem = pl.BlockSpec(memory_space=pltpu.VMEM)
    return pl.pallas_call(
        finish_kernel,
        out_shape=(
            jax.ShapeDtypeStruct(obj.shape, F32),
            jax.ShapeDtypeStruct(probe_out.shape[1:], F32),
        ),
        in_specs=[vmem] * 4,
        out_specs=[vmem] * 2,
        name="finish",
    )(obj, obj_step, probe_out, rates)


def step(n, offsets, live, obj, probe, amps, cos, sin):
    vmem = pl.BlockSpec(memory_space=pltpu.VMEM)
    smem = pl.BlockSpec(memory_space=pltpu.SMEM)
    hbm = pl.BlockSpec(memory_space=pl.ANY)
    dma = pltpu.SemaphoreType.DMA
    columns = obj.shape[2]

    def f32(*shape):
        return pltpu.VMEM(shape, F32)

    return pl.pallas_call(
        functools.partial(step_kernel, n),
        out_shape=(
            jax.ShapeDtypeStruct((2, STRIP, columns), F32),
            jax.ShapeDtypeStruct((2, 2, 8, PATCH), F32),
            jax.ShapeDtypeStruct((8, LANES), F32),
        ),
        in_specs=[smem, smem, vmem, hbm, hbm, vmem, vmem],
        out_specs=[vmem] * 3,
        scratch_shapes=[
            pltpu.VMEM((8, LANES), jnp.int32),
            pltpu.VMEM((4 * SPLIT, 8, LANES), jnp.int32),
            pltpu.SMEM((4 * SPLIT, 8, LANES), jnp.int32),
            f32(2, MODES, PATCH, PATCH),
            f32(SPLIT, PATCH, PATCH),
            f32(2, ROWS + 16, WIN),
            f32(2, 2, STRIP, OWN),
            f32(2, ROWS + 16, WIN),
            f32(2, PATCH, PATCH),
            f32(2, PATCH, PATCH),
            f32(PATCH, PATCH),
            f32(2 * MODES + 1, PATCH, PATCH),
            pltpu.VMEM((2 * PATCH, 2 * PATCH), BF16),
            pltpu.VMEM((2 * PATCH, 2 * PATCH), BF16),
            *[pltpu.VMEM((2 * PATCH, PATCH), BF16) for m in range(MODES)],
            *[pltpu.VMEM((PATCH, 2 * PATCH), BF16) for m in range(MODES)],
            *[f32(PATCH, 2 * PATCH) for m in range(MODES)],
            f32(2, 8, 8, 5, 8, LANES),
            f32(2, ROWS, LANES),
            f32(2, STRIP, OWN),
            f32(4, 2, STRIP, OWN),
            f32(2, JITTER, OWN),
            f32(2, 2, STRIP, OWN),
            f32(2, 2, STRIP, OWN),
            f32(4, 2, STRIP, OWN),
            f32(8, 8, 5, 8, LANES),
            f32(8, 8, 5, 8, LANES),
            f32(7, 4, 5, 8, LANES),
            f32(7, 4, 5, 8, LANES),
            f32(7, 5, 8, LANES),
            f32(4, 2, STRIP, OWN),
            f32(2, 2, STRIP, OWN),
            f32(5, 8, LANES),
            f32(2, 2, 8, LANES),
            f32(2, 2, 8, LANES),
            f32(2, 8, LANES),
            f32(8, LANES),
            f32(2, 8, 8, 8, LANES),
            f32(1, KROWS, KCOLS),
            f32(1, STRIP, columns),
            f32(2, STRIP, columns),
            f32(2, STRIP, columns),
            f32(2, KROWS, PATCH),
            f32(PATCH, PATCH),
            f32(8, LANES),
            f32(16, LANES),
            f32(8, LANES),
            dma((48,)),
            dma((48,)),
            dma,
            dma,
            dma,
            dma,
            dma,
            dma((50,)),
            dma((2,)),
            dma((4,)),
            dma((2,)),
            dma((40,)),
            dma((4,)),
            dma((4,)),
            dma((2,)),
            dma((3,)),
            dma,
            dma((16,)),
            dma,
            dma((6,)),
        ],
        compiler_params=pltpu.CompilerParams(collective_id=0, has_side_effects=True),
        name="step",
    )(offsets, live, obj, probe, amps, cos, sin)


def tables(length):
    numbers = np.arange(length, dtype=np.int64)
    angles = (numbers[:, None] * numbers[None, :] % length).astype(np.float32)
    angles = angles * np.float32(2.0 * math.pi / length)
    scaling = np.float32(1.0 / math.sqrt(length))
    return tuple(jnp.asarray(f(angles) * scaling).astype(BF16) for f in (np.cos, np.sin))


def on_device(n, object_field, probe_field, amplitudes, offsets, live_counts):
    probe = probe_field.reshape(2, MODES, PATCH, PATCH)
    cos, sin = tables(PATCH)
    updates = step(n, offsets.T, live_counts, object_field, probe, amplitudes, cos, sin)
    return finish(object_field, *updates)


def solution(mesh):
    groups_scan = ("groups", "scan")
    placed = (
        P(None, groups_scan, None),
        P(None, "groups", None),
        P(groups_scan, None, None),
        P(groups_scan, None),
        P(groups_scan),
    )
    return jax.shard_map(
        functools.partial(on_device, mesh.shape["scan"]),
        mesh=mesh,
        in_specs=placed,
        out_specs=(P(None, groups_scan, None), P(None, groups_scan, None)),
        check_vma=False,
    )
```

```python
import functools
import math

import jax
import jax.numpy as jnp
import numpy as np
from jax import lax
from jax.experimental import pallas as pl
from jax.experimental.pallas import tpu as pltpu
from jax.sharding import PartitionSpec as P

MESH = pl.DeviceIdType.MESH
SPLIT = 4
JITTER = 8
STEP = 96
PATCH = 256
MODES = 4
STRIP = 24
LANES = 128
OWN = 512
WIN = 640
ROWS = JITTER + 2 * STEP + 72
ZTOP = 104
KROWS = 408
KCOLS = 384
F32 = jnp.float32
BF16 = jnp.bfloat16


def mult(value, of):
    return pl.multiple_of(value, of)


class Messages:
    def __init__(self, send, recv):
        self.send, self.recv, self.count, self.open = send, recv, 0, []

    def make(self, src, dst, scan, when=None):
        at = self.count
        self.count += 1
        self.last = self.recv.at[at]
        copy = pltpu.make_async_remote_copy(
            src_ref=src,
            dst_ref=dst,
            send_sem=self.send.at[at],
            recv_sem=self.recv.at[at],
            device_id={"scan": scan},
            device_id_type=MESH,
        )
        self.open.append((copy, when))
        return copy

    def drain(self):
        for copy, when in self.open:
            if when is None:
                copy.wait_send()
            else:
                pl.when(when)(copy.wait_send)
        self.open = []


def greet(peers):
    barrier = pltpu.get_barrier_semaphore()
    for peer in peers:
        pl.semaphore_signal(barrier, inc=1, device_id={"scan": peer}, device_id_type=MESH)
    pl.semaphore_wait(barrier, len(peers))


def long_way(me, step):
    line, at, q = me // 16, (me // SPLIT) % 4, me % SPLIT
    scale = 16

    def device(at_line, at_row):
        return (at_line + 8) % 8 * scale + (at_row + 8) % 4 * SPLIT + q

    def turn(row):
        row = (row + 8) % 4
        return jnp.where(jnp.logical_or(row == 0, row == 3), 0, 1)

    relay = device(line, at - step)
    origin = device(line, at + step)
    target = device(line + step * turn(at), at - step)
    source = device(line - step * turn(at + step), at + step)
    return relay, origin, target, source


def spread(n, kernel_pad, out, metas, line):
    me = lax.axis_index("scan")
    q = me % SPLIT
    line = line + jnp.where(q == SPLIT - 1, 1, 0)
    there = me // SPLIT - 2 + line
    inside = jnp.logical_and(there >= 0, there < n // SPLIT)
    start = mult(STRIP * q + STEP * (2 - line) - JITTER + ZTOP, 8)
    parts = out.shape[0]
    tall = STRIP + 2 * JITTER

    def one(col, carry):
        slot = line * SPLIT + col // SPLIT
        place = col % SPLIT
        top = metas[slot, 0, 2 * place]
        left = metas[slot, 0, 2 * place + 1]
        weight = jnp.where(jnp.logical_and(inside, place < metas[slot, 0, 8]), 1.0, 0.0).astype(F32)
        ahead = jnp.clip(STEP * there - top + JITTER, 0, 2 * JITTER)
        base = mult((STEP * col + 40) // LANES * LANES, LANES)
        shift = jnp.clip(left - base, 0, LANES)
        for part in range(parts):
            value = kernel_pad[part, pl.ds(start, tall), :]
            value = pltpu.roll(value, (tall - ahead) % tall, 0)[0:STRIP]
            value = pltpu.roll(value, shift, 1) * weight
            out[part, :, pl.ds(base, KCOLS)] += value
        return carry

    lax.fori_loop(0, 16, one, 0, unroll=4)


def collect(n, strip, out, metas, line):
    me = lax.axis_index("scan")
    q = me % SPLIT
    line = line + jnp.where(q == SPLIT - 1, 1, 0)
    there = me // SPLIT - 2 + line
    inside = jnp.logical_and(there >= 0, there < n // SPLIT)
    start = mult(STRIP * q + STEP * (2 - line) - JITTER + ZTOP, 8)
    tall = STRIP + 2 * JITTER

    def one(col, carry):
        slot = line * SPLIT + col // SPLIT
        place = col % SPLIT
        top = metas[slot, 0, 2 * place]
        left = metas[slot, 0, 2 * place + 1]
        weight = jnp.where(jnp.logical_and(inside, place < metas[slot, 0, 8]), 1.0, 0.0).astype(F32)
        ahead = jnp.clip(STEP * there - top + JITTER, 0, 2 * JITTER)
        base = mult((STEP * col + 40) // LANES * LANES, LANES)
        shift = jnp.clip(left - base, 0, LANES)
        below = jnp.zeros((2 * JITTER, PATCH), F32)
        summed = []
        for part in range(2):
            value = strip[part, :, pl.ds(base, KCOLS)]
            value = pltpu.roll(value, (KCOLS - shift) % KCOLS, 1)[:, 0:PATCH] * weight
            value = pltpu.roll(jnp.concatenate([value, below], 0), ahead, 0)
            summed.append(carry[part] + value)
        return tuple(summed)

    blank = jnp.zeros((tall, PATCH), F32)
    total = lax.fori_loop(0, 16, one, (blank, blank), unroll=4)
    for part in range(2):
        out[part, pl.ds(start, tall), :] += total[part]


def step_kernel(
    n, offsets, live, obj, probe_hbm, amps_hbm, cos, sin, obj_step, probe_out, rates,
    meta, metas_in, metas, probe, amps, win, relay_in, grad, patch, share, bright, sums9, ta, tb,
    w0, w1, w2, w3, h0, h1, h2, h3, f0, f1, f2, f3,
    q_in, sib_in, t2_in, t1_in, t8_in, back_in, far_in, piece, q_sib, acc, minus_in, plus_in, y_in, hold_t1, hold_far,
    tile, dp, dp_in, kmine, ksib, kk, kpad, illum, place, dobj, cross, cross_in, vec, vec1, vec2,
    send, recv, ysem, kysem, kxsem, v1sem, v2sem, bsend, dpsem, psem, lsem,
    gsend, ownsem, aheadsem, relaysem, finalsem, tailsem, mrecv, msem, holdsem,
):
    me = lax.axis_index("scan")
    q = me % SPLIT
    core = me % 2
    first = me - q
    row = me // SPLIT
    rows_all = n // SPLIT
    up = (me - SPLIT + n) % n
    down = (me + SPLIT) % n
    sibling = me + 1 - 2 * core
    side = 8
    x, y = me // (2 * side), (me // 2) % side
    msg = Messages(send, recv)

    def chip(at_x, at_y, at_core):
        return ((at_x % side) * side + at_y % side) * 2 + at_core

    def columns(quarter):
        return pl.ds(mult(768 * (quarter // 2) + OWN * (quarter % 2), LANES), OWN)

    def rows(start, size):
        return pl.ds(mult(start, 8), size)

    lanes = lax.broadcasted_iota(jnp.int32, (8, LANES), 1)
    facts = jnp.where(lanes == 2 * SPLIT, live[0], 0)
    for p in range(SPLIT):
        for i in range(2):
            facts = jnp.where(lanes == 2 * p + i, offsets[i, p], facts)
    meta[...] = facts
    load_probe = pltpu.make_async_copy(probe_hbm, probe, lsem.at[0])
    load_probe.start()
    load_amps = pltpu.make_async_copy(amps_hbm, amps, lsem.at[1])
    load_amps.start()
    peers = [(first + SPLIT * e + k + 2 * n) % n for e in (-2, -1, 1, 2) for k in range(SPLIT)]
    peers += [chip(x + k, y, cc) for k in range(1, side) for cc in range(2)]
    peers += [chip(x, y + k, cc) for k in range(1, side) for cc in range(2)]
    peers += [sibling]
    def clear_outside(ref):
        @pl.when(row == 0)
        def _():
            ref[:, 0:JITTER, :] = jnp.zeros((2, JITTER, WIN), F32)

        @pl.when(row == rows_all - 1)
        def _():
            ref[:, JITTER + STEP : JITTER + 2 * STEP, :] = jnp.zeros((2, STEP, WIN), F32)

        @pl.when(row >= rows_all - 2)
        def _():
            ref[:, JITTER + 2 * STEP : ROWS, :] = jnp.zeros((2, 72, WIN), F32)

    clear_outside(win)
    metas_in[...] = jnp.zeros_like(metas_in)
    greet(peers)

    sends = []

    def put(src, dst, recv_sem, there, when=None):
        copy = pltpu.make_async_remote_copy(
            src_ref=src,
            dst_ref=dst,
            send_sem=gsend.at[len(sends)],
            recv_sem=recv_sem,
            device_id={"scan": there},
            device_id_type=MESH,
        )
        sends.append((copy, when))
        if when is None:
            copy.start()
        else:
            pl.when(when)(copy.start)

    def landing(quarter, start, size=STRIP):
        return win.at[:, rows(start, size), pl.ds(mult(LANES * (quarter % 2), LANES), OWN)]

    for e in (-1, 0, 1, 2):
        for k in range(SPLIT):
            if e or k:
                there = (first + SPLIT * e + (q + k) % SPLIT + n) % n
                to = row + e
                known = jnp.logical_and(to >= 0, to < rows_all)
                slot = (2 - e) * SPLIT + q
                put(meta, metas_in.at[slot], mrecv.at[slot], there, when=known)
    relay, origin, target, source = long_way(me, -1)
    above1, above2 = row >= 1, row >= 2
    below1, below2 = row <= rows_all - 2, row <= rows_all - 3
    middle = jnp.logical_and(jnp.logical_or(q == 1, q == 2), above2)
    passing = origin // SPLIT >= 2
    middle_at = jnp.clip(q - 1, 0, 1)
    around = [(q + k) % SPLIT for k in range(SPLIT)]
    for there in around:
        block = obj.at[:, :, columns(there)]
        put(block, relay_in.at[middle_at], relaysem.at[middle_at], relay - q + there, when=middle)
        put(block, landing(there, JITTER + STEP + STRIP * q), aheadsem.at[q], (first - SPLIT + there + n) % n, when=above1)
    for there in around[1:]:
        block = obj.at[:, :, columns(there)]
        put(block, landing(there, JITTER + STRIP * q), ownsem.at[q], first + there)
    for there in around:
        block = obj.at[:, pl.ds(STRIP - JITTER, JITTER), columns(there)]
        put(block, landing(there, 0, JITTER), tailsem, (first + SPLIT + there) % n, when=jnp.logical_and(q == SPLIT - 1, below1))
    own_at = mult(LANES * core, LANES)
    own_cols = pl.ds(own_at, OWN)
    sib_cols = pl.ds(mult(OWN * (1 - core), LANES), LANES)
    win[:, rows(JITTER + STRIP * q, STRIP), own_cols] = obj[:, :, columns(q)]
    metas_in[2 * SPLIT + q] = facts

    c, s = cos[...], sin[...]
    ta[0:256, 0:256] = c
    ta[0:256, 256:512] = s
    ta[256:512, 0:256] = -s
    ta[256:512, 256:512] = c
    tb[0:256, 0:256] = c
    tb[0:256, 256:512] = -s
    tb[256:512, 0:256] = s
    tb[256:512, 256:512] = c
    grad[...] = jnp.zeros_like(grad)
    sums9[...] = jnp.zeros_like(sums9)
    kpad[...] = jnp.zeros_like(kpad)
    illum[...] = jnp.zeros_like(illum)
    cross[...] = jnp.zeros_like(cross)
    dobj[...] = jnp.zeros_like(dobj)
    win[:, ROWS:, :] = jnp.zeros((2, 16, WIN), F32)
    load_probe.wait()
    light = jnp.zeros((PATCH, PATCH), F32)
    for m in range(MODES):
        light = light + (probe[0, m] * probe[0, m] + probe[1, m] * probe[1, m])
    kpad[0, ZTOP : ZTOP + PATCH, 0:PATCH] = light

    def arrived(ref, sem):
        return pltpu.make_async_copy(ref, ref, sem)

    def border(start, size):
        mine = pl.ds(mult(LANES * core + 384 * (1 - core), LANES), LANES)
        src = win.at[:, pl.ds(start, size), mine]
        dst = win.at[:, pl.ds(start, size), pl.ds(mult(OWN * core, LANES), LANES)]
        copy = msg.make(src, dst, sibling)
        copy.start()
        return copy

    def far_on(j):
        pl.when(passing)(arrived(relay_in.at[j - 1], relaysem.at[j - 1]).wait)
        put(relay_in.at[j - 1], landing(q, JITTER + 2 * STEP + STRIP * j), finalsem.at[j], target, when=passing)

    for j in range(SPLIT):
        pl.when(q != j)(arrived(landing(q, JITTER + STRIP * j), ownsem.at[j]).wait)
        if j == 0:
            pl.when(below1)(arrived(landing(q, JITTER + STEP), aheadsem.at[0]).wait)
            onward = jnp.logical_and(above1, below1)
            put(landing(q, JITTER + STEP), landing(q, JITTER + 2 * STEP), finalsem.at[0], up, when=onward)
            far_on(1)
        if j == 1:
            far_on(2)
    borders = [border(JITTER, STEP)]
    pl.when(above1)(arrived(landing(q, 0, JITTER), tailsem).wait)
    borders.append(border(0, JITTER))
    for j in range(1, SPLIT):
        pl.when(below1)(arrived(landing(q, JITTER + STEP + STRIP * j), aheadsem.at[j]).wait)
    borders.append(border(JITTER + STEP, STEP))
    for j in range(3):
        pl.when(below2)(arrived(landing(q, JITTER + 2 * STEP + STRIP * j), finalsem.at[j]).wait)
    borders.append(border(JITTER + 2 * STEP, 72))
    for line in range(4):
        there = row - 2 + line
        known = jnp.logical_and(there >= 0, there < rows_all)
        for at in range(SPLIT):
            slot = line * SPLIT + at
            other = known if line != 2 else q != at
            pl.when(other)(arrived(metas_in.at[slot], mrecv.at[slot]).wait)
    to_smem = pltpu.make_async_copy(metas_in, metas, msem)
    to_smem.start()
    load_amps.wait()
    for copy in borders:
        copy.wait_recv()

    msg.drain()
    for copy, when in sends:
        if when is None:
            copy.wait_send()
        else:
            pl.when(when)(copy.wait_send)

    wave, half_done, far = (w0, w1, w2, w3), (h0, h1, h2, h3), (f0, f1, f2, f3)
    chunk = 32
    chunks = PATCH // chunk
    slab = chunk + 2 * JITTER

    def visit(p, carry):
        ahead = jnp.clip(offsets[0, p] - (STEP * row - JITTER), 0, 2 * JITTER)
        base = mult((STEP * p + 40) // LANES * LANES, LANES)
        shift = jnp.clip(offsets[1, p] - STEP * SPLIT * q - base, 0, LANES)
        weight = jnp.where(p < live[0], 1.0, 0.0).astype(F32)
        steps = [slice(i * chunk, (i + 1) * chunk) for i in range(chunks)]
        lows = [slice(PATCH + i * chunk, PATCH + (i + 1) * chunk) for i in range(chunks)]
        left_half, right_half = slice(0, PATCH), slice(PATCH, 2 * PATCH)

        def across(table, m):
            z = jnp.dot(table[...], wave[m][...], preferred_element_type=F32)
            half_done[m][:, left_half] = z[left_half].astype(BF16)
            half_done[m][:, right_half] = z[right_half].astype(BF16)

        def along(table, m):
            far[m][...] = jnp.dot(half_done[m][...], table[...], preferred_element_type=F32)

        for i, at in enumerate(steps):
            for part in range(2):
                v = win[part, i * chunk : i * chunk + slab, pl.ds(base, KCOLS)]
                v = pltpu.roll(v, (slab - ahead) % slab, 0)[0:chunk]
                patch[part, at, :] = pltpu.roll(v, KCOLS - shift, 1)[:, 0:PATCH]
        for m in range(MODES):
            for at, low in zip(steps, lows):
                pr, pi = probe[0, m, at, :], probe[1, m, at, :]
                o_re, o_im = patch[0, at, :], patch[1, at, :]
                wave[m][at, :] = (pr * o_re - pi * o_im).astype(BF16)
                wave[m][low, :] = (pr * o_im + pi * o_re).astype(BF16)
            across(ta, m)
        for m in range(MODES):
            along(tb, m)
            for at in steps:
                fr, fi = far[m][at, left_half], far[m][at, right_half]
                power = fr * fr + fi * fi
                bright[at, :] = power if m == 0 else bright[at, :] + power
        for m in range(MODES):
            for at, low in zip(steps, lows):
                if m == 0:
                    root = jnp.maximum(jnp.sqrt(bright[at, :]), 0.5)
                    factor = (amps[p, at, :] / root - 1.0) * weight
                    bright[at, :] = factor
                else:
                    factor = bright[at, :]
                wave[m][at, :] = (far[m][at, left_half] * factor).astype(BF16)
                wave[m][low, :] = (far[m][at, right_half] * factor).astype(BF16)
            across(tb, m)
        for m in range(MODES):
            along(ta, m)
            for at in steps:
                pr, pi = probe[0, m, at, :], probe[1, m, at, :]
                o_re, o_im = patch[0, at, :], patch[1, at, :]
                cr, ci = far[m][at, left_half], far[m][at, right_half]
                g_re = pr * cr + pi * ci
                g_im = pr * ci - pi * cr
                if m > 0:
                    g_re = g_re + share[0, at, :]
                    g_im = g_im + share[1, at, :]
                share[0, at, :] = g_re
                share[1, at, :] = g_im
                sums9[m, at, :] += o_re * cr + o_im * ci
                sums9[MODES + m, at, :] += o_re * ci - o_im * cr
        blank = jnp.zeros((chunk, KCOLS - PATCH), F32)
        below = jnp.zeros((2 * JITTER, KCOLS), F32)
        for i, at in enumerate(steps):
            o_re, o_im = patch[0, at, :], patch[1, at, :]
            sums9[2 * MODES, at, :] += (o_re * o_re + o_im * o_im) * weight
            for part in range(2):
                v = pltpu.roll(jnp.concatenate([share[part, at, :], blank], 1), shift, 1)
                v = pltpu.roll(jnp.concatenate([v, below], 0), ahead, 0)
                grad[part, i * chunk : i * chunk + slab, pl.ds(base, KCOLS)] += v
        return carry

    lax.fori_loop(0, SPLIT, visit, 0)
    clear_outside(grad)

    for at_band in range(PATCH // 8):
        yy = (at_band // 2) % 8
        for at_lane in range(2):
            xx = (at_band // 16) * 4 + (at_band % 2) * 2 + at_lane
            at_rows = slice(8 * at_band, 8 * at_band + 8)
            at_cols = slice(LANES * at_lane, LANES * at_lane + LANES)
            for k in range(2):
                for i, m in enumerate((2 * k, 2 * k + 1, MODES + 2 * k, MODES + 2 * k + 1, 8)):
                    q_in[k, xx, yy, i] = sums9[m, at_rows, at_cols]
    chunks = [(x + k) % side for k in (4, 5, 3, 6, 2, 7, 1, 0)]
    q_copies = []
    for at in chunks:
        copy = msg.make(q_in.at[1 - core, at], q_sib.at[at], sibling)
        copy.start()
        q_copies.append(copy)
        if not q_copies[1:]:
            to_sib = msg.make(grad.at[:, pl.ds(0, ROWS), sib_cols], sib_in, sibling)
            to_sib.start()
    relay, origin, target, source = long_way(me, 1)

    band = (x // 4) * 16 + y * 2 + (x // 2) % 2
    lane = x % 2
    out_mode = x // 2
    out_band = (x % 2) * 16 + y * 2 + core
    p_tile = probe[:, pl.ds(2 * core, 2), pl.ds(mult(8 * band, 8), 8), pl.ds(mult(LANES * lane, LANES), LANES)]

    def sums(start):
        return grad.at[:, pl.ds(start, STRIP), own_cols]

    def add_sibling(i):
        q_copies[i].wait_recv()
        acc[chunks[i]] = q_in[core, chunks[i]] + q_sib[chunks[i]]

    halves = side // 2

    def send_chain(way, i):
        which = (i % 2 if way < 0 else 1 - i % 2) * halves
        reach = (4 if i % 2 == 0 else 3) - i // 2
        dest = (x + way * reach + side) % side
        copy = msg.make(
            acc.at[dest, pl.ds(which, halves)],
            (minus_in if way < 0 else plus_in).at[i],
            chip(x + way + side, y, core),
        )
        copy.start()
        return copy

    chains = {}
    add_sibling(0)
    chains[-1, 0], chains[1, 0] = send_chain(-1, 0), send_chain(1, 0)
    add_sibling(1)
    chains[-1, 1] = send_chain(-1, 1)
    add_sibling(2)
    chains[1, 1] = send_chain(1, 1)
    to_sib.wait_recv()
    edge = pl.ds(mult(LANES * core + 384 * (1 - core), LANES), LANES)
    grad[:, 0:ROWS, edge] += sib_in[...]

    far_out = []
    for j in (1, 2):
        copy = msg.make(sums(JITTER + 2 * STEP + STRIP * j), back_in.at[j - 1], relay)
        copy.start()
        far_out.append(copy)
    t2 = msg.make(sums(JITTER + 2 * STEP), t2_in, down)
    t2.start()
    t8 = msg.make(grad.at[:, pl.ds(0, JITTER), own_cols], t8_in, up)
    t8.start()

    at_row = (me // SPLIT) % 4
    crossing = at_row == 3
    holder = at_row == 0
    turning = jnp.logical_or(at_row == 1, at_row == 2)
    far_holder = at_row <= 1
    below = x * 2 * side + (at_row + 1) % 4 * SPLIT + q
    beside = chip(x + 1, y, core)

    def start_t1(j):
        src = sums(JITTER + STEP + STRIP * j)
        t1[j] = msg.make(src, t1_in.at[j], below, when=jnp.logical_not(crossing))
        final_sem = msg.last
        pl.when(jnp.logical_not(crossing))(t1[j].start)
        copy = msg.make(src, hold_t1.at[j], below, when=crossing)
        pl.when(crossing)(copy.start)
        held.append((copy, holder, hold_t1.at[j], t1_in.at[j], final_sem))

    def pass_far(j):
        there = x * 2 * side + (at_row + 3) % 4 * SPLIT + q
        final = msg.make(back_in.at[j], far_in.at[j], there, when=jnp.logical_not(turning))
        final_sem = msg.last
        pl.when(jnp.logical_not(turning))(final.start)
        copy = msg.make(back_in.at[j], hold_far.at[j], there, when=turning)
        pl.when(turning)(copy.start)
        held.append((copy, far_holder, hold_far.at[j], far_in.at[j], final_sem))
        return final

    def release(i):
        copy, here, src, dst, final_sem = held[i]
        pl.when(here)(copy.wait_recv)
        onward = pltpu.make_async_remote_copy(
            src_ref=src,
            dst_ref=dst,
            send_sem=holdsem.at[i],
            recv_sem=final_sem,
            device_id={"scan": beside},
            device_id_type=MESH,
        )
        pl.when(here)(onward.start)
        msg.open.append((onward, here))

    t1, held = {}, []
    start_t1(3)
    for i in range(3, 8):
        add_sibling(i)

    def x_step(i):
        for way, arrived in ((-1, minus_in), (1, plus_in)):
            which = (i % 2 if way < 0 else 1 - i % 2) * halves
            reach = (4 if i % 2 == 0 else 3) - 1 - i // 2
            dest = (x + way * reach + side) % side
            chains[way, i].wait_recv()
            acc[dest, which : which + halves] += arrived[i]
            if reach > 0:
                chains[way, i + 2] = send_chain(way, i + 2)

    to_smem.wait()
    x_step(0)
    start_t1(1)
    spread(n, kpad, illum, metas, 0)
    x_step(1)
    start_t1(2)
    spread(n, kpad, illum, metas, 1)
    x_step(2)
    t2.wait_recv()
    grad[:, JITTER + STEP : JITTER + STEP + STRIP, own_cols] += t2_in[...]
    x_step(3)
    far_final = []
    for j in range(2):
        far_out[j].wait_recv()
        far_final.append(pass_far(j))
    x_step(4)
    spread(n, kpad, illum, metas, 2)
    x_step(5)
    x_step(6)

    y_copies = []
    for k in range(1, side):
        copy = pltpu.make_async_remote_copy(
            src_ref=acc.at[x, (y + k) % side],
            dst_ref=y_in.at[k - 1],
            send_sem=bsend.at[k - 1],
            recv_sem=ysem,
            device_id={"scan": chip(x, y + k, core)},
            device_id_type=MESH,
        )
        copy.start()
        y_copies.append(copy)
    start_t1(0)
    for i in range(3):
        release(i)
    pltpu.make_async_copy(y_in, y_in, ysem).wait()
    release(3)
    release(4)
    tile[...] = acc[x, y] + jnp.sum(y_in[...], 0)
    norm = tile[4]
    inverse = norm + 1.0
    k_re = jnp.zeros((8, LANES), F32)
    k_im = jnp.zeros((8, LANES), F32)
    s_vv = jnp.zeros((8, LANES), F32)
    s_vc = jnp.zeros((8, LANES), F32)
    for m in range(2):
        g_re, g_im = tile[m], tile[2 + m]
        d_re, d_im = g_re / inverse, g_im / inverse
        dp[m, 0] = d_re
        dp[m, 1] = d_im
        p_re, p_im = p_tile[0, m], p_tile[1, m]
        k_re = k_re + (p_re * d_re + p_im * d_im)
        k_im = k_im + (p_re * d_im - p_im * d_re)
        s_vv = s_vv + (d_re * d_re + d_im * d_im) * norm
        s_vc = s_vc + (d_re * g_re + d_im * g_im)
    kmine[0] = k_re
    kmine[1] = k_im
    k_copy = msg.make(kmine.at[1 - core], ksib, sibling)
    k_copy.start()

    dp_sends = []
    for m in range(2):
        dest = chip(2 * (2 * core + m) + x // 4, y, (x // 2) % 2)
        away = dest != me
        copy = pltpu.make_async_remote_copy(
            src_ref=dp.at[m],
            dst_ref=dp_in.at[lane],
            send_sem=bsend.at[21 + m],
            recv_sem=dpsem.at[lane],
            device_id={"scan": dest},
            device_id_type=MESH,
        )
        pl.when(away)(copy.start)
        dp_sends.append((copy, away))

        @pl.when(jnp.logical_not(away))
        def _():
            dp_in[lane] = dp[m]

    k_copy.wait_recv()
    kk[core, x, y] = kmine[core] + ksib[...]
    ky_copies = []
    for k in range(1, side):
        copy = pltpu.make_async_remote_copy(
            src_ref=kk.at[core, x, y],
            dst_ref=kk.at[core, x, y],
            send_sem=bsend.at[7 + k - 1],
            recv_sem=kysem,
            device_id={"scan": chip(x, y + k, core)},
            device_id_type=MESH,
        )
        copy.start()
        ky_copies.append(copy)

    release(5)
    pltpu.make_async_copy(kk.at[0, 0, pl.ds(0, 7)], kk.at[0, 0, pl.ds(0, 7)], kysem).wait()
    kx_copies = []
    for k in range(1, side):
        copy = pltpu.make_async_remote_copy(
            src_ref=kk.at[core, x],
            dst_ref=kk.at[core, x],
            send_sem=bsend.at[14 + k - 1],
            recv_sem=kxsem,
            device_id={"scan": chip(x + k, y, core)},
            device_id_type=MESH,
        )
        copy.start()
        kx_copies.append(copy)
    pieces = []
    for j in (3, 1, 2, 0):
        t1[j].wait_recv()
        lo = JITTER + STRIP * j
        grad[:, lo : lo + STRIP, own_cols] += t1_in[j]
        if j == 3:
            t8.wait_recv()
            grad[:, STEP : STEP + JITTER, own_cols] += t8_in[...]
        if j in (1, 2):
            far_final[j - 1].wait_recv()
            grad[:, lo : lo + STRIP, own_cols] += far_in[j - 1]
        slot = (j - q + SPLIT) % SPLIT
        copy = pltpu.make_async_remote_copy(
            src_ref=grad.at[:, pl.ds(lo, STRIP), own_cols],
            dst_ref=piece.at[slot],
            send_sem=bsend.at[23 + j],
            recv_sem=psem.at[slot],
            device_id={"scan": first + j},
            device_id_type=MESH,
        )
        pl.when(q != j)(copy.start)
        pieces.append((copy, q != j))

    piece[0] = grad[:, pl.ds(mult(JITTER + STRIP * q, 8), STRIP), own_cols]

    for k in range(SPLIT):
        if k > 0:
            pltpu.make_async_copy(piece.at[k], piece.at[k], psem.at[k]).wait()
        source = (q - k + SPLIT) % SPLIT
        at = pl.ds(mult(768 * (source // 2) + OWN * (source % 2), LANES), OWN)
        dobj[:, :, at] += piece[k]
    lit = illum[0]
    g_re, g_im = dobj[0], dobj[1]
    o_re, o_im = obj[0], obj[1]
    d_re, d_im = g_re / (lit + 1.0), g_im / (lit + 1.0)
    s_uu = jnp.sum((d_re * d_re + d_im * d_im) * lit)
    s_uc = jnp.sum(d_re * g_re + d_im * g_im)
    dobj[0] = d_re
    dobj[1] = d_im

    place[0] = d_re * o_re + d_im * o_im
    place[1] = d_re * o_im - d_im * o_re
    for line in range(3):
        collect(n, place, cross, metas, line)
    cross_copy = msg.make(cross.at[1 - core, pl.ds(ZTOP, PATCH)], cross_in, sibling)
    cross_copy.start()
    pltpu.make_async_copy(kk.at[0, pl.ds(0, 7)], kk.at[0, pl.ds(0, 7)], kxsem).wait()
    cross_copy.wait_recv()
    product = jnp.zeros((8, LANES), F32)
    for at_band in range(PATCH // 8):
        for at_lane in range(2):
            xx = (at_band // 16) * 4 + (at_band % 2) * 2 + at_lane
            yy = (at_band // 2) % 8
            rows_at = slice(8 * at_band, 8 * at_band + 8)
            cols = slice(LANES * at_lane, LANES * at_lane + LANES)
            both = cross[core, ZTOP + 8 * at_band : ZTOP + 8 * at_band + 8, cols] + cross_in[rows_at, cols]
            product = product + kk[core, xx, yy] * both
    s_uv = jnp.sum(product) * jnp.where(core == 0, 1.0, -1.0).astype(F32)

    at = lax.broadcasted_iota(jnp.int32, (8, LANES), 1)
    own_sums = jnp.zeros((8, LANES), F32)
    for i, value in enumerate((s_uu, s_uv, jnp.sum(s_vv), s_uc, jnp.sum(s_vc))):
        own_sums = jnp.where(at == i, value, own_sums)
    vec[...] = own_sums
    v1_copies = []
    for k in range(1, 2 * side):
        copy = pltpu.make_async_remote_copy(
            src_ref=vec.at[pl.ds(0, 1)],
            dst_ref=vec1.at[pl.ds(k - 1, 1)],
            send_sem=bsend.at[27 + k - 1],
            recv_sem=v1sem,
            device_id={"scan": chip(x, y + k // 2, (core + k) % 2)},
            device_id_type=MESH,
        )
        copy.start()
        v1_copies.append(copy)
    pltpu.make_async_copy(vec1.at[pl.ds(0, 15)], vec1.at[pl.ds(0, 15)], v1sem).wait()
    for copy in v1_copies:
        copy.wait_send()
    vec[...] = own_sums + jnp.sum(vec1[0:15, :], 0, keepdims=True)
    v2_copies = []
    for k in range(1, side):
        copy = pltpu.make_async_remote_copy(
            src_ref=vec.at[pl.ds(0, 1)],
            dst_ref=vec2.at[pl.ds(k - 1, 1)],
            send_sem=bsend.at[42 + k - 1],
            recv_sem=v2sem,
            device_id={"scan": chip(x + k, y, core)},
            device_id_type=MESH,
        )
        copy.start()
        v2_copies.append(copy)
    for at_lane in range(2):
        source = chip((x % 2) * 4 + core * 2 + at_lane, y, x // 4)
        arrived = pltpu.make_async_copy(dp_in.at[at_lane], dp_in.at[at_lane], dpsem.at[at_lane])
        pl.when(source != me)(arrived.wait)
    pltpu.make_async_copy(vec2.at[pl.ds(0, 7)], vec2.at[pl.ds(0, 7)], v2sem).wait()
    totals = vec[...] + jnp.sum(vec2[0:7, :], 0, keepdims=True)
    uu, uv, vv, uc, vc = (totals[0:1, i : i + 1] for i in range(5))
    a = 1.1 * uu + 1e-06
    d = 1.1 * vv + 1e-06
    det = a * d - uv * uv
    rate_obj = (uc * d - uv * vc) / det
    rate_probe = (a * vc - uv * uc) / det
    at = lax.broadcasted_iota(jnp.int32, (8, LANES), 1)
    rates[...] = jnp.where(at == 0, rate_obj, rate_probe)
    obj_step[...] = dobj[...]
    for part in range(2):
        for at_lane in range(2):
            cols = slice(LANES * at_lane, LANES * at_lane + LANES)
            probe_out[0, part, :, cols] = dp_in[at_lane, part]
            probe_out[1, part, :, cols] = probe[part, out_mode, pl.ds(mult(8 * out_band, 8), 8), cols]

    msg.drain()
    for copy in y_copies + ky_copies + kx_copies + v2_copies:
        copy.wait_send()
    for copy, when in dp_sends + pieces:
        pl.when(when)(copy.wait_send)


def finish_kernel(obj, obj_step, probe_out, rates, new_obj, new_probe):
    rate_obj, rate_probe = rates[0:1, 0:1], rates[0:1, 1:2]
    for part in range(2):
        new_obj[part] = obj[part] + rate_obj * obj_step[part]
        new_probe[part] = probe_out[1, part] + rate_probe * probe_out[0, part]


def finish(obj, obj_step, probe_out, rates):
    vmem = pl.BlockSpec(memory_space=pltpu.VMEM)
    return pl.pallas_call(
        finish_kernel,
        out_shape=(
            jax.ShapeDtypeStruct(obj.shape, F32),
            jax.ShapeDtypeStruct(probe_out.shape[1:], F32),
        ),
        in_specs=[vmem] * 4,
        out_specs=[vmem] * 2,
        name="finish",
    )(obj, obj_step, probe_out, rates)


def step(n, offsets, live, obj, probe, amps, cos, sin):
    vmem = pl.BlockSpec(memory_space=pltpu.VMEM)
    smem = pl.BlockSpec(memory_space=pltpu.SMEM)
    hbm = pl.BlockSpec(memory_space=pl.ANY)
    dma = pltpu.SemaphoreType.DMA
    columns = obj.shape[2]

    def f32(*shape):
        return pltpu.VMEM(shape, F32)

    return pl.pallas_call(
        functools.partial(step_kernel, n),
        out_shape=(
            jax.ShapeDtypeStruct((2, STRIP, columns), F32),
            jax.ShapeDtypeStruct((2, 2, 8, PATCH), F32),
            jax.ShapeDtypeStruct((8, LANES), F32),
        ),
        in_specs=[smem, smem, vmem, hbm, hbm, vmem, vmem],
        out_specs=[vmem] * 3,
        scratch_shapes=[
            pltpu.VMEM((8, LANES), jnp.int32),
            pltpu.VMEM((4 * SPLIT, 8, LANES), jnp.int32),
            pltpu.SMEM((4 * SPLIT, 8, LANES), jnp.int32),
            f32(2, MODES, PATCH, PATCH),
            f32(SPLIT, PATCH, PATCH),
            f32(2, ROWS + 16, WIN),
            f32(2, 2, STRIP, OWN),
            f32(2, ROWS + 16, WIN),
            f32(2, PATCH, PATCH),
            f32(2, PATCH, PATCH),
            f32(PATCH, PATCH),
            f32(2 * MODES + 1, PATCH, PATCH),
            pltpu.VMEM((2 * PATCH, 2 * PATCH), BF16),
            pltpu.VMEM((2 * PATCH, 2 * PATCH), BF16),
            *[pltpu.VMEM((2 * PATCH, PATCH), BF16) for m in range(MODES)],
            *[pltpu.VMEM((PATCH, 2 * PATCH), BF16) for m in range(MODES)],
            *[f32(PATCH, 2 * PATCH) for m in range(MODES)],
            f32(2, 8, 8, 5, 8, LANES),
            f32(2, ROWS, LANES),
            f32(2, STRIP, OWN),
            f32(4, 2, STRIP, OWN),
            f32(2, JITTER, OWN),
            f32(2, 2, STRIP, OWN),
            f32(2, 2, STRIP, OWN),
            f32(4, 2, STRIP, OWN),
            f32(8, 8, 5, 8, LANES),
            f32(8, 8, 5, 8, LANES),
            f32(7, 4, 5, 8, LANES),
            f32(7, 4, 5, 8, LANES),
            f32(7, 5, 8, LANES),
            f32(4, 2, STRIP, OWN),
            f32(2, 2, STRIP, OWN),
            f32(5, 8, LANES),
            f32(2, 2, 8, LANES),
            f32(2, 2, 8, LANES),
            f32(2, 8, LANES),
            f32(8, LANES),
            f32(2, 8, 8, 8, LANES),
            f32(1, KROWS, KCOLS),
            f32(1, STRIP, columns),
            f32(2, STRIP, columns),
            f32(2, STRIP, columns),
            f32(2, KROWS, PATCH),
            f32(PATCH, PATCH),
            f32(8, LANES),
            f32(16, LANES),
            f32(8, LANES),
            dma((48,)),
            dma((48,)),
            dma,
            dma,
            dma,
            dma,
            dma,
            dma((50,)),
            dma((2,)),
            dma((4,)),
            dma((2,)),
            dma((40,)),
            dma((4,)),
            dma((4,)),
            dma((2,)),
            dma((3,)),
            dma,
            dma((16,)),
            dma,
            dma((6,)),
        ],
        compiler_params=pltpu.CompilerParams(collective_id=0, has_side_effects=True),
        name="step",
    )(offsets, live, obj, probe, amps, cos, sin)


def tables(length):
    numbers = np.arange(length, dtype=np.int64)
    angles = (numbers[:, None] * numbers[None, :] % length).astype(np.float32)
    angles = angles * np.float32(2.0 * math.pi / length)
    scaling = np.float32(1.0 / math.sqrt(length))
    return tuple(jnp.asarray(f(angles) * scaling).astype(BF16) for f in (np.cos, np.sin))


def on_device(n, object_field, probe_field, amplitudes, offsets, live_counts):
    probe = probe_field.reshape(2, MODES, PATCH, PATCH)
    cos, sin = tables(PATCH)
    updates = step(n, offsets.T, live_counts, object_field, probe, amplitudes, cos, sin)
    return finish(object_field, *updates)


def solution(mesh):
    groups_scan = ("groups", "scan")
    placed = (
        P(None, groups_scan, None),
        P(None, "groups", None),
        P(groups_scan, None, None),
        P(groups_scan, None),
        P(groups_scan),
    )
    return jax.shard_map(
        functools.partial(on_device, mesh.shape["scan"]),
        mesh=mesh,
        in_specs=placed,
        out_specs=(P(None, groups_scan, None), P(None, groups_scan, None)),
        check_vma=False,
    )
```
